256 devices in a mesh: grp: 4 (over y), blk: 64 (over z, x, core).
Axes of the slice: x: 4, y: 4, z: 8, core: 2. Of those that a mesh axis runs over, the one named last changes fastest.
Arguments:
- features: bfloat16 [262144, 256], P(('grp', 'blk')), may hold values from -40 to 40, as said below
- source_index: int32 [4096, 128], P(('grp', 'blk')), may hold values from 0 to 3071
- target_index: int32 [4096, 128], P(('grp', 'blk')), may hold values from 0 to 1023
- edge_valid: int32 [4096, 128], P(('grp', 'blk')), may hold values from 0 to 1, as said below
- edge_bias: float32 [8, 524288], P(None, ('grp', 'blk')), may hold values from -4 to 284
- send_list: int32 [256, 2048], P(('grp', 'blk')), may hold values from 0 to 1023
- w_left: bfloat16 [2, 256, 256], replicated, may hold values from -0.375 to 0.375
- w_right: bfloat16 [2, 256, 256], replicated, may hold values from -0.375 to 0.375
- w_skip: bfloat16 [2, 256, 256], replicated, may hold values from -0.375 to 0.375
- attn_vec: bfloat16 [2, 256], replicated, may hold values from -1 to 1
- norm_gain: bfloat16 [2, 256], replicated, may hold values from 0.5 to 1.5
- norm_shift: bfloat16 [2, 256], replicated, may hold values from -3 to 3
Outputs:
- node_states: bfloat16 [262144, 256], P(('grp', 'blk'))
The draws below stay inside these ranges and needn't reach their ends.
Inputs may be any that keep to these rules, and one draw needn't show every extreme that they name: `features`: A spread of order one around a few large per-device offsets. `edge_valid`: the live slots of each device form a prefix of its 2048 slots, at least a quarter of them; in every draw some device has all its slots live.
All inputs are finite; a program needn't handle non-finite values.
Results may differ from the reference program's by a relative error of at most 0.007.
Values may be sent and summed in bfloat16 or wider, within the bound.
No kernel may reach another device: no remote copies, remote signals or barrier semaphores. Data moves between devices by JAX's collectives and lax.ppermute only.
A program may use at most 64 MiB of HBM per device.

```python
import jax
import jax.numpy as jnp
from jax import lax

D = 256
HEADS = 8
HEAD = 32
NODE_DEV = 1024
SEND = 8
TILE = 128
LAYERS = 2
PEERS = 256
TILES = 16
NODES = 262144
EDGES = 524288


def draw_features(key, part):
    noise_key = jax.random.fold_in(key, 11)
    owner_key = jax.random.fold_in(key, 12)
    sign_key = jax.random.fold_in(key, 13)
    owners = jax.random.randint(owner_key, (PEERS,), 0, D)
    sign_vals = (jax.random.randint(sign_key, (PEERS,), 0, 2) * 2 - 1).astype(jnp.float32)
    noise_part = jnp.clip(jax.random.normal(noise_key, (PEERS, NODE_DEV, D), jnp.float32), -6.0, 6.0)
    height = 30.0
    owner_mask = (jnp.arange(D)[None, :] == owners[:, None]).astype(jnp.float32)
    lifted = noise_part + (height * sign_vals[:, None] * owner_mask)[:, None, :]
    return lifted.reshape(NODES, D).astype(jnp.bfloat16)


def draw_edge_bias(key, part):
    base_key = jax.random.fold_in(key, 21)
    base_part = jnp.clip(jax.random.normal(base_key, (HEADS, EDGES), jnp.float32), -4.0, 4.0)
    return base_part


def draw_edge_valid(key, part):
    live_key = jax.random.fold_in(key, 31)
    full_key = jax.random.fold_in(key, 32)
    dev_edges = TILES * TILE
    live_counts = jax.random.randint(live_key, (PEERS,), dev_edges // 4, dev_edges + 1)
    full_dev = jax.random.randint(full_key, (), 0, PEERS)
    live_counts = jnp.where(jnp.arange(PEERS) == full_dev, dev_edges, live_counts)
    positions = jnp.arange(dev_edges)
    live_flags = (positions[None, :] < live_counts[:, None]).astype(jnp.int32)
    return live_flags.reshape(PEERS * TILES, TILE)


def touch_ends(array, key, least, high):
    dims = array.shape
    spot = [jax.random.randint(jax.random.fold_in(key, axis), (), 0, dims[axis]) for axis in range(len(dims))]
    array = array.at[tuple(spot)].set(least)
    longest = dims.index(max(dims))
    spot[longest] = (spot[longest] + 1) % dims[longest]
    return array.at[tuple(spot)].set(high)


def centred(key, extent, scale, bound, kind=jnp.bfloat16):
    values = scale * jax.random.normal(key, extent, jnp.float32)
    return jnp.clip(values, min=-bound, max=bound).astype(kind)


def setup_inputs(seed: int = 0) -> dict:
    streams_of = jax.random.split(jax.random.key(seed), 13)
    return {
        "features": draw_features(jax.random.fold_in(streams_of[12], 71), 0),
        "source_index": touch_ends(jax.random.randint(streams_of[1], (PEERS * TILES, TILE), 0, NODE_DEV + SEND * PEERS), jax.random.fold_in(streams_of[1], 1), 0, (NODE_DEV + SEND * PEERS) - 1).astype(jnp.int32),
        "target_index": touch_ends(jax.random.randint(streams_of[2], (PEERS * TILES, TILE), 0, NODE_DEV), jax.random.fold_in(streams_of[2], 1), 0, NODE_DEV - 1).astype(jnp.int32),
        "edge_valid": draw_edge_valid(jax.random.fold_in(streams_of[12], 71), 0),
        "edge_bias": draw_edge_bias(jax.random.fold_in(streams_of[12], 71), 0),
        "send_list": touch_ends(jax.random.randint(streams_of[5], (PEERS, PEERS * SEND), 0, NODE_DEV), jax.random.fold_in(streams_of[5], 1), 0, NODE_DEV - 1).astype(jnp.int32),
        "w_left": centred(streams_of[6], (LAYERS, D, D), D ** -0.5, 0.375),
        "w_right": centred(streams_of[7], (LAYERS, D, D), D ** -0.5, 0.375),
        "w_skip": centred(streams_of[8], (LAYERS, D, D), D ** -0.5, 0.375),
        "attn_vec": centred(streams_of[9], (LAYERS, D), HEAD ** -0.5, 1.0),
        "norm_gain": jnp.clip(1.0 + 0.1 * jax.random.normal(streams_of[10], (LAYERS, D), jnp.float32), 0.5, 1.5).astype(jnp.bfloat16),
        "norm_shift": centred(streams_of[11], (LAYERS, D), 0.5, 3.0),
    }


def project(inputs, weight):
    return jnp.dot(inputs, weight, preferred_element_type=jnp.float32)

def leaky(values):
    return jnp.where(values > 0, values, 0.2 * values)

def head_matrix(attn_row, head_count):
    feat_width = attn_row.shape[0]
    head_ids = jnp.arange(feat_width, dtype=jnp.int32) // (feat_width // head_count)
    owner_mask = head_ids[None, :] == jnp.arange(head_count, dtype=jnp.int32)[:, None]
    return jnp.where(owner_mask, attn_row.astype(jnp.float32)[None, :], jnp.zeros((), jnp.float32)).astype(jnp.float32)

def head_scores(head_weights, hidden):
    return lax.dot_general(head_weights, hidden, (((1,), (1,)), ((), ())), precision=lax.Precision.HIGHEST)

def spread_heads(weights, feat_width):
    head_count = weights.shape[0]
    return jnp.repeat(weights, feat_width // head_count, axis=0).T

def attend(source_table, left_own, right_own, sources, targets, valids, bias_rows, head_weights):
    node_count, feat_width = left_own.shape
    head_count = head_weights.shape[0]
    edge_count = sources.shape[0]
    block_size = min(edge_count, 4096)
    block_count = edge_count // block_size
    src_blocks = sources.reshape(block_count, block_size)
    dst_blocks = targets.reshape(block_count, block_size)

    def score_block(pair_ids):
        src_ids, dst_ids = pair_ids
        hidden = leaky(source_table[src_ids].astype(jnp.float32) + right_own[dst_ids].astype(jnp.float32))
        return head_scores(head_weights, hidden)
    scores = lax.map(score_block, (src_blocks, dst_blocks))
    scores = jnp.transpose(scores, (1, 0, 2)).reshape(head_count, edge_count) + bias_rows
    live_edges = valids[None, :] > 0
    scores = jnp.where(live_edges, scores, jnp.full((), -1e+30, scores.dtype))
    own_hidden = leaky(left_own.astype(jnp.float32) + right_own.astype(jnp.float32))
    own_scores = head_scores(head_weights, own_hidden)
    seg_max = jax.vmap(lambda values: jax.ops.segment_max(values, targets, num_segments=node_count))(scores)
    score_top = jnp.maximum(seg_max, own_scores)
    edge_weights = jnp.where(live_edges, jnp.exp(scores - score_top[:, targets]), jnp.zeros((), scores.dtype))
    own_weights = jnp.exp(own_scores - score_top)
    denom_sum = own_weights + jax.vmap(lambda values: jax.ops.segment_sum(values, targets, num_segments=node_count))(edge_weights)
    edge_alpha = (edge_weights / denom_sum[:, targets]).astype(jnp.bfloat16)
    own_alpha = (own_weights / denom_sum).astype(jnp.bfloat16)
    alpha_blocks = jnp.transpose(edge_alpha.reshape(head_count, block_count, block_size), (1, 0, 2))

    def add_block(running, triple):
        src_ids, dst_ids, alpha_part = triple
        messages = source_table[src_ids].astype(jnp.float32) * spread_heads(alpha_part.astype(jnp.float32), feat_width)
        return (running + jax.ops.segment_sum(messages, dst_ids, num_segments=node_count), None)
    start_sum = spread_heads(own_alpha.astype(jnp.float32), feat_width) * left_own.astype(jnp.float32)
    gathered, _ = lax.scan(add_block, start_sum, (src_blocks, dst_blocks, alpha_blocks))
    return gathered

def normalize(summed, feat_mean, spread, gain_row, shift_row):
    scaled = (summed - feat_mean) * lax.rsqrt(spread + 0.1)
    return jax.nn.elu(scaled * gain_row.astype(jnp.float32) + shift_row.astype(jnp.float32)).astype(jnp.bfloat16)

def reference(features, source_index, target_index, edge_valid, edge_bias, send_list, w_left, w_right, w_skip, attn_vec, norm_gain, norm_shift):
    node_states = features.reshape(PEERS, NODE_DEV, D)
    sources = source_index.reshape(PEERS, TILES * TILE)
    targets = target_index.reshape(PEERS, TILES * TILE)
    valids = edge_valid.reshape(PEERS, TILES * TILE)
    biases = edge_bias.reshape(HEADS, PEERS, TILES * TILE)
    routes = send_list.reshape(PEERS, PEERS, SEND)
    for layer_idx in range(LAYERS):
        left_all = project(node_states.reshape(NODES, D), w_left[layer_idx]).astype(jnp.bfloat16).reshape(PEERS, NODE_DEV, D)
        head_weights = head_matrix(attn_vec[layer_idx], HEADS)

        def one_device(device):
            chosen = lax.dynamic_index_in_dim(routes, device, 1, keepdims=False)
            bundle = jax.vmap(lambda own_rows, row_ids: own_rows[row_ids])(left_all, chosen)
            left_own = left_all[device]
            source_table = jnp.concatenate([left_own, bundle.reshape(PEERS * SEND, D)], axis=0)
            own_states = node_states[device]
            right_own = project(own_states, w_right[layer_idx]).astype(jnp.bfloat16)
            skip_own = project(own_states, w_skip[layer_idx])
            gathered = attend(source_table, left_own, right_own, sources[device], targets[device], valids[device], biases[:, device], head_weights)
            return own_states.astype(jnp.float32) + gathered + skip_own
        summed = lax.map(one_device, jnp.arange(PEERS, dtype=jnp.int32))
        feat_mean = lax.optimization_barrier(jnp.sum(summed, axis=(0, 1))) / NODES
        spread = lax.optimization_barrier(jnp.sum((summed - feat_mean) ** 2, axis=(0, 1))) / NODES
        node_states = normalize(summed, feat_mean, spread, norm_gain[layer_idx], norm_shift[layer_idx])
    return node_states.reshape(NODES, D)
```

```python
import functools

import jax
import jax.numpy as jnp
from jax import lax
from jax.experimental import pallas as pl
from jax.experimental.pallas import tpu as pltpu
from jax.sharding import Mesh
from jax.sharding import PartitionSpec as P

HEADS = 8
LAYERS = 2
GRP_BLK = ("grp", "blk_0", "blk_1", "blk_2")
NODES_OWN = 1024
EDGES_OWN = 2048
ROWS_IN = 2048
FEAT = 256
CHUNK = 256
EDGE_CHUNKS = EDGES_OWN // CHUNK
NODE_CHUNKS = NODES_OWN // CHUNK
F32 = jnp.float32
BF16 = jnp.bfloat16


def iota(shape, dim):
    return lax.broadcasted_iota(jnp.int32, shape, dim)


def one_hot(mask):
    return jnp.where(mask, 1.0, 0.0).astype(BF16)


def dot(lhs, rhs):
    return jnp.dot(lhs, rhs, preferred_element_type=F32)


def dot_t(lhs, rhs):
    return lax.dot_general(lhs, rhs, (((1,), (1,)), ((), ())), preferred_element_type=F32)


def leaky(values):
    return jnp.where(values > 0, values, 0.2 * values)


def split_two(values):
    high = values.astype(BF16)
    return high, (values - high.astype(F32)).astype(BF16)


def split_three(values):
    high = values.astype(BF16)
    rest = values - high.astype(F32)
    mid = rest.astype(BF16)
    return high, mid, (rest - mid.astype(F32)).astype(BF16)


def head_rows(attn_ref, layer):
    shape = (16, FEAT)
    owner = iota(shape, 1) // (FEAT // HEADS) == iota(shape, 0)
    row = attn_ref[layer : layer + 1, :].astype(F32)
    return jnp.where(owner, row, 0.0).astype(BF16)


def head_spread():
    shape = (16, 2 * FEAT)
    return one_hot(iota(shape, 1) // (FEAT // HEADS) == iota(shape, 0))


def scores_of(heads, hidden):
    high, low = split_two(hidden)
    return (dot_t(heads, high) + dot_t(heads, low))[:HEADS]


def norm_terms(stats, total_nodes, gain, shift):
    mean = stats[0:1, :] / total_nodes
    spread = jnp.maximum(stats[1:2, :] / total_nodes - mean * mean, 0.0)
    return mean, lax.rsqrt(spread + 0.1), gain, shift


def normalize(values, terms):
    mean, inv, gain, shift = terms
    scaled = (values - mean) * inv * gain + shift
    grown = jnp.exp(jnp.minimum(scaled, 0.0)) - 1.0
    return jnp.where(scaled > 0, scaled, grown).astype(BF16)


def columns_of(row):
    return jnp.transpose(jnp.broadcast_to(row, (8, row.shape[1])))


def pick_rows(list_ref, table_ref, out_ref, col_ref):
    col_ref[...] = columns_of(list_ref[...].astype(F32)).astype(jnp.int32)

    def step(c, carry):
        at = pl.ds(pl.multiple_of(c * CHUNK, CHUNK), CHUNK)
        hot = one_hot(col_ref[at, 0:1] == iota((CHUNK, NODES_OWN), 1))
        out_ref[at, :] = dot(hot, table_ref[...]).astype(BF16)
        return carry

    lax.fori_loop(0, ROWS_IN // CHUNK, step, 0)


def send_kernel(list_ref, table_ref, out_ref, col_ref):
    pick_rows(list_ref, table_ref, out_ref, col_ref)


def sort_kernel(
    src_ref, tgt_ref, valid_ref, bias_ref, rows_ref, cols_ref, bias_out, noedge_ref, bound_ref,
    key_ref, pos_ref, meta_ref,
):
    width = (1, EDGES_OWN)
    live_in = valid_ref[...] > 0
    src = src_ref[...]
    tgt = jnp.where(live_in, tgt_ref[...], NODES_OWN)
    key = tgt * EDGES_OWN + iota(width, 1)
    key_ref[...] = columns_of(key.astype(F32)).astype(jnp.int32)
    pos_ref[...] = jnp.zeros_like(pos_ref)

    def rank(c, carry):
        at = pl.ds(pl.multiple_of(c * CHUNK, CHUNK), CHUNK)
        less = jnp.where(key_ref[at, 0:1] < key, 1.0, 0.0)
        pos_ref[...] += jnp.sum(less, axis=0, keepdims=True)
        return carry

    lax.fori_loop(0, EDGE_CHUNKS, rank, 0)
    pos = pos_ref[...].astype(jnp.int32)
    sub = iota((8, EDGES_OWN), 0)
    ints = jnp.where(
        sub == 0,
        src // 256,
        jnp.where(sub == 1, src % 256, jnp.where(sub == 2, tgt // 256, tgt % 256)),
    )
    high, mid, low = split_three(bias_ref[...])
    meta = jnp.concatenate(
        [ints.astype(F32), high.astype(F32), mid.astype(F32), low.astype(F32)], axis=0
    ).astype(BF16)

    def place(c, carry):
        at = pl.ds(pl.multiple_of(c * CHUNK, CHUNK), CHUNK)
        perm = one_hot(pos == iota((CHUNK, EDGES_OWN), 0) + c * CHUNK)
        meta_ref[:, at] = dot_t(meta, perm)
        return carry

    lax.fori_loop(0, EDGE_CHUNKS, place, 0)
    placed = meta_ref[...]
    bias_out[...] = placed[8:16] + placed[16:24] + placed[24:32]
    src_s = (placed[0:1] * 256.0 + placed[1:2]).astype(jnp.int32)
    tgt_s = (placed[2:3] * 256.0 + placed[3:4]).astype(jnp.int32)
    lane8 = iota((8, EDGES_OWN), 1)
    both = jnp.where(sub == 0, src_s, tgt_s)
    cols_ref[...] = jnp.transpose(both.astype(F32)).astype(jnp.int32)
    tgt8 = jnp.broadcast_to(tgt_s, (8, EDGES_OWN))
    before = pltpu.roll(tgt8, 1, 1)
    after = pltpu.roll(tgt8, EDGES_OWN - 1, 1)
    live = tgt8 < NODES_OWN
    first = (lane8 == 0) | (before != tgt8)
    last = (lane8 == EDGES_OWN - 1) | (after != tgt8)
    start = jnp.where(first, lane8, 0)
    end = jnp.where(last, lane8, EDGES_OWN)
    step = 1
    while step < EDGES_OWN:
        start = jnp.maximum(start, jnp.where(lane8 >= step, pltpu.roll(start, step, 1), 0))
        shifted = pltpu.roll(end, EDGES_OWN - step, 1)
        end = jnp.minimum(end, jnp.where(lane8 + step < EDGES_OWN, shifted, EDGES_OWN))
        step *= 2
    start = jnp.where(live, start, lane8)
    end = jnp.where(live, end, lane8)
    rows_ref[...] = jnp.where(
        sub == 0, tgt8, jnp.where(sub == 1, start, jnp.where(sub == 2, end, lane8))
    )
    bound_ref[0, 2 * EDGE_CHUNKS] = jnp.max(end - start) + 1
    for c in range(EDGE_CHUNKS):
        piece = tgt8[:, c * CHUNK : (c + 1) * CHUNK]
        bound_ref[0, 2 * c] = jnp.min(piece)
        bound_ref[0, 2 * c + 1] = jnp.max(jnp.where(piece < NODES_OWN, piece, -1))
    for k in range(NODE_CHUNKS):
        hit = jnp.where(iota((CHUNK, EDGES_OWN), 0) + k * CHUNK == tgt_s, 1.0, 0.0)
        found = jnp.max(hit, axis=1, keepdims=True)
        noedge_ref[k * CHUNK : (k + 1) * CHUNK, :] = jnp.broadcast_to(1.0 - found, (CHUNK, 8))


def own_kernel(
    layer, total_nodes, with_norm, *refs,
):
    if with_norm:
        (state_ref, stats_ref, gain_ref, shift_ref, wl_ref, wr_ref, ws_ref, attn_ref, cols_ref,
         left_ref, base_ref, src_out, dst_out, self_out, right_ref) = refs
        terms = norm_terms(
            stats_ref[...],
            total_nodes,
            gain_ref[layer - 1 : layer, :].astype(F32),
            shift_ref[layer - 1 : layer, :].astype(F32),
        )
    else:
        (state_ref, wl_ref, wr_ref, ws_ref, attn_ref, cols_ref,
         left_ref, base_ref, src_out, dst_out, self_out, right_ref) = refs
    heads = head_rows(attn_ref, layer)
    self_parts = []
    for k in range(NODE_CHUNKS):
        at = slice(k * CHUNK, (k + 1) * CHUNK)
        states = state_ref[at, :]
        if with_norm:
            states = normalize(states, terms)
        left = dot(states, wl_ref[layer]).astype(BF16)
        right = dot(states, wr_ref[layer]).astype(BF16)
        left_ref[at, :] = left
        right_ref[at, :] = right
        base_ref[at, :] = states.astype(F32) + dot(states, ws_ref[layer])
        self_parts.append(scores_of(heads, leaky(left.astype(F32) + right.astype(F32))))
    own = jnp.concatenate(self_parts, axis=1)
    high, mid, low = split_three(own)
    own32 = jnp.concatenate(
        [high.astype(F32), mid.astype(F32), low.astype(F32), jnp.zeros_like(own)], axis=0
    ).astype(BF16)

    def step(c, carry):
        at = pl.ds(pl.multiple_of(c * CHUNK, CHUNK), CHUNK)
        node_ids = iota((CHUNK, NODES_OWN), 1)
        hot = one_hot(cols_ref[at, 1:2] == node_ids)
        dst_out[at, :] = dot(hot, right_ref[...]).astype(BF16)
        back = dot_t(own32, hot)
        self_out[:, at] = back[0:8] + back[8:16] + back[16:24]
        hot = one_hot(cols_ref[at, 0:1] == node_ids)
        src_out[at, :] = dot(hot, left_ref[...]).astype(BF16)
        return carry

    lax.fori_loop(0, EDGE_CHUNKS, step, 0)


def scan_both(ref, bound, lane, start, end, join, neutral):
    ref[0] = ref[2]
    ref[1] = ref[2]
    step = 1
    while step < EDGES_OWN:

        def advance(step=step):
            ahead = ref[0]
            back = ref[1]
            moved = pltpu.roll(ahead, step, 1)
            ref[0] = join(ahead, jnp.where(lane - step >= start, moved, neutral))
            moved = pltpu.roll(back, EDGES_OWN - step, 1)
            ref[1] = join(back, jnp.where(lane + step <= end, moved, neutral))

        pl.when(bound > step)(advance)
        step *= 2
    return ref[0], ref[1]


def edge_kernel(layer, total_nodes, with_norm, with_send, *refs):
    refs = list(refs)
    recv_ref, wl_ref, attn_ref, src_in, dst_in, self_ref, rows_ref, cols_ref, bias_ref = refs[:9]
    noedge_ref, bound_ref, left_ref, base_ref = refs[9:13]
    refs = refs[13:]
    if with_norm:
        stats_in, gain_ref, shift_ref = refs[:3]
        refs = refs[3:]
    if with_send:
        list_ref = refs.pop(0)
    summed_ref, stats_ref = refs[:2]
    refs = refs[2:]
    if with_send:
        send_ref = refs.pop(0)
    table_ref, edge_ref, score_ref, scan_ref, mix_ref, acc_ref = refs[:6]
    refs = refs[6:]
    if with_send:
        round_ref, col_ref = refs
    if with_norm:
        terms = norm_terms(
            stats_in[...],
            total_nodes,
            gain_ref[layer - 1 : layer, :].astype(F32),
            shift_ref[layer - 1 : layer, :].astype(F32),
        )
    heads = head_rows(attn_ref, layer)

    def fill(c, carry):
        at = pl.ds(pl.multiple_of(c * CHUNK, CHUNK), CHUNK)
        states = recv_ref[at, :]
        if with_norm:
            states = normalize(states.astype(F32), terms)
        table_ref[at, :] = dot(states, wl_ref[layer]).astype(BF16)
        return carry

    lax.fori_loop(0, ROWS_IN // CHUNK, fill, 0)

    def score(c, carry):
        at = pl.ds(pl.multiple_of(c * CHUNK, CHUNK), CHUNK)
        hot = one_hot(cols_ref[at, 0:1] - NODES_OWN == iota((CHUNK, ROWS_IN), 1))
        src = dot(hot, table_ref[...]) + src_in[at, :].astype(F32)
        edge_ref[at, :] = src.astype(BF16)
        score_ref[:, at] = scores_of(heads, leaky(src + dst_in[at, :].astype(F32)))
        return carry

    lax.fori_loop(0, EDGE_CHUNKS, score, 0)

    tgt = rows_ref[0:1, :]
    start = rows_ref[1:2, :]
    end = rows_ref[2:3, :]
    lane = iota((8, EDGES_OWN), 1)
    live = tgt < NODES_OWN
    longest = bound_ref[0, 2 * EDGE_CHUNKS]
    scores = jnp.where(live, score_ref[...] + bias_ref[...], -1e30)
    own = self_ref[...]
    scan_ref[2] = scores
    ahead, back = scan_both(scan_ref, longest, lane, start, end, jnp.maximum, -1e30)
    top = jnp.maximum(jnp.maximum(ahead, back), own)
    weights = jnp.where(live, jnp.exp(scores - top), 0.0)
    own_weights = jnp.exp(own - top)
    scan_ref[2] = weights
    ahead, back = scan_both(scan_ref, longest, lane, start, end, jnp.add, 0.0)
    denom = own_weights + (ahead + (back - weights))
    score_ref[...] = weights / denom
    last = live & (lane == end)
    scan_ref[0] = jnp.where(last, own_weights / denom, 0.0)
    spread = head_spread()

    def mix(c, carry):
        at = pl.ds(pl.multiple_of(c * CHUNK, CHUNK), CHUNK)
        pair = jnp.concatenate([score_ref[:, at], scan_ref[0, :, at]], axis=0)
        wide = dot(jnp.transpose(pair).astype(BF16), spread)
        mix_ref[at, :FEAT] = (wide[:, :FEAT] * edge_ref[at, :].astype(F32)).astype(BF16)
        mix_ref[at, FEAT:] = wide[:, FEAT:].astype(BF16)
        return carry

    lax.fori_loop(0, EDGE_CHUNKS, mix, 0)
    stats_ref[...] = jnp.zeros_like(stats_ref)
    for k in range(NODE_CHUNKS):
        at = slice(k * CHUNK, (k + 1) * CHUNK)
        acc_ref[...] = jnp.zeros_like(acc_ref)

        def gather_in(c, carry, k=k):
            near = (bound_ref[0, 2 * c] < (k + 1) * CHUNK) & (
                bound_ref[0, 2 * c + 1] >= k * CHUNK
            )

            def add():
                here = pl.ds(pl.multiple_of(c * CHUNK, CHUNK), CHUNK)
                hot = one_hot(iota((CHUNK, CHUNK), 0) + k * CHUNK == rows_ref[0:1, here])
                acc_ref[...] += dot(hot, mix_ref[here, :])

            pl.when(near)(add)
            return carry

        lax.fori_loop(0, EDGE_CHUNKS, gather_in, 0)
        own_alpha = jnp.where(noedge_ref[at, 0:1] > 0, 1.0, acc_ref[:, FEAT:])
        message = acc_ref[:, :FEAT] + own_alpha * left_ref[at, :].astype(F32)
        summed = base_ref[at, :] + message
        summed_ref[at, :] = summed
        stats_ref[0:1, :] += jnp.sum(summed, axis=0, keepdims=True)
        stats_ref[1:2, :] += jnp.sum(summed * summed, axis=0, keepdims=True)
        if with_send:
            round_ref[at, :] = summed.astype(BF16)
    if with_send:
        pick_rows(list_ref, round_ref, send_ref, col_ref)


def norm_kernel(layer, total_nodes, summed_ref, stats_ref, gain_ref, shift_ref, out_ref):
    terms = norm_terms(
        stats_ref[...],
        total_nodes,
        gain_ref[layer : layer + 1, :].astype(F32),
        shift_ref[layer : layer + 1, :].astype(F32),
    )
    out_ref[...] = normalize(summed_ref[...], terms)


def shaped(rows, cols, dtype):
    return jax.ShapeDtypeStruct((rows, cols), dtype)


SMEM = pl.BlockSpec(memory_space=pltpu.SMEM)
VMEM = pl.BlockSpec(memory_space=pltpu.VMEM)


def call(body, name, outs, scratch, flops, args, in_specs=None, out_specs=None):
    cost = pl.CostEstimate(flops=flops, bytes_accessed=4 << 20, transcendentals=0)
    return pl.pallas_call(
        body,
        name=name,
        out_shape=outs,
        in_specs=in_specs or [VMEM] * len(args),
        out_specs=out_specs or [VMEM] * len(outs),
        scratch_shapes=scratch,
        cost_estimate=cost,
    )(*args)


GIGA = 1 << 30


def send_rows(send_list, table):
    return call(
        send_kernel,
        "send_rows",
        [shaped(ROWS_IN, FEAT, BF16)],
        [pltpu.VMEM((ROWS_IN, 8), jnp.int32)],
        GIGA,
        [send_list, table],
    )[0]


def sort_edges(sources, targets, valids, bias):
    return call(
        sort_kernel,
        "sort_edges",
        [
            shaped(8, EDGES_OWN, jnp.int32),
            shaped(EDGES_OWN, 8, jnp.int32),
            shaped(8, EDGES_OWN, F32),
            shaped(NODES_OWN, 8, F32),
            shaped(1, 32, jnp.int32),
        ],
        [
            pltpu.VMEM((EDGES_OWN, 8), jnp.int32),
            pltpu.VMEM((1, EDGES_OWN), F32),
            pltpu.VMEM((32, EDGES_OWN), F32),
        ],
        2 * GIGA,
        [sources, targets, valids, bias],
        out_specs=[VMEM, VMEM, VMEM, VMEM, SMEM],
    )


def own_part(layer, total_nodes, args):
    with_norm = layer > 0
    return call(
        functools.partial(own_kernel, layer, total_nodes, with_norm),
        "own_part",
        [
            shaped(NODES_OWN, FEAT, BF16),
            shaped(NODES_OWN, FEAT, F32),
            shaped(EDGES_OWN, FEAT, BF16),
            shaped(EDGES_OWN, FEAT, BF16),
            shaped(8, EDGES_OWN, F32),
        ],
        [pltpu.VMEM((NODES_OWN, FEAT), BF16)],
        3 * GIGA,
        args,
    )


def edge_part(layer, total_nodes, with_send, args):
    with_norm = layer > 0
    outs = [shaped(NODES_OWN, FEAT, F32), shaped(2, FEAT, F32)]
    scratch = [
        pltpu.VMEM((ROWS_IN, FEAT), BF16),
        pltpu.VMEM((EDGES_OWN, FEAT), BF16),
        pltpu.VMEM((8, EDGES_OWN), F32),
        pltpu.VMEM((3, 8, EDGES_OWN), F32),
        pltpu.VMEM((EDGES_OWN, 2 * FEAT), BF16),
        pltpu.VMEM((CHUNK, 2 * FEAT), F32),
    ]
    if with_send:
        outs.append(shaped(ROWS_IN, FEAT, BF16))
        scratch += [pltpu.VMEM((NODES_OWN, FEAT), BF16), pltpu.VMEM((ROWS_IN, 8), jnp.int32)]
    in_specs = [VMEM] * len(args)
    in_specs[10] = SMEM
    return call(
        functools.partial(edge_kernel, layer, total_nodes, with_norm, with_send),
        "edge_part",
        outs,
        scratch,
        5 * GIGA,
        args,
        in_specs=in_specs,
    )


def deliver(rows):
    return lax.all_to_all(
        rows.reshape(-1, 8, rows.shape[1]), GRP_BLK, split_axis=0, concat_axis=0, tiled=True
    ).reshape(rows.shape)


def shifted(value, axis, amount):
    size = lax.axis_size(axis)
    return lax.ppermute(value, axis, [(i, (i + amount) % size) for i in range(size)])


def total_inside(stats):
    stats = stats + shifted(stats, "blk_2", 1)
    for axis in ("blk_1", "grp"):
        stats = stats + (
            shifted(stats, axis, 1) + shifted(stats, axis, 2) + shifted(stats, axis, 3)
        )
    stats = stats + (
        shifted(stats, "blk_0", 2) + shifted(stats, "blk_0", 4) + shifted(stats, "blk_0", 6)
    )
    return stats + shifted(stats, "blk_0", 1)


def total_alone(stats):
    for axes in (("blk_1", "blk_2"), ("grp", "blk_0")):
        size = lax.axis_size(axes)
        copies = jnp.broadcast_to(stats[None], (size,) + stats.shape)
        stats = jnp.sum(lax.all_to_all(copies, axes, 0, 0, tiled=True), axis=0)
    return stats


def local(
    features,
    source_index,
    target_index,
    edge_valid,
    edge_bias,
    send_list,
    w_left,
    w_right,
    w_skip,
    attn_vec,
    norm_gain,
    norm_shift,
    peers,
):
    total_nodes = float(features.shape[0] * peers)
    row = (1, EDGES_OWN)
    sent = send_rows(send_list, features)
    received = deliver(sent)
    rows, cols, bias, noedge, bound = sort_edges(
        source_index.reshape(row), target_index.reshape(row), edge_valid.reshape(row), edge_bias
    )
    weights = [w_left, w_right, w_skip, attn_vec, cols]
    left, base, src, dst, own = own_part(0, total_nodes, [features] + weights)
    tail = [rows, cols, bias, noedge, bound]
    summed, stats, sent = edge_part(
        0,
        total_nodes,
        True,
        [received, w_left, attn_vec, src, dst, own] + tail + [left, base, send_list],
    )
    received = deliver(sent)
    stats = total_inside(stats)
    norms = [stats, norm_gain, norm_shift]
    left, base, src, dst, own = own_part(1, total_nodes, [summed] + norms + weights)
    summed, stats = edge_part(
        1,
        total_nodes,
        False,
        [received, w_left, attn_vec, src, dst, own] + tail + [left, base] + norms,
    )
    stats = total_alone(stats)
    return call(
        functools.partial(norm_kernel, 1, total_nodes),
        "norm_out",
        [shaped(NODES_OWN, FEAT, BF16)],
        [],
        1 << 20,
        [summed, stats, norm_gain, norm_shift],
    )[0]


def solution(mesh):
    split = Mesh(
        mesh.devices.reshape(mesh.shape["grp"], 8, 4, 2), ("grp", "blk_0", "blk_1", "blk_2")
    )
    edge = P(GRP_BLK, None)
    in_specs = (edge,) * 4 + (P(None, GRP_BLK), edge) + (P(),) * 6
    return jax.shard_map(
        functools.partial(local, peers=mesh.size),
        mesh=split,
        in_specs=in_specs,
        out_specs=edge,
        check_vma=False,
    )
```

```python
import functools

import jax
import jax.numpy as jnp
from jax import lax
from jax.experimental import pallas as pl
from jax.experimental.pallas import tpu as pltpu
from jax.sharding import Mesh
from jax.sharding import PartitionSpec as P

HEADS = 8
LAYERS = 2
GRP_BLK = ("grp", "blk_0", "blk_1", "blk_2")
NODES_OWN = 1024
EDGES_OWN = 2048
ROWS_IN = 2048
FEAT = 256
CHUNK = 256
EDGE_CHUNKS = EDGES_OWN // CHUNK
NODE_CHUNKS = NODES_OWN // CHUNK
WINDOW = 160
TABLE_ROWS = NODES_OWN + ROWS_IN
F32 = jnp.float32
BF16 = jnp.bfloat16


def iota(shape, dim):
    return lax.broadcasted_iota(jnp.int32, shape, dim)


def one_hot(mask):
    return jnp.where(mask, 1.0, 0.0).astype(BF16)


def dot(lhs, rhs):
    return jnp.dot(lhs, rhs, preferred_element_type=F32)


def dot_t(lhs, rhs):
    return lax.dot_general(lhs, rhs, (((1,), (1,)), ((), ())), preferred_element_type=F32)


def leaky(values):
    return jnp.where(values > 0, values, 0.2 * values)


def split_two(values):
    high = values.astype(BF16)
    return high, (values - high.astype(F32)).astype(BF16)


def split_three(values):
    high = values.astype(BF16)
    rest = values - high.astype(F32)
    mid = rest.astype(BF16)
    return high, mid, (rest - mid.astype(F32)).astype(BF16)


def head_rows(attn_ref, layer):
    shape = (16, FEAT)
    owner = iota(shape, 1) // (FEAT // HEADS) == iota(shape, 0)
    row = attn_ref[layer : layer + 1, :].astype(F32)
    return jnp.where(owner, row, 0.0).astype(BF16)


def head_spread():
    shape = (16, 2 * FEAT)
    return one_hot(iota(shape, 1) // (FEAT // HEADS) == iota(shape, 0))


def scores_of(heads, hidden):
    high, low = split_two(hidden)
    return (dot_t(heads, high) + dot_t(heads, low))[:HEADS]


def norm_terms(stats, total_nodes, gain, shift):
    mean = stats[0:1, :] / total_nodes
    spread = jnp.maximum(stats[1:2, :] / total_nodes - mean * mean, 0.0)
    return mean, lax.rsqrt(spread + 0.1), gain, shift


def normalize(values, terms):
    mean, inv, gain, shift = terms
    scaled = (values - mean) * inv * gain + shift
    grown = jnp.exp(jnp.minimum(scaled, 0.0)) - 1.0
    return jnp.where(scaled > 0, scaled, grown).astype(BF16)


def columns_of(row):
    return jnp.transpose(jnp.broadcast_to(row, (8, row.shape[1])))


def pick_rows(list_ref, table_ref, out_ref, col_ref):
    col_ref[...] = columns_of(list_ref[...].astype(F32)).astype(jnp.int32)

    def step(c, carry):
        at = pl.ds(pl.multiple_of(c * CHUNK, CHUNK), CHUNK)
        hot = one_hot(col_ref[at, 0:1] == iota((CHUNK, NODES_OWN), 1))
        out_ref[at, :] = dot(hot, table_ref[...]).astype(BF16)
        return carry

    lax.fori_loop(0, ROWS_IN // CHUNK, step, 0)


def send_kernel(list_ref, table_ref, out_ref, col_ref):
    pick_rows(list_ref, table_ref, out_ref, col_ref)


def sort_kernel(
    src_ref, tgt_ref, valid_ref, bias_ref, rows_ref, srcs_ref, bias_out, noedge_ref, bound_ref,
    key_ref, pos_ref, meta_ref,
):
    width = (1, EDGES_OWN)
    live_in = valid_ref[...] > 0
    src = src_ref[...]
    tgt = jnp.where(live_in, tgt_ref[...], NODES_OWN)
    key = tgt * EDGES_OWN + iota(width, 1)
    key_ref[...] = columns_of(key.astype(F32)).astype(jnp.int32)
    pos_ref[...] = jnp.zeros_like(pos_ref)

    def rank(c, carry):
        at = pl.ds(pl.multiple_of(c * CHUNK, CHUNK), CHUNK)
        less = jnp.where(key_ref[at, 0:1] < key, 1.0, 0.0)
        pos_ref[...] += jnp.sum(less, axis=0, keepdims=True)
        return carry

    lax.fori_loop(0, EDGE_CHUNKS, rank, 0)
    pos = pos_ref[...].astype(jnp.int32)
    sub = iota((8, EDGES_OWN), 0)
    ints = jnp.where(
        sub == 0,
        src // 256,
        jnp.where(sub == 1, src % 256, jnp.where(sub == 2, tgt // 256, tgt % 256)),
    )
    high, mid, low = split_three(bias_ref[...])
    meta = jnp.concatenate(
        [ints.astype(F32), high.astype(F32), mid.astype(F32), low.astype(F32)], axis=0
    ).astype(BF16)

    def place(c, carry):
        at = pl.ds(pl.multiple_of(c * CHUNK, CHUNK), CHUNK)
        perm = one_hot(pos == iota((CHUNK, EDGES_OWN), 0) + c * CHUNK)
        meta_ref[:, at] = dot_t(meta, perm)
        return carry

    lax.fori_loop(0, EDGE_CHUNKS, place, 0)
    placed = meta_ref[...]
    bias_out[...] = placed[8:16] + placed[16:24] + placed[24:32]
    src_s = (placed[0:1] * 256.0 + placed[1:2]).astype(jnp.int32)
    tgt_s = (placed[2:3] * 256.0 + placed[3:4]).astype(jnp.int32)
    lane8 = iota((8, EDGES_OWN), 1)
    srcs_ref[...] = src_s
    tgt8 = jnp.broadcast_to(tgt_s, (8, EDGES_OWN))
    before = pltpu.roll(tgt8, 1, 1)
    after = pltpu.roll(tgt8, EDGES_OWN - 1, 1)
    live = tgt8 < NODES_OWN
    first = (lane8 == 0) | (before != tgt8)
    last = (lane8 == EDGES_OWN - 1) | (after != tgt8)
    start = jnp.where(first, lane8, 0)
    end = jnp.where(last, lane8, EDGES_OWN)
    step = 1
    while step < EDGES_OWN:
        start = jnp.maximum(start, jnp.where(lane8 >= step, pltpu.roll(start, step, 1), 0))
        shifted = pltpu.roll(end, EDGES_OWN - step, 1)
        end = jnp.minimum(end, jnp.where(lane8 + step < EDGES_OWN, shifted, EDGES_OWN))
        step *= 2
    start = jnp.where(live, start, lane8)
    end = jnp.where(live, end, lane8)
    rows_ref[...] = jnp.where(
        sub == 0, tgt8, jnp.where(sub == 1, start, jnp.where(sub == 2, end, lane8))
    )
    bound_ref[0, 2 * EDGE_CHUNKS] = jnp.max(end - start) + 1
    for c in range(EDGE_CHUNKS):
        piece = tgt8[:, c * CHUNK : (c + 1) * CHUNK]
        bound_ref[0, 2 * c] = jnp.min(piece)
        bound_ref[0, 2 * c + 1] = jnp.max(jnp.where(piece < NODES_OWN, piece, -1))
    for k in range(NODE_CHUNKS):
        hit = jnp.where(iota((CHUNK, EDGES_OWN), 0) + k * CHUNK == tgt_s, 1.0, 0.0)
        found = jnp.max(hit, axis=1, keepdims=True)
        noedge_ref[k * CHUNK : (k + 1) * CHUNK, :] = jnp.broadcast_to(1.0 - found, (CHUNK, 8))


def own_kernel(layer, total_nodes, with_norm, *refs):
    refs = list(refs)
    state_ref = refs.pop(0)
    if with_norm:
        stats_ref, gain_ref, shift_ref = refs[:3]
        refs = refs[3:]
        terms = norm_terms(
            stats_ref[...],
            total_nodes,
            gain_ref[layer - 1 : layer, :].astype(F32),
            shift_ref[layer - 1 : layer, :].astype(F32),
        )
    wl_ref, wr_ref, ws_ref, attn_ref, rows_ref, bound_ref = refs[:6]
    left_ref, base_ref, dst_out, self_out, table_ref, acc_ref = refs[6:]
    heads = head_rows(attn_ref, layer)
    for k in range(NODE_CHUNKS):
        at = slice(k * CHUNK, (k + 1) * CHUNK)
        states = state_ref[at, :]
        if with_norm:
            states = normalize(states, terms)
        left = dot(states, wl_ref[layer]).astype(BF16)
        right = dot(states, wr_ref[layer]).astype(BF16)
        left_ref[at, :] = left
        table_ref[at, :FEAT] = right
        base_ref[at, :] = states.astype(F32) + dot(states, ws_ref[layer])
        own = scores_of(heads, leaky(left.astype(F32) + right.astype(F32)))
        high, mid, low = split_three(own)
        parts = [high.astype(F32), mid.astype(F32), low.astype(F32)]
        parts += [jnp.zeros((128 - 3 * HEADS, CHUNK), F32)]
        table_ref[at, FEAT:] = jnp.transpose(jnp.concatenate(parts, axis=0)).astype(BF16)
    table_ref[NODES_OWN:, :] = jnp.zeros((CHUNK, FEAT + 128), BF16)

    def step(c, carry):
        at = pl.ds(pl.multiple_of(c * CHUNK, CHUNK), CHUNK)
        col = columns_of(rows_ref[0:1, at].astype(F32)).astype(jnp.int32)[:, 0:1]
        low = lax.div(bound_ref[0, 2 * c], 16) * 16
        extra = lax.div(jnp.maximum(bound_ref[0, 2 * c + 1] - low, 0), CHUNK)

        def window(w):
            base = pl.multiple_of(jnp.minimum(low + w * CHUNK, NODES_OWN), 16)
            hot = one_hot(col - base == iota((CHUNK, CHUNK), 1))
            return dot(hot, table_ref[pl.ds(base, CHUNK), :])

        acc_ref[...] = window(0)

        def more(w, carry):
            acc_ref[...] += window(w)
            return carry

        lax.fori_loop(1, extra + 1, more, 0)
        dst_out[at, :] = acc_ref[:, :FEAT].astype(BF16)
        back = jnp.transpose(acc_ref[:, FEAT:])
        self_out[:, at] = back[0:8] + back[8:16] + back[16:24]
        return carry

    lax.fori_loop(0, EDGE_CHUNKS, step, 0, unroll=2)


def scan_both(ref, longest, lane, start, end, join, neutral, values):
    def advance(ahead, back, step):
        moved = pltpu.roll(ahead, step, 1)
        ahead = join(ahead, jnp.where(lane - step >= start, moved, neutral))
        moved = pltpu.roll(back, EDGES_OWN - step, 1)
        return ahead, join(back, jnp.where(lane + step <= end, moved, neutral))

    ahead, back = values, values
    for step in (1, 2, 4, 8):
        ahead, back = advance(ahead, back, step)
    ref[0] = ahead
    ref[1] = back

    def rest():
        step = 16
        while step < EDGES_OWN:
            ref[0], ref[1] = advance(ref[0], ref[1], step)
            step *= 2

    pl.when(longest > 16)(rest)
    return ref[0], ref[1]


def edge_kernel(layer, total_nodes, with_norm, with_send, *refs):
    refs = list(refs)
    recv_any, left_any, dst_any, noedge_any, base_any = refs[:5]
    wl_ref, attn_ref, self_ref, rows_ref, srcs_ref, bias_ref, bound_ref = refs[5:12]
    refs = refs[12:]
    if with_norm:
        stats_in, gain_ref, shift_ref = refs[:3]
        refs = refs[3:]
    if with_send:
        list_ref = refs.pop(0)
    summed_ref, stats_ref = refs[:2]
    refs = refs[2:]
    if with_send:
        send_ref = refs.pop(0)
    recv_ref, left_ref, dst_ref, noedge_ref, base_ref, sems = refs[:6]
    table_ref, even_ref, odd_ref, edge_ref, score_ref, scan_ref, mix_ref, acc_ref = refs[6:14]
    refs = refs[14:]
    if with_send:
        round_ref, col_ref = refs
    copies = [
        pltpu.make_async_copy(source, target, sems.at[i])
        for i, (source, target) in enumerate(
            (
                (left_any, left_ref),
                (recv_any, recv_ref),
                (dst_any, dst_ref),
                (noedge_any, noedge_ref),
                (base_any, base_ref),
            )
        )
    ]
    for copy in copies:
        copy.start()
    if with_norm:
        terms = norm_terms(
            stats_in[...],
            total_nodes,
            gain_ref[layer - 1 : layer, :].astype(F32),
            shift_ref[layer - 1 : layer, :].astype(F32),
        )
    heads = head_rows(attn_ref, layer)
    half = FEAT // 2

    def put_rows(first, values):
        table_ref[pl.ds(2 * first, CHUNK, stride=2), :] = values[:, :half]
        table_ref[pl.ds(2 * first + 1, CHUNK, stride=2), :] = values[:, half:]

    copies[0].wait()
    for k in range(NODE_CHUNKS):
        put_rows(k * CHUNK, left_ref[k * CHUNK : (k + 1) * CHUNK, :].astype(F32))
    copies[1].wait()

    def fill(c, carry):
        at = pl.ds(pl.multiple_of(c * CHUNK, CHUNK), CHUNK)
        states = recv_ref[at, :]
        if with_norm:
            states = normalize(states.astype(F32), terms)
        left = dot(states, wl_ref[layer]).astype(BF16).astype(F32)
        put_rows(pl.multiple_of(NODES_OWN + c * CHUNK, CHUNK), left)
        return carry

    lax.fori_loop(0, ROWS_IN // CHUNK, fill, 0, unroll=2)

    def fetch(c, out_ref):
        first = c * CHUNK
        for e in range(CHUNK):
            row = srcs_ref[0, first + e]
            out_ref[2 * e : 2 * e + 2, :] = table_ref[pl.ds(pl.multiple_of(2 * row, 2), 2), :]

    def score(c, in_ref):
        at = pl.ds(pl.multiple_of(c * CHUNK, CHUNK), CHUNK)
        src = jnp.concatenate(
            [in_ref[pl.ds(0, CHUNK, stride=2), :], in_ref[pl.ds(1, CHUNK, stride=2), :]], axis=1
        )
        edge_ref[at, :] = src.astype(BF16)
        score_ref[:, at] = scores_of(heads, leaky(src + dst_ref[at, :].astype(F32)))

    fetch(0, even_ref)
    copies[2].wait()

    def pair(c, carry):
        fetch(2 * c + 1, odd_ref)
        score(2 * c, even_ref)
        fetch(lax.rem(2 * c + 2, EDGE_CHUNKS), even_ref)
        score(2 * c + 1, odd_ref)
        return carry

    lax.fori_loop(0, EDGE_CHUNKS // 2, pair, 0)

    tgt = rows_ref[0:1, :]
    start = rows_ref[1:2, :]
    end = rows_ref[2:3, :]
    lane = iota((8, EDGES_OWN), 1)
    live = tgt < NODES_OWN
    longest = bound_ref[0, 2 * EDGE_CHUNKS]
    scores = jnp.where(live, score_ref[...] + bias_ref[...], -1e30)
    own = self_ref[...]
    ahead, back = scan_both(scan_ref, longest, lane, start, end, jnp.maximum, -1e30, scores)
    top = jnp.maximum(jnp.maximum(ahead, back), own)
    weights = jnp.where(live, jnp.exp(scores - top), 0.0)
    own_weights = jnp.exp(own - top)
    ahead, back = scan_both(scan_ref, longest, lane, start, end, jnp.add, 0.0, weights)
    denom = own_weights + (ahead + (back - weights))
    last = live & (lane == end)
    score_ref[...] = weights / denom
    scan_ref[0] = jnp.where(last, own_weights / denom, 0.0)
    spread = head_spread()

    def mix(c, carry):
        at = pl.ds(pl.multiple_of(c * CHUNK, CHUNK), CHUNK)
        pair = jnp.concatenate([score_ref[:, at], scan_ref[0, :, at]], axis=0)
        wide = dot(jnp.transpose(pair).astype(BF16), spread)
        mix_ref[at, :FEAT] = (wide[:, :FEAT] * edge_ref[at, :].astype(F32)).astype(BF16)
        mix_ref[at, FEAT:] = wide[:, FEAT:].astype(BF16)
        return carry

    lax.fori_loop(0, EDGE_CHUNKS, mix, 0, unroll=4)
    acc_ref[...] = jnp.zeros_like(acc_ref)

    def gather_in(c, carry):
        here = pl.ds(pl.multiple_of(c * CHUNK, CHUNK), CHUNK)
        low = lax.div(bound_ref[0, 2 * c], 8) * 8
        count = lax.div(jnp.maximum(bound_ref[0, 2 * c + 1] - low + WINDOW, 0), WINDOW)

        def window(w, carry):
            first = pl.multiple_of(low + w * WINDOW, 8)
            hot = one_hot(iota((WINDOW, CHUNK), 0) + first == rows_ref[0:1, here])
            acc_ref[pl.ds(first, WINDOW), :] += dot(hot, mix_ref[here, :])
            return carry

        return lax.fori_loop(0, count, window, carry)

    lax.fori_loop(0, EDGE_CHUNKS, gather_in, 0)
    copies[3].wait()
    copies[4].wait()
    stats_ref[...] = jnp.zeros_like(stats_ref)
    for k in range(NODE_CHUNKS):
        at = slice(k * CHUNK, (k + 1) * CHUNK)
        own_alpha = jnp.where(noedge_ref[at, 0:1] > 0, 1.0, acc_ref[at, FEAT:])
        message = acc_ref[at, :FEAT] + own_alpha * left_ref[at, :].astype(F32)
        summed = base_ref[at, :] + message
        summed_ref[at, :] = summed
        stats_ref[0:1, :] += jnp.sum(summed, axis=0, keepdims=True)
        stats_ref[1:2, :] += jnp.sum(summed * summed, axis=0, keepdims=True)
        if with_send:
            round_ref[at, :] = summed.astype(BF16)
    if with_send:
        pick_rows(list_ref, round_ref, send_ref, col_ref)


def norm_kernel(layer, total_nodes, summed_ref, stats_ref, gain_ref, shift_ref, out_ref):
    terms = norm_terms(
        stats_ref[...],
        total_nodes,
        gain_ref[layer : layer + 1, :].astype(F32),
        shift_ref[layer : layer + 1, :].astype(F32),
    )
    out_ref[...] = normalize(summed_ref[...], terms)


def shaped(rows, cols, dtype):
    return jax.ShapeDtypeStruct((rows, cols), dtype)


SMEM = pl.BlockSpec(memory_space=pltpu.SMEM)
VMEM = pl.BlockSpec(memory_space=pltpu.VMEM)
ANY = pl.BlockSpec(memory_space=pl.ANY)


def call(body, name, outs, scratch, flops, args, in_specs=None, out_specs=None):
    cost = pl.CostEstimate(flops=flops, bytes_accessed=4 << 20, transcendentals=0)
    return pl.pallas_call(
        body,
        name=name,
        out_shape=outs,
        in_specs=in_specs or [VMEM] * len(args),
        out_specs=out_specs or [VMEM] * len(outs),
        scratch_shapes=scratch,
        cost_estimate=cost,
        compiler_params=pltpu.CompilerParams(vmem_limit_bytes=24 << 20),
    )(*args)


GIGA = 1 << 30


def send_rows(send_list, table):
    return call(
        send_kernel,
        "send_rows",
        [shaped(ROWS_IN, FEAT, BF16)],
        [pltpu.VMEM((ROWS_IN, 8), jnp.int32)],
        GIGA,
        [send_list, table],
    )[0]


def sort_edges(sources, targets, valids, bias):
    return call(
        sort_kernel,
        "sort_edges",
        [
            shaped(8, EDGES_OWN, jnp.int32),
            shaped(1, EDGES_OWN, jnp.int32),
            shaped(8, EDGES_OWN, F32),
            shaped(NODES_OWN, 8, F32),
            shaped(1, 32, jnp.int32),
        ],
        [
            pltpu.VMEM((EDGES_OWN, 8), jnp.int32),
            pltpu.VMEM((1, EDGES_OWN), F32),
            pltpu.VMEM((32, EDGES_OWN), F32),
        ],
        2 * GIGA,
        [sources, targets, valids, bias],
        out_specs=[VMEM, VMEM, VMEM, VMEM, SMEM],
    )


def own_part(layer, total_nodes, args):
    in_specs = [VMEM] * len(args)
    in_specs[-1] = SMEM
    return call(
        functools.partial(own_kernel, layer, total_nodes, layer > 0),
        "own_part",
        [
            shaped(NODES_OWN, FEAT, BF16),
            shaped(NODES_OWN, FEAT, F32),
            shaped(EDGES_OWN, FEAT, BF16),
            shaped(8, EDGES_OWN, F32),
        ],
        [pltpu.VMEM((NODES_OWN + CHUNK, FEAT + 128), BF16), pltpu.VMEM((CHUNK, FEAT + 128), F32)],
        3 * GIGA,
        args,
        in_specs=in_specs,
    )


def edge_part(layer, total_nodes, with_send, args):
    outs = [shaped(NODES_OWN, FEAT, F32), shaped(2, FEAT, F32)]
    half = FEAT // 2
    scratch = [
        pltpu.VMEM((ROWS_IN, FEAT), BF16),
        pltpu.VMEM((NODES_OWN, FEAT), BF16),
        pltpu.VMEM((EDGES_OWN, FEAT), BF16),
        pltpu.VMEM((NODES_OWN, 8), F32),
        pltpu.VMEM((NODES_OWN, FEAT), F32),
        pltpu.SemaphoreType.DMA((5,)),
        pltpu.VMEM((2 * TABLE_ROWS, half), F32),
        pltpu.VMEM((2 * CHUNK, half), F32),
        pltpu.VMEM((2 * CHUNK, half), F32),
        pltpu.VMEM((EDGES_OWN, FEAT), BF16),
        pltpu.VMEM((8, EDGES_OWN), F32),
        pltpu.VMEM((2, 8, EDGES_OWN), F32),
        pltpu.VMEM((EDGES_OWN, 2 * FEAT), BF16),
        pltpu.VMEM((NODES_OWN + WINDOW, 2 * FEAT), F32),
    ]
    if with_send:
        outs.append(shaped(ROWS_IN, FEAT, BF16))
        scratch += [pltpu.VMEM((NODES_OWN, FEAT), BF16), pltpu.VMEM((ROWS_IN, 8), jnp.int32)]
    in_specs = [ANY] * 5 + [VMEM] * (len(args) - 5)
    in_specs[9] = SMEM
    in_specs[11] = SMEM
    return call(
        functools.partial(edge_kernel, layer, total_nodes, layer > 0, with_send),
        "edge_part",
        outs,
        scratch,
        5 * GIGA,
        args,
        in_specs=in_specs,
    )


def deliver(rows):
    return lax.all_to_all(
        rows.reshape(-1, 8, rows.shape[1]), GRP_BLK, split_axis=0, concat_axis=0, tiled=True
    ).reshape(rows.shape)


def shifted(value, axis, amount):
    size = lax.axis_size(axis)
    return lax.ppermute(value, axis, [(i, (i + amount) % size) for i in range(size)])


def total_inside(stats):
    stats = stats + shifted(stats, "blk_2", 1)
    for axis in ("blk_1", "grp"):
        stats = stats + (
            shifted(stats, axis, 1) + shifted(stats, axis, 2) + shifted(stats, axis, 3)
        )
    stats = stats + (
        shifted(stats, "blk_0", 2) + shifted(stats, "blk_0", 4) + shifted(stats, "blk_0", 6)
    )
    return stats + shifted(stats, "blk_0", 1)


def total_alone(stats):
    for axes in (("blk_1", "blk_2"), ("grp", "blk_0")):
        size = lax.axis_size(axes)
        copies = jnp.broadcast_to(stats[None], (size,) + stats.shape)
        stats = jnp.sum(lax.all_to_all(copies, axes, 0, 0, tiled=True), axis=0)
    return stats


def local(
    features,
    source_index,
    target_index,
    edge_valid,
    edge_bias,
    send_list,
    w_left,
    w_right,
    w_skip,
    attn_vec,
    norm_gain,
    norm_shift,
    peers,
):
    total_nodes = float(features.shape[0] * peers)
    row = (1, EDGES_OWN)
    sent = send_rows(send_list, features)
    received = deliver(sent)
    rows, srcs, bias, noedge, bound = sort_edges(
        source_index.reshape(row), target_index.reshape(row), edge_valid.reshape(row), edge_bias
    )
    weights = [w_left, w_right, w_skip, attn_vec, rows, bound]
    left, base, dst, own = own_part(0, total_nodes, [features] + weights)
    edges = [rows, srcs, bias, bound]
    summed, stats, sent = edge_part(
        0,
        total_nodes,
        True,
        [received, left, dst, noedge, base, w_left, attn_vec, own] + edges + [send_list],
    )
    received = deliver(sent)
    stats = total_inside(stats)
    norms = [stats, norm_gain, norm_shift]
    left, base, dst, own = own_part(1, total_nodes, [summed] + norms + weights)
    summed, stats = edge_part(
        1,
        total_nodes,
        False,
        [received, left, dst, noedge, base, w_left, attn_vec, own] + edges + norms,
    )
    stats = total_alone(stats)
    return call(
        functools.partial(norm_kernel, 1, total_nodes),
        "norm_out",
        [shaped(NODES_OWN, FEAT, BF16)],
        [],
        1 << 20,
        [summed, stats, norm_gain, norm_shift],
    )[0]


def solution(mesh):
    split = Mesh(
        mesh.devices.reshape(mesh.shape["grp"], 8, 4, 2), ("grp", "blk_0", "blk_1", "blk_2")
    )
    edge = P(GRP_BLK, None)
    in_specs = (edge,) * 4 + (P(None, GRP_BLK), edge) + (P(),) * 6
    return jax.shard_map(
        functools.partial(local, peers=mesh.size),
        mesh=split,
        in_specs=in_specs,
        out_specs=edge,
        check_vma=False,
    )
```

```python
import functools

import jax
import jax.numpy as jnp
from jax import lax
from jax.experimental import pallas as pl
from jax.experimental.pallas import tpu as pltpu
from jax.sharding import Mesh
from jax.sharding import PartitionSpec as P

HEADS = 8
LAYERS = 2
GRP_BLK = ("grp", "blk_0", "blk_1", "blk_2")
NODES_OWN = 1024
EDGES_OWN = 2048
ROWS_IN = 2048
FEAT = 256
CHUNK = 256
EDGE_CHUNKS = EDGES_OWN // CHUNK
NODE_CHUNKS = NODES_OWN // CHUNK
WINDOW = 160
TABLE_ROWS = NODES_OWN + ROWS_IN
F32 = jnp.float32
BF16 = jnp.bfloat16


def iota(shape, dim):
    return lax.broadcasted_iota(jnp.int32, shape, dim)


def one_hot(mask):
    return jnp.where(mask, 1.0, 0.0).astype(BF16)


def dot(lhs, rhs):
    return jnp.dot(lhs, rhs, preferred_element_type=F32)


def dot_t(lhs, rhs):
    return lax.dot_general(lhs, rhs, (((1,), (1,)), ((), ())), preferred_element_type=F32)


def leaky(values):
    return jnp.where(values > 0, values, 0.2 * values)


def split_two(values):
    high = values.astype(BF16)
    return high, (values - high.astype(F32)).astype(BF16)


def split_three(values):
    high = values.astype(BF16)
    rest = values - high.astype(F32)
    mid = rest.astype(BF16)
    return high, mid, (rest - mid.astype(F32)).astype(BF16)


def head_rows(attn_ref, layer):
    shape = (16, FEAT)
    owner = iota(shape, 1) // (FEAT // HEADS) == iota(shape, 0)
    row = attn_ref[layer : layer + 1, :].astype(F32)
    return jnp.where(owner, row, 0.0).astype(BF16)


def head_spread():
    shape = (16, 2 * FEAT)
    return one_hot(iota(shape, 1) // (FEAT // HEADS) == iota(shape, 0))


def scores_of(heads, hidden):
    high, low = split_two(hidden)
    return (dot_t(heads, high) + dot_t(heads, low))[:HEADS]


def norm_terms(stats, total_nodes, gain, shift):
    mean = stats[0:1, :] / total_nodes
    spread = jnp.maximum(stats[1:2, :] / total_nodes - mean * mean, 0.0)
    return mean, lax.rsqrt(spread + 0.1), gain, shift


def normalize(values, terms):
    mean, inv, gain, shift = terms
    scaled = (values - mean) * inv * gain + shift
    grown = jnp.exp(jnp.minimum(scaled, 0.0)) - 1.0
    return jnp.where(scaled > 0, scaled, grown).astype(BF16)


def columns_of(row):
    return jnp.transpose(jnp.broadcast_to(row, (8, row.shape[1])))


def pick_rows(list_ref, table_ref, out_ref, col_ref):
    col_ref[...] = columns_of(list_ref[...].astype(F32)).astype(jnp.int32)

    def step(c, carry):
        at = pl.ds(pl.multiple_of(c * CHUNK, CHUNK), CHUNK)
        hot = one_hot(col_ref[at, 0:1] == iota((CHUNK, NODES_OWN), 1))
        out_ref[at, :] = dot(hot, table_ref[...]).astype(BF16)
        return carry

    lax.fori_loop(0, ROWS_IN // CHUNK, step, 0)


def send_kernel(list_ref, table_ref, out_ref, col_ref):
    pick_rows(list_ref, table_ref, out_ref, col_ref)


def sort_kernel(
    src_ref, tgt_ref, valid_ref, bias_ref, rows_ref, srcs_ref, bias_out, noedge_ref, bound_ref,
    key_ref, pos_ref, meta_ref,
):
    width = (1, EDGES_OWN)
    live_in = valid_ref[...] > 0
    src = src_ref[...]
    tgt = jnp.where(live_in, tgt_ref[...], NODES_OWN)
    key = tgt * EDGES_OWN + iota(width, 1)
    key_ref[...] = columns_of(key.astype(F32)).astype(jnp.int32)
    pos_ref[...] = jnp.zeros_like(pos_ref)

    def rank(c, carry):
        at = pl.ds(pl.multiple_of(c * CHUNK, CHUNK), CHUNK)
        less = jnp.where(key_ref[at, 0:1] < key, 1.0, 0.0)
        pos_ref[...] += jnp.sum(less, axis=0, keepdims=True)
        return carry

    lax.fori_loop(0, EDGE_CHUNKS, rank, 0)
    pos = pos_ref[...].astype(jnp.int32)
    sub = iota((8, EDGES_OWN), 0)
    ints = jnp.where(
        sub == 0,
        src // 256,
        jnp.where(sub == 1, src % 256, jnp.where(sub == 2, tgt // 256, tgt % 256)),
    )
    high, mid, low = split_three(bias_ref[...])
    meta = jnp.concatenate(
        [ints.astype(F32), high.astype(F32), mid.astype(F32), low.astype(F32)], axis=0
    ).astype(BF16)

    def place(c, carry):
        at = pl.ds(pl.multiple_of(c * CHUNK, CHUNK), CHUNK)
        perm = one_hot(pos == iota((CHUNK, EDGES_OWN), 0) + c * CHUNK)
        meta_ref[:, at] = dot_t(meta, perm)
        return carry

    lax.fori_loop(0, EDGE_CHUNKS, place, 0)
    placed = meta_ref[...]
    bias_out[...] = placed[8:16] + placed[16:24] + placed[24:32]
    src_s = (placed[0:1] * 256.0 + placed[1:2]).astype(jnp.int32)
    tgt_s = (placed[2:3] * 256.0 + placed[3:4]).astype(jnp.int32)
    lane8 = iota((8, EDGES_OWN), 1)
    srcs_ref[...] = src_s
    tgt8 = jnp.broadcast_to(tgt_s, (8, EDGES_OWN))
    before = pltpu.roll(tgt8, 1, 1)
    after = pltpu.roll(tgt8, EDGES_OWN - 1, 1)
    live = tgt8 < NODES_OWN
    first = (lane8 == 0) | (before != tgt8)
    last = (lane8 == EDGES_OWN - 1) | (after != tgt8)
    start = jnp.where(first, lane8, 0)
    end = jnp.where(last, lane8, EDGES_OWN)
    step = 1
    while step < EDGES_OWN:
        start = jnp.maximum(start, jnp.where(lane8 >= step, pltpu.roll(start, step, 1), 0))
        shifted = pltpu.roll(end, EDGES_OWN - step, 1)
        end = jnp.minimum(end, jnp.where(lane8 + step < EDGES_OWN, shifted, EDGES_OWN))
        step *= 2
    start = jnp.where(live, start, lane8)
    end = jnp.where(live, end, lane8)
    rows_ref[...] = jnp.where(
        sub == 0, tgt8, jnp.where(sub == 1, start, jnp.where(sub == 2, end, lane8))
    )
    bound_ref[0, 2 * EDGE_CHUNKS] = jnp.max(end - start) + 1
    for c in range(EDGE_CHUNKS):
        piece = tgt8[:, c * CHUNK : (c + 1) * CHUNK]
        bound_ref[0, 2 * c] = jnp.min(piece)
        bound_ref[0, 2 * c + 1] = jnp.max(jnp.where(piece < NODES_OWN, piece, -1))
    for k in range(NODE_CHUNKS):
        hit = jnp.where(iota((CHUNK, EDGES_OWN), 0) + k * CHUNK == tgt_s, 1.0, 0.0)
        found = jnp.max(hit, axis=1, keepdims=True)
        noedge_ref[k * CHUNK : (k + 1) * CHUNK, :] = jnp.broadcast_to(1.0 - found, (CHUNK, 8))


def own_kernel(layer, total_nodes, with_norm, *refs):
    refs = list(refs)
    state_ref = refs.pop(0)
    if with_norm:
        stats_ref, gain_ref, shift_ref = refs[:3]
        refs = refs[3:]
        terms = norm_terms(
            stats_ref[...],
            total_nodes,
            gain_ref[layer - 1 : layer, :].astype(F32),
            shift_ref[layer - 1 : layer, :].astype(F32),
        )
    wl_ref, wr_ref, ws_ref, attn_ref, rows_ref, bound_ref = refs[:6]
    left_out, base_out, dst_hbm, self_out = refs[6:10]
    table_ref, acc_ref, own_ref, left_ref, base_ref, dst_out, sems = refs[10:]
    loads = []
    for k in range(NODE_CHUNKS):
        at = slice(k * CHUNK, (k + 1) * CHUNK)
        loads.append(pltpu.make_async_copy(state_ref.at[at], own_ref.at[at], sems.at[k]))
        loads[-1].start()
    stores = [
        pltpu.make_async_copy(left_ref, left_out, sems.at[NODE_CHUNKS]),
        pltpu.make_async_copy(base_ref, base_out, sems.at[NODE_CHUNKS + 1]),
        pltpu.make_async_copy(dst_out, dst_hbm, sems.at[NODE_CHUNKS + 2]),
    ]
    heads = head_rows(attn_ref, layer)
    for k in range(NODE_CHUNKS):
        at = slice(k * CHUNK, (k + 1) * CHUNK)
        loads[k].wait()
        states = own_ref[at, :]
        if with_norm:
            states = normalize(states, terms)
        left = dot(states, wl_ref[layer]).astype(BF16)
        right = dot(states, wr_ref[layer]).astype(BF16)
        left_ref[at, :] = left
        table_ref[at, :FEAT] = right
        base_ref[at, :] = states.astype(F32) + dot(states, ws_ref[layer])
        own = scores_of(heads, leaky(left.astype(F32) + right.astype(F32)))
        high, mid, low = split_three(own)
        parts = [high.astype(F32), mid.astype(F32), low.astype(F32)]
        parts += [jnp.zeros((128 - 3 * HEADS, CHUNK), F32)]
        table_ref[at, FEAT:] = jnp.transpose(jnp.concatenate(parts, axis=0)).astype(BF16)
    table_ref[NODES_OWN:, :] = jnp.zeros((CHUNK, FEAT + 128), BF16)
    stores[0].start()
    stores[1].start()

    def step(c, carry):
        at = pl.ds(pl.multiple_of(c * CHUNK, CHUNK), CHUNK)
        col = columns_of(rows_ref[0:1, at].astype(F32)).astype(jnp.int32)[:, 0:1]
        low = lax.div(bound_ref[0, 2 * c], 16) * 16
        extra = lax.div(jnp.maximum(bound_ref[0, 2 * c + 1] - low, 0), CHUNK)

        def window(w):
            base = pl.multiple_of(jnp.minimum(low + w * CHUNK, NODES_OWN), 16)
            hot = one_hot(col - base == iota((CHUNK, CHUNK), 1))
            return dot(hot, table_ref[pl.ds(base, CHUNK), :])

        acc_ref[...] = window(0)

        def more(w, carry):
            acc_ref[...] += window(w)
            return carry

        lax.fori_loop(1, extra + 1, more, 0)
        dst_out[at, :] = acc_ref[:, :FEAT].astype(BF16)
        back = jnp.transpose(acc_ref[:, FEAT:])
        self_out[:, at] = back[0:8] + back[8:16] + back[16:24]
        return carry

    lax.fori_loop(0, EDGE_CHUNKS, step, 0, unroll=2)
    stores[2].start()
    for store in stores:
        store.wait()


def scan_both(ref, longest, lane, start, end, join, neutral, values):
    def advance(ahead, back, step):
        moved = pltpu.roll(ahead, step, 1)
        ahead = join(ahead, jnp.where(lane - step >= start, moved, neutral))
        moved = pltpu.roll(back, EDGES_OWN - step, 1)
        return ahead, join(back, jnp.where(lane + step <= end, moved, neutral))

    ahead, back = values, values
    for step in (1, 2, 4, 8):
        ahead, back = advance(ahead, back, step)
    ref[0] = ahead
    ref[1] = back

    def rest():
        step = 16
        while step < EDGES_OWN:
            ref[0], ref[1] = advance(ref[0], ref[1], step)
            step *= 2

    pl.when(longest > 16)(rest)
    return ref[0], ref[1]


def edge_kernel(layer, total_nodes, with_norm, with_send, *refs):
    refs = list(refs)
    recv_any, left_any, dst_any, noedge_any, base_any = refs[:5]
    wl_ref, attn_ref, self_ref, rows_ref, srcs_ref, bias_ref, bound_ref = refs[5:12]
    refs = refs[12:]
    if with_norm:
        stats_in, gain_ref, shift_ref = refs[:3]
        refs = refs[3:]
    if with_send:
        summed_hbm, stats_ref, round_ref = refs[:3]
        refs = refs[3:]
        summed_ref, out_sems = refs.pop(), refs.pop()
    else:
        summed_ref, stats_ref = refs[:2]
        refs = refs[2:]
    recv_ref, left_ref, dst_ref, noedge_ref, base_ref, sems = refs[:6]
    table_ref, even_ref, odd_ref, edge_ref, score_ref, scan_ref, mix_ref, acc_ref = refs[6:14]
    copies = [
        pltpu.make_async_copy(source, target, sems.at[i])
        for i, (source, target) in enumerate(
            (
                (left_any, left_ref),
                (recv_any, recv_ref),
                (dst_any, dst_ref),
                (noedge_any, noedge_ref),
                (base_any, base_ref),
            )
        )
    ]
    for copy in copies:
        copy.start()
    if with_norm:
        terms = norm_terms(
            stats_in[...],
            total_nodes,
            gain_ref[layer - 1 : layer, :].astype(F32),
            shift_ref[layer - 1 : layer, :].astype(F32),
        )
    heads = head_rows(attn_ref, layer)
    half = FEAT // 2

    def put_rows(first, values):
        table_ref[pl.ds(2 * first, CHUNK, stride=2), :] = values[:, :half]
        table_ref[pl.ds(2 * first + 1, CHUNK, stride=2), :] = values[:, half:]

    copies[0].wait()
    for k in range(NODE_CHUNKS):
        put_rows(k * CHUNK, left_ref[k * CHUNK : (k + 1) * CHUNK, :].astype(F32))
    copies[1].wait()

    def fill(c, carry):
        at = pl.ds(pl.multiple_of(c * CHUNK, CHUNK), CHUNK)
        states = recv_ref[at, :]
        if with_norm:
            states = normalize(states.astype(F32), terms)
        left = dot(states, wl_ref[layer]).astype(BF16).astype(F32)
        put_rows(pl.multiple_of(NODES_OWN + c * CHUNK, CHUNK), left)
        return carry

    lax.fori_loop(0, ROWS_IN // CHUNK, fill, 0, unroll=2)

    def fetch(c, out_ref):
        first = c * CHUNK
        for e in range(CHUNK):
            row = srcs_ref[0, first + e]
            out_ref[2 * e : 2 * e + 2, :] = table_ref[pl.ds(pl.multiple_of(2 * row, 2), 2), :]

    def score(c, in_ref):
        at = pl.ds(pl.multiple_of(c * CHUNK, CHUNK), CHUNK)
        src = jnp.concatenate(
            [in_ref[pl.ds(0, CHUNK, stride=2), :], in_ref[pl.ds(1, CHUNK, stride=2), :]], axis=1
        )
        edge_ref[at, :] = src.astype(BF16)
        score_ref[:, at] = scores_of(heads, leaky(src + dst_ref[at, :].astype(F32)))

    fetch(0, even_ref)
    copies[2].wait()

    def pair(c, carry):
        fetch(2 * c + 1, odd_ref)
        score(2 * c, even_ref)
        fetch(lax.rem(2 * c + 2, EDGE_CHUNKS), even_ref)
        score(2 * c + 1, odd_ref)
        return carry

    lax.fori_loop(0, EDGE_CHUNKS // 2, pair, 0)

    tgt = rows_ref[0:1, :]
    start = rows_ref[1:2, :]
    end = rows_ref[2:3, :]
    lane = iota((8, EDGES_OWN), 1)
    live = tgt < NODES_OWN
    longest = bound_ref[0, 2 * EDGE_CHUNKS]
    scores = jnp.where(live, score_ref[...] + bias_ref[...], -1e30)
    own = self_ref[...]
    ahead, back = scan_both(scan_ref, longest, lane, start, end, jnp.maximum, -1e30, scores)
    top = jnp.maximum(jnp.maximum(ahead, back), own)
    weights = jnp.where(live, jnp.exp(scores - top), 0.0)
    own_weights = jnp.exp(own - top)
    ahead, back = scan_both(scan_ref, longest, lane, start, end, jnp.add, 0.0, weights)
    denom = own_weights + (ahead + (back - weights))
    last = live & (lane == end)
    score_ref[...] = weights / denom
    scan_ref[0] = jnp.where(last, own_weights / denom, 0.0)
    spread = head_spread()

    def mix(c, carry):
        at = pl.ds(pl.multiple_of(c * CHUNK, CHUNK), CHUNK)
        pair = jnp.concatenate([score_ref[:, at], scan_ref[0, :, at]], axis=0)
        wide = dot(jnp.transpose(pair).astype(BF16), spread)
        mix_ref[at, :FEAT] = (wide[:, :FEAT] * edge_ref[at, :].astype(F32)).astype(BF16)
        mix_ref[at, FEAT:] = wide[:, FEAT:].astype(BF16)
        return carry

    lax.fori_loop(0, EDGE_CHUNKS, mix, 0, unroll=4)
    acc_ref[...] = jnp.zeros_like(acc_ref)

    def gather_in(c, carry):
        here = pl.ds(pl.multiple_of(c * CHUNK, CHUNK), CHUNK)
        low = lax.div(bound_ref[0, 2 * c], 8) * 8
        count = lax.div(jnp.maximum(bound_ref[0, 2 * c + 1] - low + WINDOW, 0), WINDOW)

        def window(w, carry):
            first = pl.multiple_of(low + w * WINDOW, 8)
            hot = one_hot(iota((WINDOW, CHUNK), 0) + first == rows_ref[0:1, here])
            acc_ref[pl.ds(first, WINDOW), :] += dot(hot, mix_ref[here, :])
            return carry

        return lax.fori_loop(0, count, window, carry)

    lax.fori_loop(0, EDGE_CHUNKS, gather_in, 0)
    copies[3].wait()
    copies[4].wait()
    stats_ref[...] = jnp.zeros_like(stats_ref)
    stores = []
    for k in range(NODE_CHUNKS):
        at = slice(k * CHUNK, (k + 1) * CHUNK)
        own_alpha = jnp.where(noedge_ref[at, 0:1] > 0, 1.0, acc_ref[at, FEAT:])
        message = acc_ref[at, :FEAT] + own_alpha * left_ref[at, :].astype(F32)
        summed = base_ref[at, :] + message
        summed_ref[at, :] = summed
        stats_ref[0:1, :] += jnp.sum(summed, axis=0, keepdims=True)
        stats_ref[1:2, :] += jnp.sum(summed * summed, axis=0, keepdims=True)
        if with_send:
            round_ref[at, :] = summed.astype(BF16)
            store = pltpu.make_async_copy(summed_ref.at[at], summed_hbm.at[at], out_sems.at[k])
            store.start()
            stores.append(store)
    for store in stores:
        store.wait()


def norm_kernel(layer, total_nodes, summed_ref, stats_ref, gain_ref, shift_ref, out_ref):
    terms = norm_terms(
        stats_ref[...],
        total_nodes,
        gain_ref[layer : layer + 1, :].astype(F32),
        shift_ref[layer : layer + 1, :].astype(F32),
    )
    out_ref[...] = normalize(summed_ref[...], terms)


def shaped(rows, cols, dtype):
    return jax.ShapeDtypeStruct((rows, cols), dtype)


SMEM = pl.BlockSpec(memory_space=pltpu.SMEM)
VMEM = pl.BlockSpec(memory_space=pltpu.VMEM)
ANY = pl.BlockSpec(memory_space=pl.ANY)
HBM = pl.BlockSpec(memory_space=pltpu.HBM)


def call(body, name, outs, scratch, flops, args, in_specs=None, out_specs=None):
    cost = pl.CostEstimate(flops=flops, bytes_accessed=4 << 20, transcendentals=0)
    return pl.pallas_call(
        body,
        name=name,
        out_shape=outs,
        in_specs=in_specs or [VMEM] * len(args),
        out_specs=out_specs or [VMEM] * len(outs),
        scratch_shapes=scratch,
        cost_estimate=cost,
        compiler_params=pltpu.CompilerParams(vmem_limit_bytes=67_000_000),
    )(*args)


GIGA = 1 << 30


def send_rows(send_list, table):
    return call(
        send_kernel,
        "send_rows",
        [shaped(ROWS_IN, FEAT, BF16)],
        [pltpu.VMEM((ROWS_IN, 8), jnp.int32)],
        GIGA,
        [send_list, table],
    )[0]


def sort_edges(sources, targets, valids, bias):
    return call(
        sort_kernel,
        "sort_edges",
        [
            shaped(8, EDGES_OWN, jnp.int32),
            shaped(1, EDGES_OWN, jnp.int32),
            shaped(8, EDGES_OWN, F32),
            shaped(NODES_OWN, 8, F32),
            shaped(1, 32, jnp.int32),
        ],
        [
            pltpu.VMEM((EDGES_OWN, 8), jnp.int32),
            pltpu.VMEM((1, EDGES_OWN), F32),
            pltpu.VMEM((32, EDGES_OWN), F32),
        ],
        2 * GIGA,
        [sources, targets, valids, bias],
        out_specs=[VMEM, VMEM, VMEM, VMEM, SMEM],
    )


def own_part(layer, total_nodes, args):
    in_specs = [VMEM] * len(args)
    in_specs[0] = HBM
    in_specs[-1] = SMEM
    return call(
        functools.partial(own_kernel, layer, total_nodes, layer > 0),
        "own_part",
        [
            shaped(NODES_OWN, FEAT, BF16),
            shaped(NODES_OWN, FEAT, F32),
            shaped(EDGES_OWN, FEAT, BF16),
            shaped(8, EDGES_OWN, F32),
        ],
        [
            pltpu.VMEM((NODES_OWN + CHUNK, FEAT + 128), BF16),
            pltpu.VMEM((CHUNK, FEAT + 128), F32),
            pltpu.VMEM((NODES_OWN, FEAT), args[0].dtype),
            pltpu.VMEM((NODES_OWN, FEAT), BF16),
            pltpu.VMEM((NODES_OWN, FEAT), F32),
            pltpu.VMEM((EDGES_OWN, FEAT), BF16),
            pltpu.SemaphoreType.DMA((NODE_CHUNKS + 3,)),
        ],
        3 * GIGA,
        args,
        in_specs=in_specs,
        out_specs=[HBM, HBM, HBM, VMEM],
    )


def edge_part(layer, total_nodes, with_send, args):
    outs = [shaped(NODES_OWN, FEAT, F32), shaped(2, FEAT, F32)]
    half = FEAT // 2
    scratch = [
        pltpu.VMEM((ROWS_IN, FEAT), BF16),
        pltpu.VMEM((NODES_OWN, FEAT), BF16),
        pltpu.VMEM((EDGES_OWN, FEAT), BF16),
        pltpu.VMEM((NODES_OWN, 8), F32),
        pltpu.VMEM((NODES_OWN, FEAT), F32),
        pltpu.SemaphoreType.DMA((5,)),
        pltpu.VMEM((2 * TABLE_ROWS, half), F32),
        pltpu.VMEM((2 * CHUNK, half), F32),
        pltpu.VMEM((2 * CHUNK, half), F32),
        pltpu.VMEM((EDGES_OWN, FEAT), BF16),
        pltpu.VMEM((8, EDGES_OWN), F32),
        pltpu.VMEM((2, 8, EDGES_OWN), F32),
        pltpu.VMEM((EDGES_OWN, 2 * FEAT), BF16),
        pltpu.VMEM((NODES_OWN + WINDOW, 2 * FEAT), F32),
    ]
    if with_send:
        outs.append(shaped(NODES_OWN, FEAT, BF16))
        scratch += [pltpu.SemaphoreType.DMA((NODE_CHUNKS,)), pltpu.VMEM((NODES_OWN, FEAT), F32)]
    in_specs = [ANY] + [HBM] * 4 + [VMEM] * (len(args) - 5)
    in_specs[9] = SMEM
    in_specs[11] = SMEM
    return call(
        functools.partial(edge_kernel, layer, total_nodes, layer > 0, with_send),
        "edge_part",
        outs,
        scratch,
        5 * GIGA,
        args,
        in_specs=in_specs,
        out_specs=[HBM, VMEM, VMEM] if with_send else None,
    )


def deliver(rows):
    return lax.all_to_all(
        rows.reshape(-1, 8, rows.shape[1]), GRP_BLK, split_axis=0, concat_axis=0, tiled=True
    ).reshape(rows.shape)


def shifted(value, axis, amount):
    size = lax.axis_size(axis)
    return lax.ppermute(value, axis, [(i, (i + amount) % size) for i in range(size)])


def total_along(stats):
    stats = stats + (
        shifted(stats, "blk_0", 2) + shifted(stats, "blk_0", 4) + shifted(stats, "blk_0", 6)
    )
    return stats + shifted(stats, "blk_0", 1)


def total_inside(stats):
    stats = stats + shifted(stats, "blk_2", 1)
    for axis in ("blk_1", "grp"):
        stats = stats + (
            shifted(stats, axis, 1) + shifted(stats, axis, 2) + shifted(stats, axis, 3)
        )
    return stats


def total_alone(stats):
    for axes in (("blk_1", "blk_2"), ("grp", "blk_0")):
        size = lax.axis_size(axes)
        copies = jnp.broadcast_to(stats[None], (size,) + stats.shape)
        stats = jnp.sum(lax.all_to_all(copies, axes, 0, 0, tiled=True), axis=0)
    return stats


def local(
    features,
    source_index,
    target_index,
    edge_valid,
    edge_bias,
    send_list,
    w_left,
    w_right,
    w_skip,
    attn_vec,
    norm_gain,
    norm_shift,
    peers,
):
    total_nodes = float(features.shape[0] * peers)
    row = (1, EDGES_OWN)
    sent = send_rows(send_list, features)
    received = deliver(sent)
    rows, srcs, bias, noedge, bound = sort_edges(
        source_index.reshape(row), target_index.reshape(row), edge_valid.reshape(row), edge_bias
    )
    weights = [w_left, w_right, w_skip, attn_vec, rows, bound]
    left, base, dst, own = own_part(0, total_nodes, [features] + weights)
    edges = [rows, srcs, bias, bound]
    summed, stats, rounded = edge_part(
        0,
        total_nodes,
        True,
        [received, left, dst, noedge, base, w_left, attn_vec, own] + edges,
    )
    stats = total_along(stats)
    sent = send_rows(send_list, rounded)
    sent, stats = lax.optimization_barrier((sent, stats))
    received = deliver(sent)
    stats = total_inside(stats)
    norms = [stats, norm_gain, norm_shift]
    left, base, dst, own = own_part(1, total_nodes, [summed] + norms + weights)
    summed, stats = edge_part(
        1,
        total_nodes,
        False,
        [received, left, dst, noedge, base, w_left, attn_vec, own] + edges + norms,
    )
    stats = total_alone(stats)
    return call(
        functools.partial(norm_kernel, 1, total_nodes),
        "norm_out",
        [shaped(NODES_OWN, FEAT, BF16)],
        [],
        1 << 20,
        [summed, stats, norm_gain, norm_shift],
    )[0]


def solution(mesh):
    split = Mesh(
        mesh.devices.reshape(mesh.shape["grp"], 8, 4, 2), ("grp", "blk_0", "blk_1", "blk_2")
    )
    edge = P(GRP_BLK, None)
    in_specs = (edge,) * 4 + (P(None, GRP_BLK), edge) + (P(),) * 6
    return jax.shard_map(
        functools.partial(local, peers=mesh.size),
        mesh=split,
        in_specs=in_specs,
        out_specs=edge,
        check_vma=False,
    )
```

```python
import functools

import jax
import jax.numpy as jnp
from jax import lax
from jax.experimental import pallas as pl
from jax.experimental.pallas import tpu as pltpu
from jax.sharding import Mesh
from jax.sharding import PartitionSpec as P

HEADS = 8
LAYERS = 2
GRP_BLK = ("grp", "blk_0", "blk_1", "blk_2")
NODES_OWN = 1024
EDGES_OWN = 2048
ROWS_IN = 2048
FEAT = 256
CHUNK = 256
EDGE_CHUNKS = EDGES_OWN // CHUNK
NODE_CHUNKS = NODES_OWN // CHUNK
WINDOW = 160
TABLE_ROWS = NODES_OWN + ROWS_IN
F32 = jnp.float32
BF16 = jnp.bfloat16


def iota(shape, dim):
    return lax.broadcasted_iota(jnp.int32, shape, dim)


def one_hot(mask):
    return jnp.where(mask, 1.0, 0.0).astype(BF16)


def dot(lhs, rhs):
    return jnp.dot(lhs, rhs, preferred_element_type=F32)


def dot_t(lhs, rhs):
    return lax.dot_general(lhs, rhs, (((1,), (1,)), ((), ())), preferred_element_type=F32)


def leaky(values):
    return jnp.where(values > 0, values, 0.2 * values)


def split_two(values):
    high = values.astype(BF16)
    return high, (values - high.astype(F32)).astype(BF16)


def split_three(values):
    high = values.astype(BF16)
    rest = values - high.astype(F32)
    mid = rest.astype(BF16)
    return high, mid, (rest - mid.astype(F32)).astype(BF16)


def head_rows(attn_ref, layer):
    shape = (16, FEAT)
    owner = iota(shape, 1) // (FEAT // HEADS) == iota(shape, 0)
    row = attn_ref[layer : layer + 1, :].astype(F32)
    return jnp.where(owner, row, 0.0).astype(BF16)


def head_spread():
    shape = (16, 2 * FEAT)
    return one_hot(iota(shape, 1) // (FEAT // HEADS) == iota(shape, 0))


def scores_of(heads, hidden):
    high, low = split_two(hidden)
    return (dot_t(heads, high) + dot_t(heads, low))[:HEADS]


def norm_terms(stats, total_nodes, gain, shift):
    mean = stats[0:1, :] / total_nodes
    spread = jnp.maximum(stats[1:2, :] / total_nodes - mean * mean, 0.0)
    return mean, lax.rsqrt(spread + 0.1), gain, shift


def normalize(values, terms):
    mean, inv, gain, shift = terms
    scaled = (values - mean) * inv * gain + shift
    grown = jnp.exp(jnp.minimum(scaled, 0.0)) - 1.0
    return jnp.where(scaled > 0, scaled, grown).astype(BF16)


def columns_of(row):
    return jnp.transpose(jnp.broadcast_to(row, (8, row.shape[1])))


def put_rows(pairs_ref, first, values):
    half = FEAT // 2
    pairs_ref[pl.ds(2 * first, CHUNK, stride=2), :] = values[:, :half]
    pairs_ref[pl.ds(2 * first + 1, CHUNK, stride=2), :] = values[:, half:]


def get_rows(pairs_ref):
    return jnp.concatenate(
        [pairs_ref[pl.ds(0, CHUNK, stride=2), :], pairs_ref[pl.ds(1, CHUNK, stride=2), :]], axis=1
    )


def fetch_rows(index_ref, first, pairs_ref, got_ref):
    for e in range(CHUNK):
        row = index_ref[0, first + e]
        got_ref[2 * e : 2 * e + 2, :] = pairs_ref[pl.ds(pl.multiple_of(2 * row, 2), 2), :]


def send_kernel(index_ref, list_ref, table_ref, out_hbm, pairs_ref, got_ref, out_ref, sems):
    for k in range(NODE_CHUNKS):
        put_rows(pairs_ref, k * CHUNK, table_ref[k * CHUNK : (k + 1) * CHUNK, :].astype(F32))

    def store(c):
        at = pl.ds(pl.multiple_of(c * 2 * CHUNK, 2 * CHUNK), 2 * CHUNK)
        return pltpu.make_async_copy(out_ref.at[at], out_hbm.at[at], sems.at[c])

    def pair(c, carry):
        here = pl.ds(pl.multiple_of(c * 2 * CHUNK, CHUNK), CHUNK)
        after = pl.ds(pl.multiple_of(c * 2 * CHUNK + CHUNK, CHUNK), CHUNK)
        fetch_rows(index_ref, c * 2 * CHUNK + CHUNK, pairs_ref, got_ref)
        col = columns_of(list_ref[0:1, here].astype(F32)).astype(jnp.int32)[:, 0:1]
        hot = one_hot(col == iota((CHUNK, NODES_OWN), 1))
        out_ref[here, :] = dot(hot, table_ref[...]).astype(BF16)
        out_ref[after, :] = get_rows(got_ref).astype(BF16)
        store(c).start()
        return carry

    count = ROWS_IN // (2 * CHUNK)
    lax.fori_loop(0, count, pair, 0)
    for c in range(count):
        store(c).wait()


def sort_kernel(
    src_ref, tgt_ref, valid_ref, bias_ref, rows_ref, srcs_ref, bias_out, noedge_ref, bound_ref,
    key_ref, pos_ref, meta_ref,
):
    width = (1, EDGES_OWN)
    live_in = valid_ref[...] > 0
    src = src_ref[...]
    tgt = jnp.where(live_in, tgt_ref[...], NODES_OWN)
    key = tgt * EDGES_OWN + iota(width, 1)
    key_ref[...] = columns_of(key.astype(F32)).astype(jnp.int32)
    pos_ref[...] = jnp.zeros_like(pos_ref)

    def rank(c, carry):
        at = pl.ds(pl.multiple_of(c * CHUNK, CHUNK), CHUNK)
        less = jnp.where(key_ref[at, 0:1] < key, 1.0, 0.0)
        pos_ref[...] += jnp.sum(less, axis=0, keepdims=True)
        return carry

    lax.fori_loop(0, EDGE_CHUNKS, rank, 0)
    pos = pos_ref[...].astype(jnp.int32)
    sub = iota((8, EDGES_OWN), 0)
    ints = jnp.where(
        sub == 0,
        src // 256,
        jnp.where(sub == 1, src % 256, jnp.where(sub == 2, tgt // 256, tgt % 256)),
    )
    high, mid, low = split_three(bias_ref[...])
    meta = jnp.concatenate(
        [ints.astype(F32), high.astype(F32), mid.astype(F32), low.astype(F32)], axis=0
    ).astype(BF16)

    def place(c, carry):
        at = pl.ds(pl.multiple_of(c * CHUNK, CHUNK), CHUNK)
        perm = one_hot(pos == iota((CHUNK, EDGES_OWN), 0) + c * CHUNK)
        meta_ref[:, at] = dot_t(meta, perm)
        return carry

    lax.fori_loop(0, EDGE_CHUNKS, place, 0)
    placed = meta_ref[...]
    bias_out[...] = placed[8:16] + placed[16:24] + placed[24:32]
    src_s = (placed[0:1] * 256.0 + placed[1:2]).astype(jnp.int32)
    tgt_s = (placed[2:3] * 256.0 + placed[3:4]).astype(jnp.int32)
    lane8 = iota((8, EDGES_OWN), 1)
    srcs_ref[...] = src_s
    tgt8 = jnp.broadcast_to(tgt_s, (8, EDGES_OWN))
    before = pltpu.roll(tgt8, 1, 1)
    after = pltpu.roll(tgt8, EDGES_OWN - 1, 1)
    live = tgt8 < NODES_OWN
    first = (lane8 == 0) | (before != tgt8)
    last = (lane8 == EDGES_OWN - 1) | (after != tgt8)
    start = jnp.where(first, lane8, 0)
    end = jnp.where(last, lane8, EDGES_OWN)
    step = 1
    while step < EDGES_OWN:
        start = jnp.maximum(start, jnp.where(lane8 >= step, pltpu.roll(start, step, 1), 0))
        shifted = pltpu.roll(end, EDGES_OWN - step, 1)
        end = jnp.minimum(end, jnp.where(lane8 + step < EDGES_OWN, shifted, EDGES_OWN))
        step *= 2
    start = jnp.where(live, start, lane8)
    end = jnp.where(live, end, lane8)
    rows_ref[...] = jnp.where(
        sub == 0, tgt8, jnp.where(sub == 1, start, jnp.where(sub == 2, end, lane8))
    )
    bound_ref[0, 2 * EDGE_CHUNKS] = jnp.max(end - start) + 1
    for c in range(EDGE_CHUNKS):
        piece = tgt8[:, c * CHUNK : (c + 1) * CHUNK]
        bound_ref[0, 2 * c] = jnp.min(piece)
        bound_ref[0, 2 * c + 1] = jnp.max(jnp.where(piece < NODES_OWN, piece, -1))
    for k in range(NODE_CHUNKS):
        hit = jnp.where(iota((CHUNK, EDGES_OWN), 0) + k * CHUNK == tgt_s, 1.0, 0.0)
        found = jnp.max(hit, axis=1, keepdims=True)
        noedge_ref[k * CHUNK : (k + 1) * CHUNK, :] = jnp.broadcast_to(1.0 - found, (CHUNK, 8))


def own_kernel(layer, total_nodes, with_norm, *refs):
    refs = list(refs)
    state_ref = refs.pop(0)
    if with_norm:
        stats_ref, gain_ref, shift_ref = refs[:3]
        refs = refs[3:]
        terms = norm_terms(
            stats_ref[...],
            total_nodes,
            gain_ref[layer - 1 : layer, :].astype(F32),
            shift_ref[layer - 1 : layer, :].astype(F32),
        )
    wl_ref, wr_ref, ws_ref, attn_ref, rows_ref, bound_ref = refs[:6]
    left_out, base_out, dst_hbm, self_out = refs[6:10]
    table_ref, acc_ref, own_ref, left_ref, base_ref, dst_out, sems = refs[10:]
    loads = []
    for k in range(NODE_CHUNKS):
        at = slice(k * CHUNK, (k + 1) * CHUNK)
        loads.append(pltpu.make_async_copy(state_ref.at[at], own_ref.at[at], sems.at[k]))
        loads[-1].start()
    stores = [
        pltpu.make_async_copy(left_ref, left_out, sems.at[NODE_CHUNKS]),
        pltpu.make_async_copy(base_ref, base_out, sems.at[NODE_CHUNKS + 1]),
        pltpu.make_async_copy(dst_out, dst_hbm, sems.at[NODE_CHUNKS + 2]),
    ]
    heads = head_rows(attn_ref, layer)
    for k in range(NODE_CHUNKS):
        at = slice(k * CHUNK, (k + 1) * CHUNK)
        loads[k].wait()
        states = own_ref[at, :]
        if with_norm:
            states = normalize(states, terms)
        left = dot(states, wl_ref[layer]).astype(BF16)
        right = dot(states, wr_ref[layer]).astype(BF16)
        left_ref[at, :] = left
        table_ref[at, :FEAT] = right
        base_ref[at, :] = states.astype(F32) + dot(states, ws_ref[layer])
        own = scores_of(heads, leaky(left.astype(F32) + right.astype(F32)))
        high, mid, low = split_three(own)
        parts = [high.astype(F32), mid.astype(F32), low.astype(F32)]
        parts += [jnp.zeros((128 - 3 * HEADS, CHUNK), F32)]
        table_ref[at, FEAT:] = jnp.transpose(jnp.concatenate(parts, axis=0)).astype(BF16)
    table_ref[NODES_OWN:, :] = jnp.zeros((CHUNK, FEAT + 128), BF16)
    stores[0].start()
    stores[1].start()

    def step(c, carry):
        at = pl.ds(pl.multiple_of(c * CHUNK, CHUNK), CHUNK)
        col = columns_of(rows_ref[0:1, at].astype(F32)).astype(jnp.int32)[:, 0:1]
        low = lax.div(bound_ref[0, 2 * c], 16) * 16
        extra = lax.div(jnp.maximum(bound_ref[0, 2 * c + 1] - low, 0), CHUNK)

        def window(w):
            base = pl.multiple_of(jnp.minimum(low + w * CHUNK, NODES_OWN), 16)
            hot = one_hot(col - base == iota((CHUNK, CHUNK), 1))
            return dot(hot, table_ref[pl.ds(base, CHUNK), :])

        acc_ref[...] = window(0)

        def more(w, carry):
            acc_ref[...] += window(w)
            return carry

        lax.fori_loop(1, extra + 1, more, 0)
        dst_out[at, :] = acc_ref[:, :FEAT].astype(BF16)
        back = jnp.transpose(acc_ref[:, FEAT:])
        self_out[:, at] = back[0:8] + back[8:16] + back[16:24]
        return carry

    lax.fori_loop(0, EDGE_CHUNKS, step, 0, unroll=2)
    stores[2].start()
    for store in stores:
        store.wait()


def scan_both(ref, longest, lane, start, end, join, neutral, values):
    def advance(ahead, back, step):
        moved = pltpu.roll(ahead, step, 1)
        ahead = join(ahead, jnp.where(lane - step >= start, moved, neutral))
        moved = pltpu.roll(back, EDGES_OWN - step, 1)
        return ahead, join(back, jnp.where(lane + step <= end, moved, neutral))

    ahead, back = values, values
    for step in (1, 2, 4, 8):
        ahead, back = advance(ahead, back, step)
    ref[0] = ahead
    ref[1] = back

    def rest():
        step = 16
        while step < EDGES_OWN:
            ref[0], ref[1] = advance(ref[0], ref[1], step)
            step *= 2

    pl.when(longest > 16)(rest)
    return ref[0], ref[1]


def edge_kernel(layer, total_nodes, with_norm, with_send, *refs):
    refs = list(refs)
    recv_any, left_any, dst_any, noedge_any, base_any = refs[:5]
    wl_ref, attn_ref, self_ref, rows_ref, srcs_ref, bias_ref, bound_ref = refs[5:12]
    refs = refs[12:]
    if with_norm:
        stats_in, gain_ref, shift_ref = refs[:3]
        refs = refs[3:]
    summed_hbm, stats_ref = refs[:2]
    refs = refs[2:]
    if with_send:
        round_ref = refs.pop(0)
    summed_ref, out_sems = refs.pop(), refs.pop()
    recv_ref, left_ref, dst_ref, noedge_ref, base_ref, sems = refs[:6]
    table_ref, even_ref, odd_ref, edge_ref, score_ref, scan_ref, mix_ref, acc_ref = refs[6:14]
    piece = ROWS_IN // 4
    moves = [
        (recv_any.at[k * piece : (k + 1) * piece], recv_ref.at[k * piece : (k + 1) * piece])
        for k in range(4)
    ]
    moves += [(left_any, left_ref), (dst_any, dst_ref)]
    moves += [(noedge_any, noedge_ref), (base_any, base_ref)]
    copies = [
        pltpu.make_async_copy(source, target, sems.at[i])
        for i, (source, target) in enumerate(moves)
    ]
    for copy in copies:
        copy.start()
    if with_norm:
        terms = norm_terms(
            stats_in[...],
            total_nodes,
            gain_ref[layer - 1 : layer, :].astype(F32),
            shift_ref[layer - 1 : layer, :].astype(F32),
        )
    heads = head_rows(attn_ref, layer)
    for c in range(ROWS_IN // CHUNK):
        if c * CHUNK % piece == 0:
            copies[c * CHUNK // piece].wait()
        states = recv_ref[c * CHUNK : (c + 1) * CHUNK, :]
        if with_norm:
            states = normalize(states.astype(F32), terms)
        left = dot(states, wl_ref[layer]).astype(BF16).astype(F32)
        put_rows(table_ref, NODES_OWN + c * CHUNK, left)
    copies[4].wait()
    for k in range(NODE_CHUNKS):
        put_rows(table_ref, k * CHUNK, left_ref[k * CHUNK : (k + 1) * CHUNK, :].astype(F32))

    def fetch(c, out_ref):
        fetch_rows(srcs_ref, c * CHUNK, table_ref, out_ref)

    def score(c, in_ref):
        at = pl.ds(pl.multiple_of(c * CHUNK, CHUNK), CHUNK)
        src = get_rows(in_ref)
        edge_ref[at, :] = src.astype(BF16)
        score_ref[:, at] = scores_of(heads, leaky(src + dst_ref[at, :].astype(F32)))

    fetch(0, even_ref)
    copies[5].wait()

    def pair(c, carry):
        fetch(2 * c + 1, odd_ref)
        score(2 * c, even_ref)
        fetch(lax.rem(2 * c + 2, EDGE_CHUNKS), even_ref)
        score(2 * c + 1, odd_ref)
        return carry

    lax.fori_loop(0, EDGE_CHUNKS // 2, pair, 0)

    tgt = rows_ref[0:1, :]
    start = rows_ref[1:2, :]
    end = rows_ref[2:3, :]
    lane = iota((8, EDGES_OWN), 1)
    live = tgt < NODES_OWN
    longest = bound_ref[0, 2 * EDGE_CHUNKS]
    scores = jnp.where(live, score_ref[...] + bias_ref[...], -1e30)
    own = self_ref[...]
    ahead, back = scan_both(scan_ref, longest, lane, start, end, jnp.maximum, -1e30, scores)
    top = jnp.maximum(jnp.maximum(ahead, back), own)
    weights = jnp.where(live, jnp.exp(scores - top), 0.0)
    own_weights = jnp.exp(own - top)
    ahead, back = scan_both(scan_ref, longest, lane, start, end, jnp.add, 0.0, weights)
    denom = own_weights + (ahead + (back - weights))
    last = live & (lane == end)
    score_ref[...] = weights / denom
    scan_ref[0] = jnp.where(last, own_weights / denom, 0.0)
    spread = head_spread()

    def mix(c, carry):
        at = pl.ds(pl.multiple_of(c * CHUNK, CHUNK), CHUNK)
        pair = jnp.concatenate([score_ref[:, at], scan_ref[0, :, at]], axis=0)
        wide = dot(jnp.transpose(pair).astype(BF16), spread)
        mix_ref[at, :FEAT] = (wide[:, :FEAT] * edge_ref[at, :].astype(F32)).astype(BF16)
        mix_ref[at, FEAT:] = wide[:, FEAT:].astype(BF16)
        return carry

    lax.fori_loop(0, EDGE_CHUNKS, mix, 0, unroll=4)
    acc_ref[...] = jnp.zeros_like(acc_ref)

    def gather_in(c, carry):
        here = pl.ds(pl.multiple_of(c * CHUNK, CHUNK), CHUNK)
        low = lax.div(bound_ref[0, 2 * c], 8) * 8
        count = lax.div(jnp.maximum(bound_ref[0, 2 * c + 1] - low + WINDOW, 0), WINDOW)

        def window(w, carry):
            first = pl.multiple_of(low + w * WINDOW, 8)
            hot = one_hot(iota((WINDOW, CHUNK), 0) + first == rows_ref[0:1, here])
            acc_ref[pl.ds(first, WINDOW), :] += dot(hot, mix_ref[here, :])
            return carry

        return lax.fori_loop(0, count, window, carry)

    lax.fori_loop(0, EDGE_CHUNKS, gather_in, 0)
    copies[6].wait()
    copies[7].wait()
    stats_ref[...] = jnp.zeros_like(stats_ref)
    stores = []
    for k in range(NODE_CHUNKS):
        at = slice(k * CHUNK, (k + 1) * CHUNK)
        own_alpha = jnp.where(noedge_ref[at, 0:1] > 0, 1.0, acc_ref[at, FEAT:])
        message = acc_ref[at, :FEAT] + own_alpha * left_ref[at, :].astype(F32)
        summed = base_ref[at, :] + message
        summed_ref[at, :] = summed
        stats_ref[0:1, :] += jnp.sum(summed, axis=0, keepdims=True)
        stats_ref[1:2, :] += jnp.sum(summed * summed, axis=0, keepdims=True)
        if with_send:
            round_ref[at, :] = summed.astype(BF16)
        store = pltpu.make_async_copy(summed_ref.at[at], summed_hbm.at[at], out_sems.at[k])
        store.start()
        stores.append(store)
    for store in stores:
        store.wait()


def shaped(rows, cols, dtype):
    return jax.ShapeDtypeStruct((rows, cols), dtype)


SMEM = pl.BlockSpec(memory_space=pltpu.SMEM)
VMEM = pl.BlockSpec(memory_space=pltpu.VMEM)
ANY = pl.BlockSpec(memory_space=pl.ANY)
HBM = pl.BlockSpec(memory_space=pltpu.HBM)


def call(body, name, outs, scratch, flops, args, in_specs=None, out_specs=None):
    cost = pl.CostEstimate(flops=flops, bytes_accessed=4 << 20, transcendentals=0)
    return pl.pallas_call(
        body,
        name=name,
        out_shape=outs,
        in_specs=in_specs or [VMEM] * len(args),
        out_specs=out_specs or [VMEM] * len(outs),
        scratch_shapes=scratch,
        cost_estimate=cost,
        compiler_params=pltpu.CompilerParams(vmem_limit_bytes=67_000_000),
    )(*args)


GIGA = 1 << 30


def send_rows(send_list, table):
    return call(
        send_kernel,
        "send_rows",
        [shaped(ROWS_IN, FEAT, BF16)],
        [
            pltpu.VMEM((2 * NODES_OWN, FEAT // 2), F32),
            pltpu.VMEM((2 * CHUNK, FEAT // 2), F32),
            pltpu.VMEM((ROWS_IN, FEAT), BF16),
            pltpu.SemaphoreType.DMA((ROWS_IN // (2 * CHUNK),)),
        ],
        GIGA,
        [send_list, send_list, table],
        in_specs=[SMEM, VMEM, VMEM],
        out_specs=[HBM],
    )[0]


def sort_edges(sources, targets, valids, bias):
    return call(
        sort_kernel,
        "sort_edges",
        [
            shaped(8, EDGES_OWN, jnp.int32),
            shaped(1, EDGES_OWN, jnp.int32),
            shaped(8, EDGES_OWN, F32),
            shaped(NODES_OWN, 8, F32),
            shaped(1, 32, jnp.int32),
        ],
        [
            pltpu.VMEM((EDGES_OWN, 8), jnp.int32),
            pltpu.VMEM((1, EDGES_OWN), F32),
            pltpu.VMEM((32, EDGES_OWN), F32),
        ],
        2 * GIGA,
        [sources, targets, valids, bias],
        out_specs=[VMEM, VMEM, VMEM, VMEM, SMEM],
    )


def own_part(layer, total_nodes, args):
    in_specs = [VMEM] * len(args)
    in_specs[0] = HBM
    in_specs[-1] = SMEM
    return call(
        functools.partial(own_kernel, layer, total_nodes, layer > 0),
        "own_part",
        [
            shaped(NODES_OWN, FEAT, BF16),
            shaped(NODES_OWN, FEAT, F32),
            shaped(EDGES_OWN, FEAT, BF16),
            shaped(8, EDGES_OWN, F32),
        ],
        [
            pltpu.VMEM((NODES_OWN + CHUNK, FEAT + 128), BF16),
            pltpu.VMEM((CHUNK, FEAT + 128), F32),
            pltpu.VMEM((NODES_OWN, FEAT), args[0].dtype),
            pltpu.VMEM((NODES_OWN, FEAT), BF16),
            pltpu.VMEM((NODES_OWN, FEAT), F32),
            pltpu.VMEM((EDGES_OWN, FEAT), BF16),
            pltpu.SemaphoreType.DMA((NODE_CHUNKS + 3,)),
        ],
        3 * GIGA,
        args,
        in_specs=in_specs,
        out_specs=[HBM, HBM, HBM, VMEM],
    )


def edge_part(layer, total_nodes, with_send, args):
    outs = [shaped(NODES_OWN, FEAT, F32), shaped(2, FEAT, F32)]
    half = FEAT // 2
    scratch = [
        pltpu.VMEM((ROWS_IN, FEAT), BF16),
        pltpu.VMEM((NODES_OWN, FEAT), BF16),
        pltpu.VMEM((EDGES_OWN, FEAT), BF16),
        pltpu.VMEM((NODES_OWN, 8), F32),
        pltpu.VMEM((NODES_OWN, FEAT), F32),
        pltpu.SemaphoreType.DMA((8,)),
        pltpu.VMEM((2 * TABLE_ROWS, half), F32),
        pltpu.VMEM((2 * CHUNK, half), F32),
        pltpu.VMEM((2 * CHUNK, half), F32),
        pltpu.VMEM((EDGES_OWN, FEAT), BF16),
        pltpu.VMEM((8, EDGES_OWN), F32),
        pltpu.VMEM((2, 8, EDGES_OWN), F32),
        pltpu.VMEM((EDGES_OWN, 2 * FEAT), BF16),
        pltpu.VMEM((NODES_OWN + WINDOW, 2 * FEAT), F32),
    ]
    if with_send:
        outs.append(shaped(NODES_OWN, FEAT, BF16))
    scratch += [pltpu.SemaphoreType.DMA((NODE_CHUNKS,)), pltpu.VMEM((NODES_OWN, FEAT), F32)]
    in_specs = [ANY] + [HBM] * 4 + [VMEM] * (len(args) - 5)
    in_specs[9] = SMEM
    in_specs[11] = SMEM
    return call(
        functools.partial(edge_kernel, layer, total_nodes, layer > 0, with_send),
        "edge_part",
        outs,
        scratch,
        5 * GIGA,
        args,
        in_specs=in_specs,
        out_specs=[HBM] + [VMEM] * (len(outs) - 1),
    )


def deliver(rows):
    return lax.all_to_all(
        rows.reshape(-1, 8, rows.shape[1]), GRP_BLK, split_axis=0, concat_axis=0, tiled=True
    ).reshape(rows.shape)


def shifted(value, axis, amount):
    size = lax.axis_size(axis)
    return lax.ppermute(value, axis, [(i, (i + amount) % size) for i in range(size)])


def copies_summed(stats, axes):
    size = lax.axis_size(axes)
    copies = jnp.broadcast_to(stats[None], (size,) + stats.shape)
    return jnp.sum(lax.all_to_all(copies, axes, 0, 0, tiled=True), axis=0)


def total_along(stats):
    return copies_summed(stats, ("blk_0",))


def total_inside(stats):
    stats = stats + shifted(stats, "blk_2", 1)
    for axis in ("blk_1", "grp"):
        stats = stats + (
            shifted(stats, axis, 1) + shifted(stats, axis, 2) + shifted(stats, axis, 3)
        )
    return stats


def total_alone(stats):
    first = lax.axis_index("blk_2") == 0
    mine = jnp.where(first, stats[0:1], stats[1:2])
    other = jnp.where(first, stats[1:2], stats[0:1])
    mine = (mine + shifted(other, "blk_2", 1)).reshape(2, FEAT // 2)
    mine = copies_summed(mine, ("grp", "blk_0", "blk_1")).reshape(1, FEAT)
    other = shifted(mine, "blk_2", 1)
    return jnp.concatenate([jnp.where(first, mine, other), jnp.where(first, other, mine)])


def local(
    features,
    source_index,
    target_index,
    edge_valid,
    edge_bias,
    send_list,
    w_left,
    w_right,
    w_skip,
    attn_vec,
    norm_gain,
    norm_shift,
    peers,
):
    total_nodes = float(features.shape[0] * peers)
    row = (1, EDGES_OWN)
    sent = send_rows(send_list, features)
    received = deliver(sent)
    rows, srcs, bias, noedge, bound = sort_edges(
        source_index.reshape(row), target_index.reshape(row), edge_valid.reshape(row), edge_bias
    )
    weights = [w_left, w_right, w_skip, attn_vec, rows, bound]
    left, base, dst, own = own_part(0, total_nodes, [features] + weights)
    edges = [rows, srcs, bias, bound]
    summed, stats, rounded = edge_part(
        0,
        total_nodes,
        True,
        [received, left, dst, noedge, base, w_left, attn_vec, own] + edges,
    )
    stats = total_along(stats)
    sent = send_rows(send_list, rounded)
    sent, stats = lax.optimization_barrier((sent, stats))
    received = deliver(sent)
    stats = total_inside(stats)
    norms = [stats, norm_gain, norm_shift]
    left, base, dst, own = own_part(1, total_nodes, [summed] + norms + weights)
    summed, stats = edge_part(
        1,
        total_nodes,
        False,
        [received, left, dst, noedge, base, w_left, attn_vec, own] + edges + norms,
    )
    stats = total_alone(stats)
    terms = norm_terms(stats, total_nodes, norm_gain[1:2].astype(F32), norm_shift[1:2].astype(F32))
    return normalize(summed, terms)


def solution(mesh):
    split = Mesh(
        mesh.devices.reshape(mesh.shape["grp"], 8, 4, 2), ("grp", "blk_0", "blk_1", "blk_2")
    )
    edge = P(GRP_BLK, None)
    in_specs = (edge,) * 4 + (P(None, GRP_BLK), edge) + (P(),) * 6
    return jax.shard_map(
        functools.partial(local, peers=mesh.size),
        mesh=split,
        in_specs=in_specs,
        out_specs=edge,
        check_vma=False,
    )
```

```python
import functools

import jax
import jax.numpy as jnp
from jax import lax
from jax.experimental import pallas as pl
from jax.experimental.pallas import tpu as pltpu
from jax.sharding import Mesh
from jax.sharding import PartitionSpec as P

HEADS = 8
LAYERS = 2
GRP_BLK = ("grp", "blk_0", "blk_1", "blk_2")
NODES_OWN = 1024
EDGES_OWN = 2048
ROWS_IN = 2048
FEAT = 256
CHUNK = 256
EDGE_CHUNKS = EDGES_OWN // CHUNK
NODE_CHUNKS = NODES_OWN // CHUNK
WINDOW = 160
COPIES = 8
TABLE_ROWS = NODES_OWN + ROWS_IN
F32 = jnp.float32
BF16 = jnp.bfloat16


def iota(shape, dim):
    return lax.broadcasted_iota(jnp.int32, shape, dim)


def one_hot(mask):
    return jnp.where(mask, 1.0, 0.0).astype(BF16)


def dot(lhs, rhs):
    return jnp.dot(lhs, rhs, preferred_element_type=F32)


def dot_t(lhs, rhs):
    return lax.dot_general(lhs, rhs, (((1,), (1,)), ((), ())), preferred_element_type=F32)


def leaky(values):
    return jnp.where(values > 0, values, 0.2 * values)


def split_two(values):
    high = values.astype(BF16)
    return high, (values - high.astype(F32)).astype(BF16)


def split_three(values):
    high = values.astype(BF16)
    rest = values - high.astype(F32)
    mid = rest.astype(BF16)
    return high, mid, (rest - mid.astype(F32)).astype(BF16)


def head_rows(attn_ref, layer):
    shape = (16, FEAT)
    owner = iota(shape, 1) // (FEAT // HEADS) == iota(shape, 0)
    row = attn_ref[layer : layer + 1, :].astype(F32)
    return jnp.where(owner, row, 0.0).astype(BF16)


def head_spread():
    shape = (16, 2 * FEAT)
    return one_hot(iota(shape, 1) // (FEAT // HEADS) == iota(shape, 0))


def scores_of(heads, hidden):
    high, low = split_two(hidden)
    return (dot_t(heads, high) + dot_t(heads, low))[:HEADS]


def norm_terms(stats, total_nodes, gain, shift):
    mean = stats[0:1, :] / total_nodes
    spread = jnp.maximum(stats[1:2, :] / total_nodes - mean * mean, 0.0)
    return mean, lax.rsqrt(spread + 0.1), gain, shift


def normalize(values, terms):
    mean, inv, gain, shift = terms
    scaled = (values - mean) * inv * gain + shift
    grown = jnp.exp(jnp.minimum(scaled, 0.0)) - 1.0
    return jnp.where(scaled > 0, scaled, grown).astype(BF16)


def columns_of(row):
    return jnp.transpose(jnp.broadcast_to(row, (8, row.shape[1])))


def put_rows(pairs_ref, first, values):
    half = FEAT // 2
    pairs_ref[pl.ds(2 * first, CHUNK, stride=2), :] = values[:, :half]
    pairs_ref[pl.ds(2 * first + 1, CHUNK, stride=2), :] = values[:, half:]


def get_rows(pairs_ref):
    return jnp.concatenate(
        [pairs_ref[pl.ds(0, CHUNK, stride=2), :], pairs_ref[pl.ds(1, CHUNK, stride=2), :]], axis=1
    )


def fetch_rows(index_ref, first, pairs_ref, got_ref):
    for e in range(CHUNK):
        row = index_ref[0, first + e]
        got_ref[2 * e : 2 * e + 2, :] = pairs_ref[pl.ds(pl.multiple_of(2 * row, 2), 2), :]


def send_kernel(index_ref, list_ref, table_ref, out_hbm, pairs_ref, got_ref, out_ref, sems):
    for k in range(NODE_CHUNKS):
        put_rows(pairs_ref, k * CHUNK, table_ref[k * CHUNK : (k + 1) * CHUNK, :].astype(F32))

    def store(c):
        at = pl.ds(pl.multiple_of(c * 2 * CHUNK, 2 * CHUNK), 2 * CHUNK)
        return pltpu.make_async_copy(out_ref.at[at], out_hbm.at[at], sems.at[c])

    def pair(c, carry):
        here = pl.ds(pl.multiple_of(c * 2 * CHUNK, CHUNK), CHUNK)
        after = pl.ds(pl.multiple_of(c * 2 * CHUNK + CHUNK, CHUNK), CHUNK)
        fetch_rows(index_ref, c * 2 * CHUNK + CHUNK, pairs_ref, got_ref)
        col = columns_of(list_ref[0:1, here].astype(F32)).astype(jnp.int32)[:, 0:1]
        hot = one_hot(col == iota((CHUNK, NODES_OWN), 1))
        out_ref[here, :] = dot(hot, table_ref[...]).astype(BF16)
        out_ref[after, :] = get_rows(got_ref).astype(BF16)
        store(c).start()
        return carry

    count = ROWS_IN // (2 * CHUNK)
    lax.fori_loop(0, count, pair, 0)
    for c in range(count):
        store(c).wait()


def sort_kernel(
    src_ref, tgt_ref, valid_ref, bias_ref, rows_ref, srcs_ref, bias_out, noedge_ref, bound_ref,
    key_ref, pos_ref, meta_ref,
):
    width = (1, EDGES_OWN)
    live_in = valid_ref[...] > 0
    src = src_ref[...]
    tgt = jnp.where(live_in, tgt_ref[...], NODES_OWN)
    key = tgt * EDGES_OWN + iota(width, 1)
    key_ref[...] = columns_of(key.astype(F32)).astype(jnp.int32)
    pos_ref[...] = jnp.zeros_like(pos_ref)

    def rank(c, carry):
        at = pl.ds(pl.multiple_of(c * CHUNK, CHUNK), CHUNK)
        less = jnp.where(key_ref[at, 0:1] < key, 1.0, 0.0)
        pos_ref[...] += jnp.sum(less, axis=0, keepdims=True)
        return carry

    lax.fori_loop(0, EDGE_CHUNKS, rank, 0)
    pos = pos_ref[...].astype(jnp.int32)
    sub = iota((8, EDGES_OWN), 0)
    ints = jnp.where(
        sub == 0,
        src // 256,
        jnp.where(sub == 1, src % 256, jnp.where(sub == 2, tgt // 256, tgt % 256)),
    )
    high, mid, low = split_three(bias_ref[...])
    meta = jnp.concatenate(
        [ints.astype(F32), high.astype(F32), mid.astype(F32), low.astype(F32)], axis=0
    ).astype(BF16)

    def place(c, carry):
        at = pl.ds(pl.multiple_of(c * CHUNK, CHUNK), CHUNK)
        perm = one_hot(pos == iota((CHUNK, EDGES_OWN), 0) + c * CHUNK)
        meta_ref[:, at] = dot_t(meta, perm)
        return carry

    lax.fori_loop(0, EDGE_CHUNKS, place, 0)
    placed = meta_ref[...]
    bias_out[...] = placed[8:16] + placed[16:24] + placed[24:32]
    src_s = (placed[0:1] * 256.0 + placed[1:2]).astype(jnp.int32)
    tgt_s = (placed[2:3] * 256.0 + placed[3:4]).astype(jnp.int32)
    lane8 = iota((8, EDGES_OWN), 1)
    srcs_ref[...] = src_s
    tgt8 = jnp.broadcast_to(tgt_s, (8, EDGES_OWN))
    before = pltpu.roll(tgt8, 1, 1)
    after = pltpu.roll(tgt8, EDGES_OWN - 1, 1)
    live = tgt8 < NODES_OWN
    first = (lane8 == 0) | (before != tgt8)
    last = (lane8 == EDGES_OWN - 1) | (after != tgt8)
    start = jnp.where(first, lane8, 0)
    end = jnp.where(last, lane8, EDGES_OWN)
    step = 1
    while step < EDGES_OWN:
        start = jnp.maximum(start, jnp.where(lane8 >= step, pltpu.roll(start, step, 1), 0))
        shifted = pltpu.roll(end, EDGES_OWN - step, 1)
        end = jnp.minimum(end, jnp.where(lane8 + step < EDGES_OWN, shifted, EDGES_OWN))
        step *= 2
    start = jnp.where(live, start, lane8)
    end = jnp.where(live, end, lane8)
    rows_ref[...] = jnp.where(
        sub == 0, tgt8, jnp.where(sub == 1, start, jnp.where(sub == 2, end, lane8))
    )
    bound_ref[0, 2 * EDGE_CHUNKS] = jnp.max(end - start) + 1
    for c in range(EDGE_CHUNKS):
        piece = tgt8[:, c * CHUNK : (c + 1) * CHUNK]
        bound_ref[0, 2 * c] = jnp.min(piece)
        bound_ref[0, 2 * c + 1] = jnp.max(jnp.where(piece < NODES_OWN, piece, -1))
    for k in range(NODE_CHUNKS):
        hit = jnp.where(iota((CHUNK, EDGES_OWN), 0) + k * CHUNK == tgt_s, 1.0, 0.0)
        found = jnp.max(hit, axis=1, keepdims=True)
        noedge_ref[k * CHUNK : (k + 1) * CHUNK, :] = jnp.broadcast_to(1.0 - found, (CHUNK, 8))


def own_kernel(layer, total_nodes, with_norm, *refs):
    refs = list(refs)
    state_ref = refs.pop(0)
    if with_norm:
        stats_ref, gain_ref, shift_ref = refs[:3]
        refs = refs[3:]
        terms = norm_terms(
            stats_ref[...],
            total_nodes,
            gain_ref[layer - 1 : layer, :].astype(F32),
            shift_ref[layer - 1 : layer, :].astype(F32),
        )
    wl_ref, wr_ref, ws_ref, attn_ref, rows_ref, bound_ref = refs[:6]
    left_out, base_out, dst_hbm, self_out = refs[6:10]
    table_ref, acc_ref, own_ref, left_ref, base_ref, dst_out, sems = refs[10:]
    loads = []
    for k in range(NODE_CHUNKS):
        at = slice(k * CHUNK, (k + 1) * CHUNK)
        loads.append(pltpu.make_async_copy(state_ref.at[at], own_ref.at[at], sems.at[k]))
        loads[-1].start()
    stores = [
        pltpu.make_async_copy(left_ref, left_out, sems.at[NODE_CHUNKS]),
        pltpu.make_async_copy(base_ref, base_out, sems.at[NODE_CHUNKS + 1]),
        pltpu.make_async_copy(dst_out, dst_hbm, sems.at[NODE_CHUNKS + 2]),
    ]
    heads = head_rows(attn_ref, layer)
    for k in range(NODE_CHUNKS):
        at = slice(k * CHUNK, (k + 1) * CHUNK)
        loads[k].wait()
        states = own_ref[at, :]
        if with_norm:
            states = normalize(states, terms)
        left = dot(states, wl_ref[layer]).astype(BF16)
        right = dot(states, wr_ref[layer]).astype(BF16)
        left_ref[at, :] = left
        table_ref[at, :FEAT] = right
        base_ref[at, :] = states.astype(F32) + dot(states, ws_ref[layer])
        own = scores_of(heads, leaky(left.astype(F32) + right.astype(F32)))
        high, mid, low = split_three(own)
        parts = [high.astype(F32), mid.astype(F32), low.astype(F32)]
        parts += [jnp.zeros((128 - 3 * HEADS, CHUNK), F32)]
        table_ref[at, FEAT:] = jnp.transpose(jnp.concatenate(parts, axis=0)).astype(BF16)
    table_ref[NODES_OWN:, :] = jnp.zeros((CHUNK, FEAT + 128), BF16)
    stores[0].start()
    stores[1].start()

    def step(c, carry):
        at = pl.ds(pl.multiple_of(c * CHUNK, CHUNK), CHUNK)
        col = columns_of(rows_ref[0:1, at].astype(F32)).astype(jnp.int32)[:, 0:1]
        low = lax.div(bound_ref[0, 2 * c], 16) * 16
        extra = lax.div(jnp.maximum(bound_ref[0, 2 * c + 1] - low, 0), CHUNK)

        def window(w):
            base = pl.multiple_of(jnp.minimum(low + w * CHUNK, NODES_OWN), 16)
            hot = one_hot(col - base == iota((CHUNK, CHUNK), 1))
            return dot(hot, table_ref[pl.ds(base, CHUNK), :])

        acc_ref[...] = window(0)

        def more(w, carry):
            acc_ref[...] += window(w)
            return carry

        lax.fori_loop(1, extra + 1, more, 0)
        dst_out[at, :] = acc_ref[:, :FEAT].astype(BF16)
        back = jnp.transpose(acc_ref[:, FEAT:])
        self_out[:, at] = back[0:8] + back[8:16] + back[16:24]
        return carry

    lax.fori_loop(0, EDGE_CHUNKS, step, 0, unroll=2)
    stores[2].start()
    for store in stores:
        store.wait()


def scan_both(ref, longest, lane, start, end, join, neutral, values):
    def advance(ahead, back, step):
        moved = pltpu.roll(ahead, step, 1)
        ahead = join(ahead, jnp.where(lane - step >= start, moved, neutral))
        moved = pltpu.roll(back, EDGES_OWN - step, 1)
        return ahead, join(back, jnp.where(lane + step <= end, moved, neutral))

    ahead, back = values, values
    for step in (1, 2, 4, 8):
        ahead, back = advance(ahead, back, step)
    ref[0] = ahead
    ref[1] = back

    def rest():
        step = 16
        while step < EDGES_OWN:
            ref[0], ref[1] = advance(ref[0], ref[1], step)
            step *= 2

    pl.when(longest > 16)(rest)
    return ref[0], ref[1]


def edge_kernel(layer, total_nodes, with_norm, with_send, *refs):
    refs = list(refs)
    recv_any, left_any, dst_any, noedge_any, base_any = refs[:5]
    small = 10 if with_norm else 7
    small_any = refs[5 : 5 + small]
    refs = refs[5 + small :]
    summed_hbm, stats_hbm = refs[:2]
    refs = refs[2:]
    if with_send:
        round_hbm = refs.pop(0)
    recv_ref, left_ref, dst_ref, noedge_ref, base_ref, sems = refs[:6]
    table_ref, even_ref, odd_ref, edge_ref, score_ref, scan_ref, mix_ref, acc_ref = refs[6:14]
    out_sems, summed_ref, stats_ref, round_ref = refs[14:18]
    small_refs = refs[18:]
    wl_ref, attn_ref, self_ref, rows_ref, srcs_ref, bias_ref, bound_ref = small_refs[:7]
    piece = ROWS_IN // 4
    pieces = [slice(k * piece, (k + 1) * piece) for k in range(4)]
    moves = [(small_any[0].at[layer], wl_ref), (recv_any.at[pieces[0]], recv_ref.at[pieces[0]])]
    moves += list(zip(small_any[7:], small_refs[7:]))
    moves += [(recv_any.at[at], recv_ref.at[at]) for at in pieces[1:]]
    moves += [(small_any[4], srcs_ref), (left_any, left_ref), (small_any[1], attn_ref)]
    moves += [(dst_any, dst_ref), (small_any[3], rows_ref), (small_any[6], bound_ref)]
    moves += [(small_any[2], self_ref), (small_any[5], bias_ref)]
    moves += [(noedge_any, noedge_ref), (base_any, base_ref)]
    copies = [
        pltpu.make_async_copy(source, target, sems.at[i])
        for i, (source, target) in enumerate(moves)
    ]
    for copy in copies:
        copy.start()
    waiting = iter(copies)

    def settle(count):
        for _ in range(count):
            next(waiting).wait()

    if with_norm:
        stats_in, gain_ref, shift_ref = small_refs[7:]
        settle(5)
        terms = norm_terms(
            stats_in[...],
            total_nodes,
            gain_ref[layer - 1 : layer, :].astype(F32),
            shift_ref[layer - 1 : layer, :].astype(F32),
        )
    else:
        settle(2)
    for c in range(ROWS_IN // CHUNK):
        if c and c * CHUNK % piece == 0:
            settle(1)
        states = recv_ref[c * CHUNK : (c + 1) * CHUNK, :]
        if with_norm:
            states = normalize(states.astype(F32), terms)
        left = dot(states, wl_ref[...]).astype(BF16).astype(F32)
        put_rows(table_ref, NODES_OWN + c * CHUNK, left)
    settle(3)
    heads = head_rows(attn_ref, layer)
    for k in range(NODE_CHUNKS):
        put_rows(table_ref, k * CHUNK, left_ref[k * CHUNK : (k + 1) * CHUNK, :].astype(F32))

    def fetch(c, out_ref):
        fetch_rows(srcs_ref, c * CHUNK, table_ref, out_ref)

    def score(c, in_ref):
        at = pl.ds(pl.multiple_of(c * CHUNK, CHUNK), CHUNK)
        src = get_rows(in_ref)
        edge_ref[at, :] = src.astype(BF16)
        score_ref[:, at] = scores_of(heads, leaky(src + dst_ref[at, :].astype(F32)))

    fetch(0, even_ref)
    settle(1)

    def pair(c, carry):
        fetch(2 * c + 1, odd_ref)
        score(2 * c, even_ref)
        fetch(lax.rem(2 * c + 2, EDGE_CHUNKS), even_ref)
        score(2 * c + 1, odd_ref)
        return carry

    lax.fori_loop(0, EDGE_CHUNKS // 2, pair, 0)

    settle(4)
    tgt = rows_ref[0:1, :]
    start = rows_ref[1:2, :]
    end = rows_ref[2:3, :]
    lane = iota((8, EDGES_OWN), 1)
    live = tgt < NODES_OWN
    longest = bound_ref[0, 2 * EDGE_CHUNKS]
    scores = jnp.where(live, score_ref[...] + bias_ref[...], -1e30)
    own = self_ref[...]
    ahead, back = scan_both(scan_ref, longest, lane, start, end, jnp.maximum, -1e30, scores)
    top = jnp.maximum(jnp.maximum(ahead, back), own)
    weights = jnp.where(live, jnp.exp(scores - top), 0.0)
    own_weights = jnp.exp(own - top)
    ahead, back = scan_both(scan_ref, longest, lane, start, end, jnp.add, 0.0, weights)
    denom = own_weights + (ahead + (back - weights))
    last = live & (lane == end)
    score_ref[...] = weights / denom
    scan_ref[0] = jnp.where(last, own_weights / denom, 0.0)
    spread = head_spread()

    def mix(c, carry):
        at = pl.ds(pl.multiple_of(c * CHUNK, CHUNK), CHUNK)
        pair = jnp.concatenate([score_ref[:, at], scan_ref[0, :, at]], axis=0)
        wide = dot(jnp.transpose(pair).astype(BF16), spread)
        mix_ref[at, :FEAT] = (wide[:, :FEAT] * edge_ref[at, :].astype(F32)).astype(BF16)
        mix_ref[at, FEAT:] = wide[:, FEAT:].astype(BF16)
        return carry

    lax.fori_loop(0, EDGE_CHUNKS, mix, 0, unroll=4)
    acc_ref[...] = jnp.zeros_like(acc_ref)

    def gather_in(c, carry):
        here = pl.ds(pl.multiple_of(c * CHUNK, CHUNK), CHUNK)
        low = lax.div(bound_ref[0, 2 * c], 8) * 8
        count = lax.div(jnp.maximum(bound_ref[0, 2 * c + 1] - low + WINDOW, 0), WINDOW)

        def window(w, carry):
            first = pl.multiple_of(low + w * WINDOW, 8)
            hot = one_hot(iota((WINDOW, CHUNK), 0) + first == rows_ref[0:1, here])
            acc_ref[pl.ds(first, WINDOW), :] += dot(hot, mix_ref[here, :])
            return carry

        return lax.fori_loop(0, count, window, carry)

    lax.fori_loop(0, EDGE_CHUNKS, gather_in, 0)
    settle(2)
    totals = jnp.zeros((2, FEAT), F32)
    stores = []
    for k in range(NODE_CHUNKS):
        at = slice(k * CHUNK, (k + 1) * CHUNK)
        own_alpha = jnp.where(noedge_ref[at, 0:1] > 0, 1.0, acc_ref[at, FEAT:])
        message = acc_ref[at, :FEAT] + own_alpha * left_ref[at, :].astype(F32)
        summed = base_ref[at, :] + message
        summed_ref[at, :] = summed
        sums = [jnp.sum(summed, axis=0, keepdims=True)]
        sums += [jnp.sum(summed * summed, axis=0, keepdims=True)]
        totals += jnp.concatenate(sums, axis=0)
        if with_send:
            round_ref[at, :] = summed.astype(BF16)
        store = pltpu.make_async_copy(summed_ref.at[at], summed_hbm.at[at], out_sems.at[k])
        store.start()
        stores.append(store)
    for k in range(COPIES):
        stats_ref[k] = totals
    stores.append(pltpu.make_async_copy(stats_ref, stats_hbm, out_sems.at[NODE_CHUNKS]))
    stores[-1].start()
    if with_send:
        stores.append(pltpu.make_async_copy(round_ref, round_hbm, out_sems.at[NODE_CHUNKS + 1]))
        stores[-1].start()
    for store in stores:
        store.wait()


def shaped(rows, cols, dtype):
    return jax.ShapeDtypeStruct((rows, cols), dtype)


SMEM = pl.BlockSpec(memory_space=pltpu.SMEM)
VMEM = pl.BlockSpec(memory_space=pltpu.VMEM)
ANY = pl.BlockSpec(memory_space=pl.ANY)
HBM = pl.BlockSpec(memory_space=pltpu.HBM)


def call(body, name, outs, scratch, flops, args, in_specs=None, out_specs=None):
    cost = pl.CostEstimate(flops=flops, bytes_accessed=4 << 20, transcendentals=0)
    return pl.pallas_call(
        body,
        name=name,
        out_shape=outs,
        in_specs=in_specs or [VMEM] * len(args),
        out_specs=out_specs or [VMEM] * len(outs),
        scratch_shapes=scratch,
        cost_estimate=cost,
        compiler_params=pltpu.CompilerParams(vmem_limit_bytes=67_000_000),
    )(*args)


GIGA = 1 << 30


def send_rows(send_list, table):
    return call(
        send_kernel,
        "send_rows",
        [shaped(ROWS_IN, FEAT, BF16)],
        [
            pltpu.VMEM((2 * NODES_OWN, FEAT // 2), F32),
            pltpu.VMEM((2 * CHUNK, FEAT // 2), F32),
            pltpu.VMEM((ROWS_IN, FEAT), BF16),
            pltpu.SemaphoreType.DMA((ROWS_IN // (2 * CHUNK),)),
        ],
        GIGA,
        [send_list, send_list, table],
        in_specs=[SMEM, VMEM, VMEM],
        out_specs=[HBM],
    )[0]


def sort_edges(sources, targets, valids, bias):
    return call(
        sort_kernel,
        "sort_edges",
        [
            shaped(8, EDGES_OWN, jnp.int32),
            shaped(1, EDGES_OWN, jnp.int32),
            shaped(8, EDGES_OWN, F32),
            shaped(NODES_OWN, 8, F32),
            shaped(1, 32, jnp.int32),
        ],
        [
            pltpu.VMEM((EDGES_OWN, 8), jnp.int32),
            pltpu.VMEM((1, EDGES_OWN), F32),
            pltpu.VMEM((32, EDGES_OWN), F32),
        ],
        2 * GIGA,
        [sources, targets, valids, bias],
        out_specs=[VMEM, VMEM, VMEM, VMEM, SMEM],
    )


def own_part(layer, total_nodes, args):
    in_specs = [VMEM] * len(args)
    in_specs[0] = HBM
    in_specs[-1] = SMEM
    return call(
        functools.partial(own_kernel, layer, total_nodes, layer > 0),
        "own_part",
        [
            shaped(NODES_OWN, FEAT, BF16),
            shaped(NODES_OWN, FEAT, F32),
            shaped(EDGES_OWN, FEAT, BF16),
            shaped(8, EDGES_OWN, F32),
        ],
        [
            pltpu.VMEM((NODES_OWN + CHUNK, FEAT + 128), BF16),
            pltpu.VMEM((CHUNK, FEAT + 128), F32),
            pltpu.VMEM((NODES_OWN, FEAT), args[0].dtype),
            pltpu.VMEM((NODES_OWN, FEAT), BF16),
            pltpu.VMEM((NODES_OWN, FEAT), F32),
            pltpu.VMEM((EDGES_OWN, FEAT), BF16),
            pltpu.SemaphoreType.DMA((NODE_CHUNKS + 3,)),
        ],
        3 * GIGA,
        args,
        in_specs=in_specs,
        out_specs=[HBM, HBM, HBM, VMEM],
    )


def edge_part(layer, total_nodes, with_send, args):
    outs = [
        shaped(NODES_OWN, FEAT, F32),
        jax.ShapeDtypeStruct((COPIES, 2, FEAT), F32),
    ]
    if with_send:
        outs.append(shaped(NODES_OWN, FEAT, BF16))
    half = FEAT // 2
    scratch = [
        pltpu.VMEM((ROWS_IN, FEAT), BF16),
        pltpu.VMEM((NODES_OWN, FEAT), BF16),
        pltpu.VMEM((EDGES_OWN, FEAT), BF16),
        pltpu.VMEM((NODES_OWN, 8), F32),
        pltpu.VMEM((NODES_OWN, FEAT), F32),
        pltpu.SemaphoreType.DMA((len(args) + 3,)),
        pltpu.VMEM((2 * TABLE_ROWS, half), F32),
        pltpu.VMEM((2 * CHUNK, half), F32),
        pltpu.VMEM((2 * CHUNK, half), F32),
        pltpu.VMEM((EDGES_OWN, FEAT), BF16),
        pltpu.VMEM((8, EDGES_OWN), F32),
        pltpu.VMEM((2, 8, EDGES_OWN), F32),
        pltpu.VMEM((EDGES_OWN, 2 * FEAT), BF16),
        pltpu.VMEM((NODES_OWN + WINDOW, 2 * FEAT), F32),
        pltpu.SemaphoreType.DMA((NODE_CHUNKS + 2,)),
        pltpu.VMEM((NODES_OWN, FEAT), F32),
        pltpu.VMEM((COPIES, 2, FEAT), F32),
        pltpu.VMEM((NODES_OWN, FEAT), BF16),
        pltpu.VMEM((FEAT, FEAT), BF16),
        pltpu.VMEM((LAYERS, FEAT), BF16),
        pltpu.VMEM((8, EDGES_OWN), F32),
        pltpu.VMEM((8, EDGES_OWN), jnp.int32),
        pltpu.SMEM((1, EDGES_OWN), jnp.int32),
        pltpu.VMEM((8, EDGES_OWN), F32),
        pltpu.SMEM((1, 32), jnp.int32),
    ]
    if layer > 0:
        scratch += [pltpu.VMEM((2, FEAT), F32)]
        scratch += [pltpu.VMEM((LAYERS, FEAT), BF16)] * 2
    return call(
        functools.partial(edge_kernel, layer, total_nodes, layer > 0, with_send),
        "edge_part",
        outs,
        scratch,
        5 * GIGA,
        args,
        in_specs=[HBM] * len(args),
        out_specs=[HBM] * len(outs),
    )


def deliver(rows):
    return lax.all_to_all(
        rows.reshape(-1, 8, rows.shape[1]), GRP_BLK, split_axis=0, concat_axis=0, tiled=True
    ).reshape(rows.shape)


def shifted(value, axis, amount):
    size = lax.axis_size(axis)
    return lax.ppermute(value, axis, [(i, (i + amount) % size) for i in range(size)])


def copies_summed(copies, axes):
    return jnp.sum(lax.all_to_all(copies, axes, 0, 0, tiled=True), axis=0)


def total_along(copies):
    return copies_summed(copies, ("blk_0",))


def total_inside(stats):
    stats = stats + shifted(stats, "blk_2", 1)
    for axis in ("blk_1", "grp"):
        stats = stats + (
            shifted(stats, axis, 1) + shifted(stats, axis, 2) + shifted(stats, axis, 3)
        )
    return stats


def total_alone(copies):
    stats = copies_summed(copies, ("blk_1", "blk_2"))
    axes = ("grp", "blk_0")
    copies = jnp.broadcast_to(stats[None], (lax.axis_size(axes),) + stats.shape)
    return copies_summed(copies, axes)


def local(
    features,
    source_index,
    target_index,
    edge_valid,
    edge_bias,
    send_list,
    w_left,
    w_right,
    w_skip,
    attn_vec,
    norm_gain,
    norm_shift,
    peers,
):
    total_nodes = float(features.shape[0] * peers)
    row = (1, EDGES_OWN)
    sent = send_rows(send_list, features)
    received = deliver(sent)
    rows, srcs, bias, noedge, bound = sort_edges(
        source_index.reshape(row), target_index.reshape(row), edge_valid.reshape(row), edge_bias
    )
    weights = [w_left, w_right, w_skip, attn_vec, rows, bound]
    left, base, dst, own = own_part(0, total_nodes, [features] + weights)
    edges = [rows, srcs, bias, bound]
    summed, stats, rounded = edge_part(
        0,
        total_nodes,
        True,
        [received, left, dst, noedge, base, w_left, attn_vec, own] + edges,
    )
    stats = total_along(stats)
    sent = send_rows(send_list, rounded)
    sent, stats = lax.optimization_barrier((sent, stats))
    received = deliver(sent)
    stats = total_inside(stats)
    norms = [stats, norm_gain, norm_shift]
    left, base, dst, own = own_part(1, total_nodes, [summed] + norms + weights)
    summed, stats = edge_part(
        1,
        total_nodes,
        False,
        [received, left, dst, noedge, base, w_left, attn_vec, own] + edges + norms,
    )
    stats = total_alone(stats)
    terms = norm_terms(stats, total_nodes, norm_gain[1:2].astype(F32), norm_shift[1:2].astype(F32))
    return normalize(summed, terms)


def solution(mesh):
    split = Mesh(
        mesh.devices.reshape(mesh.shape["grp"], 8, 4, 2), ("grp", "blk_0", "blk_1", "blk_2")
    )
    edge = P(GRP_BLK, None)
    in_specs = (edge,) * 4 + (P(None, GRP_BLK), edge) + (P(),) * 6
    return jax.shard_map(
        functools.partial(local, peers=mesh.size),
        mesh=split,
        in_specs=in_specs,
        out_specs=edge,
        check_vma=False,
    )
```

```python
import functools

import jax
import jax.numpy as jnp
from jax import lax
from jax.experimental import pallas as pl
from jax.experimental.pallas import tpu as pltpu
from jax.sharding import Mesh
from jax.sharding import PartitionSpec as P

HEADS = 8
LAYERS = 2
GRP_BLK = ("grp", "blk_0", "blk_1", "blk_2")
NODES_OWN = 1024
EDGES_OWN = 2048
ROWS_IN = 2048
FEAT = 256
CHUNK = 256
EDGE_CHUNKS = EDGES_OWN // CHUNK
NODE_CHUNKS = NODES_OWN // CHUNK
WINDOW = 160
COPIES = 8
TABLE_ROWS = NODES_OWN + ROWS_IN
F32 = jnp.float32
BF16 = jnp.bfloat16


def iota(shape, dim):
    return lax.broadcasted_iota(jnp.int32, shape, dim)


def one_hot(mask):
    return jnp.where(mask, 1.0, 0.0).astype(BF16)


def dot(lhs, rhs):
    return jnp.dot(lhs, rhs, preferred_element_type=F32)


def dot_t(lhs, rhs):
    return lax.dot_general(lhs, rhs, (((1,), (1,)), ((), ())), preferred_element_type=F32)


def leaky(values):
    return jnp.where(values > 0, values, 0.2 * values)


def split_two(values):
    high = values.astype(BF16)
    return high, (values - high.astype(F32)).astype(BF16)


def split_three(values):
    high = values.astype(BF16)
    rest = values - high.astype(F32)
    mid = rest.astype(BF16)
    return high, mid, (rest - mid.astype(F32)).astype(BF16)


def head_rows(attn_ref, layer):
    shape = (16, FEAT)
    owner = iota(shape, 1) // (FEAT // HEADS) == iota(shape, 0)
    row = attn_ref[layer : layer + 1, :].astype(F32)
    return jnp.where(owner, row, 0.0).astype(BF16)


def head_spread():
    shape = (16, 2 * FEAT)
    return one_hot(iota(shape, 1) // (FEAT // HEADS) == iota(shape, 0))


def scores_of(heads, hidden):
    high, low = split_two(hidden)
    return (dot_t(heads, high) + dot_t(heads, low))[:HEADS]


def norm_terms(stats, total_nodes, gain, shift):
    mean = stats[0:1, :] / total_nodes
    spread = jnp.maximum(stats[1:2, :] / total_nodes - mean * mean, 0.0)
    return mean, lax.rsqrt(spread + 0.1), gain, shift


def normalize(values, terms):
    mean, inv, gain, shift = terms
    scaled = (values - mean) * inv * gain + shift
    grown = jnp.exp(jnp.minimum(scaled, 0.0)) - 1.0
    return jnp.where(scaled > 0, scaled, grown).astype(BF16)


def columns_of(row):
    return jnp.transpose(jnp.broadcast_to(row, (8, row.shape[1])))


def put_rows(pairs_ref, first, values):
    half = FEAT // 2
    pairs_ref[pl.ds(2 * first, CHUNK, stride=2), :] = values[:, :half]
    pairs_ref[pl.ds(2 * first + 1, CHUNK, stride=2), :] = values[:, half:]


def get_rows(pairs_ref):
    return jnp.concatenate(
        [pairs_ref[pl.ds(0, CHUNK, stride=2), :], pairs_ref[pl.ds(1, CHUNK, stride=2), :]], axis=1
    )


def fetch_rows(index_ref, first, pairs_ref, got_ref):
    for e in range(CHUNK):
        row = index_ref[0, first + e]
        got_ref[2 * e : 2 * e + 2, :] = pairs_ref[pl.ds(pl.multiple_of(2 * row, 2), 2), :]


def send_kernel(index_ref, list_ref, table_ref, out_hbm, pairs_ref, got_ref, out_ref, sems):
    for k in range(NODE_CHUNKS):
        put_rows(pairs_ref, k * CHUNK, table_ref[k * CHUNK : (k + 1) * CHUNK, :].astype(F32))

    def store(c):
        at = pl.ds(pl.multiple_of(c * 2 * CHUNK, 2 * CHUNK), 2 * CHUNK)
        return pltpu.make_async_copy(out_ref.at[at], out_hbm.at[at], sems.at[c])

    def pair(c, carry):
        here = pl.ds(pl.multiple_of(c * 2 * CHUNK, CHUNK), CHUNK)
        after = pl.ds(pl.multiple_of(c * 2 * CHUNK + CHUNK, CHUNK), CHUNK)
        fetch_rows(index_ref, c * 2 * CHUNK + CHUNK, pairs_ref, got_ref)
        col = columns_of(list_ref[0:1, here].astype(F32)).astype(jnp.int32)[:, 0:1]
        hot = one_hot(col == iota((CHUNK, NODES_OWN), 1))
        out_ref[here, :] = dot(hot, table_ref[...]).astype(BF16)
        out_ref[after, :] = get_rows(got_ref).astype(BF16)
        store(c).start()
        return carry

    count = ROWS_IN // (2 * CHUNK)
    lax.fori_loop(0, count, pair, 0)
    for c in range(count):
        store(c).wait()


def sort_kernel(
    src_ref, tgt_ref, valid_ref, bias_ref, rows_ref, srcs_ref, bias_out, noedge_ref, bound_ref,
    key_ref, pos_ref, meta_ref,
):
    width = (1, EDGES_OWN)
    live_in = valid_ref[...] > 0
    src = src_ref[...]
    tgt = jnp.where(live_in, tgt_ref[...], NODES_OWN)
    key = tgt * EDGES_OWN + iota(width, 1)
    key_ref[...] = columns_of(key.astype(F32)).astype(jnp.int32)
    pos_ref[...] = jnp.zeros_like(pos_ref)

    def rank(c, carry):
        at = pl.ds(pl.multiple_of(c * CHUNK, CHUNK), CHUNK)
        less = jnp.where(key_ref[at, 0:1] < key, 1.0, 0.0)
        pos_ref[...] += jnp.sum(less, axis=0, keepdims=True)
        return carry

    lax.fori_loop(0, EDGE_CHUNKS, rank, 0)
    pos = pos_ref[...].astype(jnp.int32)
    sub = iota((8, EDGES_OWN), 0)
    ints = jnp.where(
        sub == 0,
        src // 256,
        jnp.where(sub == 1, src % 256, jnp.where(sub == 2, tgt // 256, tgt % 256)),
    )
    high, mid, low = split_three(bias_ref[...])
    meta = jnp.concatenate(
        [ints.astype(F32), high.astype(F32), mid.astype(F32), low.astype(F32)], axis=0
    ).astype(BF16)

    def place(c, carry):
        at = pl.ds(pl.multiple_of(c * CHUNK, CHUNK), CHUNK)
        perm = one_hot(pos == iota((CHUNK, EDGES_OWN), 0) + c * CHUNK)
        meta_ref[:, at] = dot_t(meta, perm)
        return carry

    lax.fori_loop(0, EDGE_CHUNKS, place, 0)
    placed = meta_ref[...]
    bias_out[...] = placed[8:16] + placed[16:24] + placed[24:32]
    src_s = (placed[0:1] * 256.0 + placed[1:2]).astype(jnp.int32)
    tgt_s = (placed[2:3] * 256.0 + placed[3:4]).astype(jnp.int32)
    lane8 = iota((8, EDGES_OWN), 1)
    srcs_ref[...] = src_s
    tgt8 = jnp.broadcast_to(tgt_s, (8, EDGES_OWN))
    before = pltpu.roll(tgt8, 1, 1)
    after = pltpu.roll(tgt8, EDGES_OWN - 1, 1)
    live = tgt8 < NODES_OWN
    first = (lane8 == 0) | (before != tgt8)
    last = (lane8 == EDGES_OWN - 1) | (after != tgt8)
    start = jnp.where(first, lane8, 0)
    end = jnp.where(last, lane8, EDGES_OWN)
    step = 1
    while step < EDGES_OWN:
        start = jnp.maximum(start, jnp.where(lane8 >= step, pltpu.roll(start, step, 1), 0))
        shifted = pltpu.roll(end, EDGES_OWN - step, 1)
        end = jnp.minimum(end, jnp.where(lane8 + step < EDGES_OWN, shifted, EDGES_OWN))
        step *= 2
    start = jnp.where(live, start, lane8)
    end = jnp.where(live, end, lane8)
    rows_ref[...] = jnp.where(
        sub == 0, tgt8, jnp.where(sub == 1, start, jnp.where(sub == 2, end, lane8))
    )
    bound_ref[0, 2 * EDGE_CHUNKS] = jnp.max(end - start) + 1
    for c in range(EDGE_CHUNKS):
        piece = tgt8[:, c * CHUNK : (c + 1) * CHUNK]
        bound_ref[0, 2 * c] = jnp.min(piece)
        bound_ref[0, 2 * c + 1] = jnp.max(jnp.where(piece < NODES_OWN, piece, -1))
    for k in range(NODE_CHUNKS):
        hit = jnp.where(iota((CHUNK, EDGES_OWN), 0) + k * CHUNK == tgt_s, 1.0, 0.0)
        found = jnp.max(hit, axis=1, keepdims=True)
        noedge_ref[k * CHUNK : (k + 1) * CHUNK, :] = jnp.broadcast_to(1.0 - found, (CHUNK, 8))


def own_kernel(layer, total_nodes, with_norm, *refs):
    refs = list(refs)
    state_ref = refs.pop(0)
    if with_norm:
        stats_ref, gain_ref, shift_ref = refs[:3]
        refs = refs[3:]
        terms = norm_terms(
            stats_ref[...],
            total_nodes,
            gain_ref[layer - 1 : layer, :].astype(F32),
            shift_ref[layer - 1 : layer, :].astype(F32),
        )
    wl_ref, wr_ref, ws_ref, attn_ref, rows_ref, bound_ref = refs[:6]
    left_out, base_out, dst_hbm, self_out = refs[6:10]
    table_ref, acc_ref, own_ref, left_ref, base_ref, dst_out, sems = refs[10:]
    loads = []
    for k in range(NODE_CHUNKS):
        at = slice(k * CHUNK, (k + 1) * CHUNK)
        loads.append(pltpu.make_async_copy(state_ref.at[at], own_ref.at[at], sems.at[k]))
        loads[-1].start()
    stores = [
        pltpu.make_async_copy(left_ref, left_out, sems.at[NODE_CHUNKS]),
        pltpu.make_async_copy(base_ref, base_out, sems.at[NODE_CHUNKS + 1]),
        pltpu.make_async_copy(dst_out, dst_hbm, sems.at[NODE_CHUNKS + 2]),
    ]
    heads = head_rows(attn_ref, layer)
    for k in range(NODE_CHUNKS):
        at = slice(k * CHUNK, (k + 1) * CHUNK)
        loads[k].wait()
        states = own_ref[at, :]
        if with_norm:
            states = normalize(states, terms)
        left = dot(states, wl_ref[layer]).astype(BF16)
        right = dot(states, wr_ref[layer]).astype(BF16)
        left_ref[at, :] = left
        table_ref[at, :FEAT] = right
        base_ref[at, :] = states.astype(F32) + dot(states, ws_ref[layer])
        own = scores_of(heads, leaky(left.astype(F32) + right.astype(F32)))
        high, mid, low = split_three(own)
        parts = [high.astype(F32), mid.astype(F32), low.astype(F32)]
        parts += [jnp.zeros((128 - 3 * HEADS, CHUNK), F32)]
        table_ref[at, FEAT:] = jnp.transpose(jnp.concatenate(parts, axis=0)).astype(BF16)
    table_ref[NODES_OWN:, :] = jnp.zeros((CHUNK, FEAT + 128), BF16)
    stores[0].start()
    stores[1].start()

    def step(c, carry):
        at = pl.ds(pl.multiple_of(c * CHUNK, CHUNK), CHUNK)
        col = columns_of(rows_ref[0:1, at].astype(F32)).astype(jnp.int32)[:, 0:1]
        low = lax.div(bound_ref[0, 2 * c], 16) * 16
        extra = lax.div(jnp.maximum(bound_ref[0, 2 * c + 1] - low, 0), CHUNK)

        def window(w):
            base = pl.multiple_of(jnp.minimum(low + w * CHUNK, NODES_OWN), 16)
            hot = one_hot(col - base == iota((CHUNK, CHUNK), 1))
            return dot(hot, table_ref[pl.ds(base, CHUNK), :])

        acc_ref[...] = window(0)

        def more(w, carry):
            acc_ref[...] += window(w)
            return carry

        lax.fori_loop(1, extra + 1, more, 0)
        dst_out[at, :] = acc_ref[:, :FEAT].astype(BF16)
        back = jnp.transpose(acc_ref[:, FEAT:])
        self_out[:, at] = back[0:8] + back[8:16] + back[16:24]
        return carry

    lax.fori_loop(0, EDGE_CHUNKS, step, 0, unroll=2)
    stores[2].start()
    for store in stores:
        store.wait()


def scan_both(ref, longest, lane, start, end, join, neutral, values):
    def advance(ahead, back, step):
        moved = pltpu.roll(ahead, step, 1)
        ahead = join(ahead, jnp.where(lane - step >= start, moved, neutral))
        moved = pltpu.roll(back, EDGES_OWN - step, 1)
        return ahead, join(back, jnp.where(lane + step <= end, moved, neutral))

    ahead, back = values, values
    for step in (1, 2, 4, 8):
        ahead, back = advance(ahead, back, step)
    ref[0] = ahead
    ref[1] = back

    def rest():
        step = 16
        while step < EDGES_OWN:
            ref[0], ref[1] = advance(ref[0], ref[1], step)
            step *= 2

    pl.when(longest > 16)(rest)
    return ref[0], ref[1]


def edge_kernel(layer, total_nodes, with_norm, with_send, *refs):
    refs = list(refs)
    recv_any, left_any, dst_any, noedge_any, base_any = refs[:5]
    small = 10 if with_norm else 7
    small_any = refs[5 : 5 + small]
    refs = refs[5 + small :]
    summed_hbm, stats_hbm = refs[:2]
    refs = refs[2:]
    if with_send:
        round_hbm = refs.pop(0)
    recv_ref, left_ref, dst_ref, noedge_ref, base_ref, sems = refs[:6]
    table_ref, even_ref, odd_ref, edge_ref, score_ref, scan_ref, mix_ref, acc_ref = refs[6:14]
    out_sems, summed_ref, stats_ref, round_ref = refs[14:18]
    small_refs = refs[18:]
    wl_ref, attn_ref, self_ref, rows_ref, srcs_ref, bias_ref, bound_ref = small_refs[:7]
    piece = ROWS_IN // 4
    pieces = [slice(k * piece, (k + 1) * piece) for k in range(4)]
    moves = [(small_any[0].at[layer], wl_ref), (recv_any.at[pieces[0]], recv_ref.at[pieces[0]])]
    moves += list(zip(small_any[7:], small_refs[7:]))
    moves += [(recv_any.at[at], recv_ref.at[at]) for at in pieces[1:]]
    moves += [(small_any[4], srcs_ref), (left_any, left_ref), (small_any[1], attn_ref)]
    moves += [(dst_any, dst_ref), (small_any[3], rows_ref), (small_any[6], bound_ref)]
    moves += [(small_any[2], self_ref), (small_any[5], bias_ref)]
    moves += [(noedge_any, noedge_ref), (base_any, base_ref)]
    copies = [
        pltpu.make_async_copy(source, target, sems.at[i])
        for i, (source, target) in enumerate(moves)
    ]
    for copy in copies:
        copy.start()
    waiting = iter(copies)

    def settle(count):
        for _ in range(count):
            next(waiting).wait()

    if with_norm:
        stats_in, gain_ref, shift_ref = small_refs[7:]
        settle(5)
        terms = norm_terms(
            stats_in[...],
            total_nodes,
            gain_ref[layer - 1 : layer, :].astype(F32),
            shift_ref[layer - 1 : layer, :].astype(F32),
        )
    else:
        settle(2)
    for c in range(ROWS_IN // CHUNK):
        if c and c * CHUNK % piece == 0:
            settle(1)
        states = recv_ref[c * CHUNK : (c + 1) * CHUNK, :]
        if with_norm:
            states = normalize(states.astype(F32), terms)
        left = dot(states, wl_ref[...]).astype(BF16).astype(F32)
        put_rows(table_ref, NODES_OWN + c * CHUNK, left)
    settle(3)
    heads = head_rows(attn_ref, layer)
    for k in range(NODE_CHUNKS):
        put_rows(table_ref, k * CHUNK, left_ref[k * CHUNK : (k + 1) * CHUNK, :].astype(F32))

    def fetch(c, out_ref):
        fetch_rows(srcs_ref, c * CHUNK, table_ref, out_ref)

    def score(c, in_ref):
        at = pl.ds(pl.multiple_of(c * CHUNK, CHUNK), CHUNK)
        src = get_rows(in_ref)
        edge_ref[at, :] = src.astype(BF16)
        score_ref[:, at] = scores_of(heads, leaky(src + dst_ref[at, :].astype(F32)))

    fetch(0, even_ref)
    settle(1)

    def pair(c, carry):
        fetch(2 * c + 1, odd_ref)
        score(2 * c, even_ref)
        fetch(lax.rem(2 * c + 2, EDGE_CHUNKS), even_ref)
        score(2 * c + 1, odd_ref)
        return carry

    lax.fori_loop(0, EDGE_CHUNKS // 2, pair, 0)

    settle(4)
    tgt = rows_ref[0:1, :]
    start = rows_ref[1:2, :]
    end = rows_ref[2:3, :]
    lane = iota((8, EDGES_OWN), 1)
    live = tgt < NODES_OWN
    longest = bound_ref[0, 2 * EDGE_CHUNKS]
    scores = jnp.where(live, score_ref[...] + bias_ref[...], -1e30)
    own = self_ref[...]
    ahead, back = scan_both(scan_ref, longest, lane, start, end, jnp.maximum, -1e30, scores)
    top = jnp.maximum(jnp.maximum(ahead, back), own)
    weights = jnp.where(live, jnp.exp(scores - top), 0.0)
    own_weights = jnp.exp(own - top)
    ahead, back = scan_both(scan_ref, longest, lane, start, end, jnp.add, 0.0, weights)
    denom = own_weights + (ahead + (back - weights))
    last = live & (lane == end)
    score_ref[...] = weights / denom
    scan_ref[0] = jnp.where(last, own_weights / denom, 0.0)
    spread = head_spread()

    def mix(c, carry):
        at = pl.ds(pl.multiple_of(c * CHUNK, CHUNK), CHUNK)
        pair = jnp.concatenate([score_ref[:, at], scan_ref[0, :, at]], axis=0)
        wide = dot(jnp.transpose(pair).astype(BF16), spread)
        mix_ref[at, :FEAT] = (wide[:, :FEAT] * edge_ref[at, :].astype(F32)).astype(BF16)
        mix_ref[at, FEAT:] = wide[:, FEAT:].astype(BF16)
        return carry

    lax.fori_loop(0, EDGE_CHUNKS, mix, 0, unroll=4)
    acc_ref[...] = jnp.zeros_like(acc_ref)

    def gather_in(c, carry):
        here = pl.ds(pl.multiple_of(c * CHUNK, CHUNK), CHUNK)
        low = lax.div(bound_ref[0, 2 * c], 8) * 8
        count = lax.div(jnp.maximum(bound_ref[0, 2 * c + 1] - low + WINDOW, 0), WINDOW)

        def window(w, carry):
            first = pl.multiple_of(low + w * WINDOW, 8)
            hot = one_hot(iota((WINDOW, CHUNK), 0) + first == rows_ref[0:1, here])
            acc_ref[pl.ds(first, WINDOW), :] += dot(hot, mix_ref[here, :])
            return carry

        return lax.fori_loop(0, count, window, carry)

    lax.fori_loop(0, EDGE_CHUNKS, gather_in, 0)
    settle(2)
    totals = jnp.zeros((2, FEAT), F32)
    stores = []
    for k in range(NODE_CHUNKS):
        at = slice(k * CHUNK, (k + 1) * CHUNK)
        own_alpha = jnp.where(noedge_ref[at, 0:1] > 0, 1.0, acc_ref[at, FEAT:])
        message = acc_ref[at, :FEAT] + own_alpha * left_ref[at, :].astype(F32)
        summed = base_ref[at, :] + message
        summed_ref[at, :] = summed
        sums = [jnp.sum(summed, axis=0, keepdims=True)]
        sums += [jnp.sum(summed * summed, axis=0, keepdims=True)]
        totals += jnp.concatenate(sums, axis=0)
        if with_send:
            round_ref[at, :] = summed.astype(BF16)
        store = pltpu.make_async_copy(summed_ref.at[at], summed_hbm.at[at], out_sems.at[k])
        store.start()
        stores.append(store)
    for k in range(COPIES):
        stats_ref[k] = totals
    stores.append(pltpu.make_async_copy(stats_ref, stats_hbm, out_sems.at[NODE_CHUNKS]))
    stores[-1].start()
    if with_send:
        stores.append(pltpu.make_async_copy(round_ref, round_hbm, out_sems.at[NODE_CHUNKS + 1]))
        stores[-1].start()
    for store in stores:
        store.wait()


def shaped(rows, cols, dtype):
    return jax.ShapeDtypeStruct((rows, cols), dtype)


SMEM = pl.BlockSpec(memory_space=pltpu.SMEM)
VMEM = pl.BlockSpec(memory_space=pltpu.VMEM)
ANY = pl.BlockSpec(memory_space=pl.ANY)
HBM = pl.BlockSpec(memory_space=pltpu.HBM)


def call(body, name, outs, scratch, flops, args, in_specs=None, out_specs=None):
    cost = pl.CostEstimate(flops=flops, bytes_accessed=4 << 20, transcendentals=0)
    return pl.pallas_call(
        body,
        name=name,
        out_shape=outs,
        in_specs=in_specs or [VMEM] * len(args),
        out_specs=out_specs or [VMEM] * len(outs),
        scratch_shapes=scratch,
        cost_estimate=cost,
        compiler_params=pltpu.CompilerParams(vmem_limit_bytes=67_000_000),
    )(*args)


GIGA = 1 << 30


def send_rows(send_list, table):
    return call(
        send_kernel,
        "send_rows",
        [shaped(ROWS_IN, FEAT, BF16)],
        [
            pltpu.VMEM((2 * NODES_OWN, FEAT // 2), F32),
            pltpu.VMEM((2 * CHUNK, FEAT // 2), F32),
            pltpu.VMEM((ROWS_IN, FEAT), BF16),
            pltpu.SemaphoreType.DMA((ROWS_IN // (2 * CHUNK),)),
        ],
        GIGA,
        [send_list, send_list, table],
        in_specs=[SMEM, VMEM, VMEM],
        out_specs=[HBM],
    )[0]


def sort_edges(sources, targets, valids, bias):
    return call(
        sort_kernel,
        "sort_edges",
        [
            shaped(8, EDGES_OWN, jnp.int32),
            shaped(1, EDGES_OWN, jnp.int32),
            shaped(8, EDGES_OWN, F32),
            shaped(NODES_OWN, 8, F32),
            shaped(1, 32, jnp.int32),
        ],
        [
            pltpu.VMEM((EDGES_OWN, 8), jnp.int32),
            pltpu.VMEM((1, EDGES_OWN), F32),
            pltpu.VMEM((32, EDGES_OWN), F32),
        ],
        2 * GIGA,
        [sources, targets, valids, bias],
        out_specs=[VMEM, VMEM, VMEM, VMEM, SMEM],
    )


def own_part(layer, total_nodes, args):
    in_specs = [VMEM] * len(args)
    in_specs[0] = HBM
    in_specs[-1] = SMEM
    return call(
        functools.partial(own_kernel, layer, total_nodes, layer > 0),
        "own_part",
        [
            shaped(NODES_OWN, FEAT, BF16),
            shaped(NODES_OWN, FEAT, F32),
            shaped(EDGES_OWN, FEAT, BF16),
            shaped(8, EDGES_OWN, F32),
        ],
        [
            pltpu.VMEM((NODES_OWN + CHUNK, FEAT + 128), BF16),
            pltpu.VMEM((CHUNK, FEAT + 128), F32),
            pltpu.VMEM((NODES_OWN, FEAT), args[0].dtype),
            pltpu.VMEM((NODES_OWN, FEAT), BF16),
            pltpu.VMEM((NODES_OWN, FEAT), F32),
            pltpu.VMEM((EDGES_OWN, FEAT), BF16),
            pltpu.SemaphoreType.DMA((NODE_CHUNKS + 3,)),
        ],
        3 * GIGA,
        args,
        in_specs=in_specs,
        out_specs=[HBM, HBM, HBM, VMEM],
    )


def edge_part(layer, total_nodes, with_send, args):
    outs = [
        shaped(NODES_OWN, FEAT, F32),
        jax.ShapeDtypeStruct((COPIES, 2, FEAT), F32),
    ]
    if with_send:
        outs.append(shaped(NODES_OWN, FEAT, BF16))
    half = FEAT // 2
    scratch = [
        pltpu.VMEM((ROWS_IN, FEAT), BF16),
        pltpu.VMEM((NODES_OWN, FEAT), BF16),
        pltpu.VMEM((EDGES_OWN, FEAT), BF16),
        pltpu.VMEM((NODES_OWN, 8), F32),
        pltpu.VMEM((NODES_OWN, FEAT), F32),
        pltpu.SemaphoreType.DMA((len(args) + 3,)),
        pltpu.VMEM((2 * TABLE_ROWS, half), F32),
        pltpu.VMEM((2 * CHUNK, half), F32),
        pltpu.VMEM((2 * CHUNK, half), F32),
        pltpu.VMEM((EDGES_OWN, FEAT), BF16),
        pltpu.VMEM((8, EDGES_OWN), F32),
        pltpu.VMEM((2, 8, EDGES_OWN), F32),
        pltpu.VMEM((EDGES_OWN, 2 * FEAT), BF16),
        pltpu.VMEM((NODES_OWN + WINDOW, 2 * FEAT), F32),
        pltpu.SemaphoreType.DMA((NODE_CHUNKS + 2,)),
        pltpu.VMEM((NODES_OWN, FEAT), F32),
        pltpu.VMEM((COPIES, 2, FEAT), F32),
        pltpu.VMEM((NODES_OWN, FEAT), BF16),
        pltpu.VMEM((FEAT, FEAT), BF16),
        pltpu.VMEM((LAYERS, FEAT), BF16),
        pltpu.VMEM((8, EDGES_OWN), F32),
        pltpu.VMEM((8, EDGES_OWN), jnp.int32),
        pltpu.SMEM((1, EDGES_OWN), jnp.int32),
        pltpu.VMEM((8, EDGES_OWN), F32),
        pltpu.SMEM((1, 32), jnp.int32),
    ]
    if layer > 0:
        scratch += [pltpu.VMEM((2, FEAT), F32)]
        scratch += [pltpu.VMEM((LAYERS, FEAT), BF16)] * 2
    return call(
        functools.partial(edge_kernel, layer, total_nodes, layer > 0, with_send),
        "edge_part",
        outs,
        scratch,
        5 * GIGA,
        args,
        in_specs=[HBM] * len(args),
        out_specs=[HBM] * len(outs),
    )


def deliver(rows):
    return lax.all_to_all(
        rows.reshape(-1, 8, rows.shape[1]), GRP_BLK, split_axis=0, concat_axis=0, tiled=True
    ).reshape(rows.shape)


def shifted(value, axis, amount):
    size = lax.axis_size(axis)
    return lax.ppermute(value, axis, [(i, (i + amount) % size) for i in range(size)])


def copies_summed(copies, axes):
    return jnp.sum(lax.all_to_all(copies, axes, 0, 0, tiled=True), axis=0)


def total_along(copies):
    return copies_summed(copies, ("blk_0",))


def total_inside(stats):
    stats = stats + shifted(stats, "blk_2", 1)
    for axis in ("blk_1", "grp"):
        stats = stats + (
            shifted(stats, axis, 1) + shifted(stats, axis, 2) + shifted(stats, axis, 3)
        )
    return stats


def total_alone(copies):
    stats = copies_summed(copies, ("blk_0",))
    stats = stats + shifted(stats, "blk_2", 1)
    axes = ("grp", "blk_1")
    copies = jnp.broadcast_to(stats[None], (lax.axis_size(axes),) + stats.shape)
    return copies_summed(copies, axes)


def local(
    features,
    source_index,
    target_index,
    edge_valid,
    edge_bias,
    send_list,
    w_left,
    w_right,
    w_skip,
    attn_vec,
    norm_gain,
    norm_shift,
    peers,
):
    total_nodes = float(features.shape[0] * peers)
    row = (1, EDGES_OWN)
    sent = send_rows(send_list, features)
    received = deliver(sent)
    rows, srcs, bias, noedge, bound = sort_edges(
        source_index.reshape(row), target_index.reshape(row), edge_valid.reshape(row), edge_bias
    )
    weights = [w_left, w_right, w_skip, attn_vec, rows, bound]
    left, base, dst, own = own_part(0, total_nodes, [features] + weights)
    edges = [rows, srcs, bias, bound]
    summed, stats, rounded = edge_part(
        0,
        total_nodes,
        True,
        [received, left, dst, noedge, base, w_left, attn_vec, own] + edges,
    )
    stats = total_along(stats)
    sent = send_rows(send_list, rounded)
    sent, stats = lax.optimization_barrier((sent, stats))
    received = deliver(sent)
    stats = total_inside(stats)
    norms = [stats, norm_gain, norm_shift]
    left, base, dst, own = own_part(1, total_nodes, [summed] + norms + weights)
    summed, stats = edge_part(
        1,
        total_nodes,
        False,
        [received, left, dst, noedge, base, w_left, attn_vec, own] + edges + norms,
    )
    stats = total_alone(stats)
    terms = norm_terms(stats, total_nodes, norm_gain[1:2].astype(F32), norm_shift[1:2].astype(F32))
    return normalize(summed, terms)


def solution(mesh):
    split = Mesh(
        mesh.devices.reshape(mesh.shape["grp"], 8, 4, 2), ("grp", "blk_0", "blk_1", "blk_2")
    )
    edge = P(GRP_BLK, None)
    in_specs = (edge,) * 4 + (P(None, GRP_BLK), edge) + (P(),) * 6
    return jax.shard_map(
        functools.partial(local, peers=mesh.size),
        mesh=split,
        in_specs=in_specs,
        out_specs=edge,
        check_vma=False,
    )
```

```python
import functools

import jax
import jax.numpy as jnp
from jax import lax
from jax.experimental import pallas as pl
from jax.experimental.pallas import tpu as pltpu
from jax.sharding import Mesh
from jax.sharding import PartitionSpec as P

HEADS = 8
LAYERS = 2
GRP_BLK = ("grp", "blk_0", "blk_1", "blk_2")
NODES_OWN = 1024
EDGES_OWN = 2048
ROWS_IN = 2048
FEAT = 256
CHUNK = 256
EDGE_CHUNKS = EDGES_OWN // CHUNK
NODE_CHUNKS = NODES_OWN // CHUNK
WINDOW = 160
COPIES = 8
TABLE_ROWS = NODES_OWN + ROWS_IN
F32 = jnp.float32
BF16 = jnp.bfloat16


def iota(shape, dim):
    return lax.broadcasted_iota(jnp.int32, shape, dim)


def one_hot(mask):
    return jnp.where(mask, 1.0, 0.0).astype(BF16)


def dot(lhs, rhs):
    return jnp.dot(lhs, rhs, preferred_element_type=F32)


def dot_t(lhs, rhs):
    return lax.dot_general(lhs, rhs, (((1,), (1,)), ((), ())), preferred_element_type=F32)


def leaky(values):
    return jnp.where(values > 0, values, 0.2 * values)


def split_two(values):
    high = values.astype(BF16)
    return high, (values - high.astype(F32)).astype(BF16)


def split_three(values):
    high = values.astype(BF16)
    rest = values - high.astype(F32)
    mid = rest.astype(BF16)
    return high, mid, (rest - mid.astype(F32)).astype(BF16)


def head_rows(attn_ref, layer):
    shape = (16, FEAT)
    owner = iota(shape, 1) // (FEAT // HEADS) == iota(shape, 0)
    row = attn_ref[layer : layer + 1, :].astype(F32)
    return jnp.where(owner, row, 0.0).astype(BF16)


def head_spread():
    shape = (16, 2 * FEAT)
    return one_hot(iota(shape, 1) // (FEAT // HEADS) == iota(shape, 0))


def scores_of(heads, hidden):
    high, low = split_two(hidden)
    return (dot_t(heads, high) + dot_t(heads, low))[:HEADS]


def norm_terms(stats, total_nodes, gain, shift):
    mean = stats[0:1, :] / total_nodes
    spread = jnp.maximum(stats[1:2, :] / total_nodes - mean * mean, 0.0)
    return mean, lax.rsqrt(spread + 0.1), gain, shift


def normalize(values, terms):
    mean, inv, gain, shift = terms
    scaled = (values - mean) * inv * gain + shift
    grown = jnp.exp(jnp.minimum(scaled, 0.0)) - 1.0
    return jnp.where(scaled > 0, scaled, grown).astype(BF16)


def columns_of(row):
    return jnp.transpose(jnp.broadcast_to(row, (8, row.shape[1])))


def put_rows(pairs_ref, first, values):
    half = FEAT // 2
    pairs_ref[pl.ds(2 * first, CHUNK, stride=2), :] = values[:, :half]
    pairs_ref[pl.ds(2 * first + 1, CHUNK, stride=2), :] = values[:, half:]


def get_rows(pairs_ref):
    return jnp.concatenate(
        [pairs_ref[pl.ds(0, CHUNK, stride=2), :], pairs_ref[pl.ds(1, CHUNK, stride=2), :]], axis=1
    )


def fetch_rows(index_ref, first, pairs_ref, got_ref, scale):
    for e in range(CHUNK):
        row = pl.multiple_of(index_ref[0, first + e] * scale, 2)
        got_ref[2 * e : 2 * e + 2, :] = pairs_ref[pl.ds(row, 2), :]


def send_kernel(index_ref, list_ref, table_ref, out_hbm, pairs_ref, got_ref, out_ref, sems):
    for k in range(NODE_CHUNKS):
        put_rows(pairs_ref, k * CHUNK, table_ref[k * CHUNK : (k + 1) * CHUNK, :].astype(F32))

    def store(c):
        at = slice(c * 2 * CHUNK, (c + 1) * 2 * CHUNK)
        return pltpu.make_async_copy(out_ref.at[at], out_hbm.at[at], sems.at[c])

    count = ROWS_IN // (2 * CHUNK)
    for c in range(count):
        here = slice(c * 2 * CHUNK, c * 2 * CHUNK + CHUNK)
        after = slice(c * 2 * CHUNK + CHUNK, (c + 1) * 2 * CHUNK)
        fetch_rows(index_ref, c * 2 * CHUNK + CHUNK, pairs_ref, got_ref, 2)
        col = columns_of(list_ref[0:1, here].astype(F32)).astype(jnp.int32)[:, 0:1]
        hot = one_hot(col == iota((CHUNK, NODES_OWN), 1))
        out_ref[here, :] = dot(hot, table_ref[...]).astype(BF16)
        out_ref[after, :] = get_rows(got_ref).astype(BF16)
        store(c).start()
    for c in range(count):
        store(c).wait()


def sort_kernel(
    src_ref, tgt_ref, valid_ref, bias_ref, rows_ref, srcs_ref, bias_out, noedge_ref, bound_ref,
    key_ref, pos_ref, meta_ref,
):
    width = (1, EDGES_OWN)
    live_in = valid_ref[...] > 0
    src = src_ref[...]
    tgt = jnp.where(live_in, tgt_ref[...], NODES_OWN)
    key = tgt * EDGES_OWN + iota(width, 1)
    key_ref[...] = columns_of(key.astype(F32)).astype(jnp.int32)
    pos_ref[...] = jnp.zeros_like(pos_ref)

    def rank(c, carry):
        at = pl.ds(pl.multiple_of(c * CHUNK, CHUNK), CHUNK)
        less = jnp.where(key_ref[at, 0:1] < key, 1.0, 0.0)
        pos_ref[...] += jnp.sum(less, axis=0, keepdims=True)
        return carry

    lax.fori_loop(0, EDGE_CHUNKS, rank, 0)
    pos = pos_ref[...].astype(jnp.int32)
    sub = iota((8, EDGES_OWN), 0)
    ints = jnp.where(
        sub == 0,
        src // 256,
        jnp.where(sub == 1, src % 256, jnp.where(sub == 2, tgt // 256, tgt % 256)),
    )
    high, mid, low = split_three(bias_ref[...])
    meta = jnp.concatenate(
        [ints.astype(F32), high.astype(F32), mid.astype(F32), low.astype(F32)], axis=0
    ).astype(BF16)

    def place(c, carry):
        at = pl.ds(pl.multiple_of(c * CHUNK, CHUNK), CHUNK)
        perm = one_hot(pos == iota((CHUNK, EDGES_OWN), 0) + c * CHUNK)
        meta_ref[:, at] = dot_t(meta, perm)
        return carry

    lax.fori_loop(0, EDGE_CHUNKS, place, 0)
    placed = meta_ref[...]
    bias_out[...] = placed[8:16] + placed[16:24] + placed[24:32]
    src_s = (placed[0:1] * 256.0 + placed[1:2]).astype(jnp.int32)
    tgt_s = (placed[2:3] * 256.0 + placed[3:4]).astype(jnp.int32)
    lane8 = iota((8, EDGES_OWN), 1)
    srcs_ref[...] = 2 * src_s
    tgt8 = jnp.broadcast_to(tgt_s, (8, EDGES_OWN))
    before = pltpu.roll(tgt8, 1, 1)
    after = pltpu.roll(tgt8, EDGES_OWN - 1, 1)
    live = tgt8 < NODES_OWN
    first = (lane8 == 0) | (before != tgt8)
    last = (lane8 == EDGES_OWN - 1) | (after != tgt8)
    start = jnp.where(first, lane8, 0)
    end = jnp.where(last, lane8, EDGES_OWN)
    step = 1
    while step < EDGES_OWN:
        start = jnp.maximum(start, jnp.where(lane8 >= step, pltpu.roll(start, step, 1), 0))
        shifted = pltpu.roll(end, EDGES_OWN - step, 1)
        end = jnp.minimum(end, jnp.where(lane8 + step < EDGES_OWN, shifted, EDGES_OWN))
        step *= 2
    start = jnp.where(live, start, lane8)
    end = jnp.where(live, end, lane8)
    rows_ref[...] = jnp.where(
        sub == 0, tgt8, jnp.where(sub == 1, start, jnp.where(sub == 2, end, lane8))
    )
    bound_ref[0, 2 * EDGE_CHUNKS] = jnp.max(end - start) + 1
    for c in range(EDGE_CHUNKS):
        piece = tgt8[:, c * CHUNK : (c + 1) * CHUNK]
        bound_ref[0, 2 * c] = jnp.min(piece)
        bound_ref[0, 2 * c + 1] = jnp.max(jnp.where(piece < NODES_OWN, piece, -1))
    for k in range(NODE_CHUNKS):
        hit = jnp.where(iota((CHUNK, EDGES_OWN), 0) + k * CHUNK == tgt_s, 1.0, 0.0)
        found = jnp.max(hit, axis=1, keepdims=True)
        noedge_ref[k * CHUNK : (k + 1) * CHUNK, :] = jnp.broadcast_to(1.0 - found, (CHUNK, 8))


def own_kernel(layer, total_nodes, with_norm, *refs):
    refs = list(refs)
    state_ref = refs.pop(0)
    if with_norm:
        stats_ref, gain_ref, shift_ref = refs[:3]
        refs = refs[3:]
        terms = norm_terms(
            stats_ref[...],
            total_nodes,
            gain_ref[layer - 1 : layer, :].astype(F32),
            shift_ref[layer - 1 : layer, :].astype(F32),
        )
    wl_ref, wr_ref, ws_ref, attn_ref, rows_ref, bound_ref = refs[:6]
    left_out, base_out, dst_hbm, self_out = refs[6:10]
    table_ref, acc_ref, own_ref, left_ref, base_ref, dst_out, sems = refs[10:]
    loads = []
    for k in range(NODE_CHUNKS):
        at = slice(k * CHUNK, (k + 1) * CHUNK)
        loads.append(pltpu.make_async_copy(state_ref.at[at], own_ref.at[at], sems.at[k]))
        loads[-1].start()
    stores = [
        pltpu.make_async_copy(left_ref, left_out, sems.at[NODE_CHUNKS]),
        pltpu.make_async_copy(base_ref, base_out, sems.at[NODE_CHUNKS + 1]),
        pltpu.make_async_copy(dst_out, dst_hbm, sems.at[NODE_CHUNKS + 2]),
    ]
    heads = head_rows(attn_ref, layer)
    for k in range(NODE_CHUNKS):
        at = slice(k * CHUNK, (k + 1) * CHUNK)
        loads[k].wait()
        states = own_ref[at, :]
        if with_norm:
            states = normalize(states, terms)
        left = dot(states, wl_ref[layer]).astype(BF16)
        right = dot(states, wr_ref[layer]).astype(BF16)
        left_ref[at, :] = left
        table_ref[at, :FEAT] = right
        base_ref[at, :] = states.astype(F32) + dot(states, ws_ref[layer])
        own = scores_of(heads, leaky(left.astype(F32) + right.astype(F32)))
        high, mid, low = split_three(own)
        parts = [high.astype(F32), mid.astype(F32), low.astype(F32)]
        parts += [jnp.zeros((128 - 3 * HEADS, CHUNK), F32)]
        table_ref[at, FEAT:] = jnp.transpose(jnp.concatenate(parts, axis=0)).astype(BF16)
    table_ref[NODES_OWN:, :] = jnp.zeros((CHUNK, FEAT + 128), BF16)
    stores[0].start()
    stores[1].start()

    def step(c, carry):
        at = pl.ds(pl.multiple_of(c * CHUNK, CHUNK), CHUNK)
        col = columns_of(rows_ref[0:1, at].astype(F32)).astype(jnp.int32)[:, 0:1]
        low = lax.div(bound_ref[0, 2 * c], 16) * 16
        extra = lax.div(jnp.maximum(bound_ref[0, 2 * c + 1] - low, 0), CHUNK)

        def window(w):
            base = pl.multiple_of(jnp.minimum(low + w * CHUNK, NODES_OWN), 16)
            hot = one_hot(col - base == iota((CHUNK, CHUNK), 1))
            return dot(hot, table_ref[pl.ds(base, CHUNK), :])

        acc_ref[...] = window(0)

        def more(w, carry):
            acc_ref[...] += window(w)
            return carry

        lax.fori_loop(1, extra + 1, more, 0)
        dst_out[at, :] = acc_ref[:, :FEAT].astype(BF16)
        back = jnp.transpose(acc_ref[:, FEAT:])
        self_out[:, at] = back[0:8] + back[8:16] + back[16:24]
        return carry

    lax.fori_loop(0, EDGE_CHUNKS, step, 0, unroll=2)
    stores[2].start()
    for store in stores:
        store.wait()


def scan_both(ref, longest, lane, start, end, join, neutral, values):
    def advance(ahead, back, step):
        moved = pltpu.roll(ahead, step, 1)
        ahead = join(ahead, jnp.where(lane - step >= start, moved, neutral))
        moved = pltpu.roll(back, EDGES_OWN - step, 1)
        return ahead, join(back, jnp.where(lane + step <= end, moved, neutral))

    ahead, back = values, values
    for step in (1, 2, 4, 8):
        ahead, back = advance(ahead, back, step)
    ref[0] = ahead
    ref[1] = back

    def rest():
        step = 16
        while step < EDGES_OWN:
            ref[0], ref[1] = advance(ref[0], ref[1], step)
            step *= 2

    pl.when(longest > 16)(rest)
    return ref[0], ref[1]


def edge_kernel(layer, total_nodes, with_norm, with_send, *refs):
    refs = list(refs)
    recv_any, left_any, dst_any, noedge_any, base_any = refs[:5]
    small = 10 if with_norm else 7
    small_any = refs[5 : 5 + small]
    refs = refs[5 + small :]
    summed_hbm, stats_hbm = refs[:2]
    refs = refs[2:]
    if with_send:
        round_hbm = refs.pop(0)
    recv_ref, left_ref, dst_ref, noedge_ref, base_ref, sems = refs[:6]
    table_ref, even_ref, odd_ref, edge_ref, score_ref, scan_ref, mix_ref, acc_ref = refs[6:14]
    out_sems, summed_ref, stats_ref, round_ref = refs[14:18]
    small_refs = refs[18:]
    wl_ref, attn_ref, self_ref, rows_ref, srcs_ref, bias_ref, bound_ref = small_refs[:7]
    piece = ROWS_IN // 4
    pieces = [slice(k * piece, (k + 1) * piece) for k in range(4)]
    moves = [(small_any[0].at[layer], wl_ref), (recv_any.at[pieces[0]], recv_ref.at[pieces[0]])]
    moves += list(zip(small_any[7:], small_refs[7:]))
    moves += [(recv_any.at[at], recv_ref.at[at]) for at in pieces[1:]]
    moves += [(small_any[4], srcs_ref), (left_any, left_ref), (small_any[1], attn_ref)]
    moves += [(dst_any, dst_ref), (small_any[3], rows_ref), (small_any[6], bound_ref)]
    moves += [(small_any[2], self_ref), (small_any[5], bias_ref)]
    moves += [(noedge_any, noedge_ref), (base_any, base_ref)]
    copies = [
        pltpu.make_async_copy(source, target, sems.at[i])
        for i, (source, target) in enumerate(moves)
    ]
    for copy in copies:
        copy.start()
    waiting = iter(copies)

    def settle(count):
        for _ in range(count):
            next(waiting).wait()

    if with_norm:
        stats_in, gain_ref, shift_ref = small_refs[7:]
        settle(5)
        terms = norm_terms(
            stats_in[...],
            total_nodes,
            gain_ref[layer - 1 : layer, :].astype(F32),
            shift_ref[layer - 1 : layer, :].astype(F32),
        )
    else:
        settle(2)
    for c in range(ROWS_IN // CHUNK):
        if c and c * CHUNK % piece == 0:
            settle(1)
        states = recv_ref[c * CHUNK : (c + 1) * CHUNK, :]
        if with_norm:
            states = normalize(states.astype(F32), terms)
        left = dot(states, wl_ref[...]).astype(BF16).astype(F32)
        put_rows(table_ref, NODES_OWN + c * CHUNK, left)
    settle(3)
    heads = head_rows(attn_ref, layer)
    for k in range(NODE_CHUNKS):
        put_rows(table_ref, k * CHUNK, left_ref[k * CHUNK : (k + 1) * CHUNK, :].astype(F32))

    def fetch(c, out_ref):
        fetch_rows(srcs_ref, c * CHUNK, table_ref, out_ref, 1)

    def score(c, in_ref):
        at = slice(c * CHUNK, (c + 1) * CHUNK)
        src = get_rows(in_ref)
        edge_ref[at, :] = src.astype(BF16)
        score_ref[:, at] = scores_of(heads, leaky(src + dst_ref[at, :].astype(F32)))

    fetch(0, even_ref)
    settle(1)

    for c in range(EDGE_CHUNKS // 2):
        fetch(2 * c + 1, odd_ref)
        score(2 * c, even_ref)
        if 2 * c + 2 < EDGE_CHUNKS:
            fetch(2 * c + 2, even_ref)
        score(2 * c + 1, odd_ref)

    settle(4)
    tgt = rows_ref[0:1, :]
    start = rows_ref[1:2, :]
    end = rows_ref[2:3, :]
    lane = iota((8, EDGES_OWN), 1)
    live = tgt < NODES_OWN
    longest = bound_ref[0, 2 * EDGE_CHUNKS]
    scores = jnp.where(live, score_ref[...] + bias_ref[...], -1e30)
    own = self_ref[...]
    ahead, back = scan_both(scan_ref, longest, lane, start, end, jnp.maximum, -1e30, scores)
    top = jnp.maximum(jnp.maximum(ahead, back), own)
    weights = jnp.where(live, jnp.exp(scores - top), 0.0)
    own_weights = jnp.exp(own - top)
    ahead, back = scan_both(scan_ref, longest, lane, start, end, jnp.add, 0.0, weights)
    denom = own_weights + (ahead + (back - weights))
    last = live & (lane == end)
    score_ref[...] = weights / denom
    scan_ref[0] = jnp.where(last, own_weights / denom, 0.0)
    spread = head_spread()

    def mix(c, carry):
        at = pl.ds(pl.multiple_of(c * CHUNK, CHUNK), CHUNK)
        pair = jnp.concatenate([score_ref[:, at], scan_ref[0, :, at]], axis=0)
        wide = dot(jnp.transpose(pair).astype(BF16), spread)
        mix_ref[at, :FEAT] = (wide[:, :FEAT] * edge_ref[at, :].astype(F32)).astype(BF16)
        mix_ref[at, FEAT:] = wide[:, FEAT:].astype(BF16)
        return carry

    lax.fori_loop(0, EDGE_CHUNKS, mix, 0, unroll=4)
    acc_ref[...] = jnp.zeros_like(acc_ref)

    def gather_in(c, carry):
        here = pl.ds(pl.multiple_of(c * CHUNK, CHUNK), CHUNK)
        low = lax.div(bound_ref[0, 2 * c], 8) * 8
        count = lax.div(jnp.maximum(bound_ref[0, 2 * c + 1] - low + WINDOW, 0), WINDOW)

        def window(w, carry):
            first = pl.multiple_of(low + w * WINDOW, 8)
            hot = one_hot(iota((WINDOW, CHUNK), 0) + first == rows_ref[0:1, here])
            acc_ref[pl.ds(first, WINDOW), :] += dot(hot, mix_ref[here, :])
            return carry

        return lax.fori_loop(0, count, window, carry)

    lax.fori_loop(0, EDGE_CHUNKS, gather_in, 0)
    settle(2)
    totals = jnp.zeros((2, FEAT), F32)
    stores = []
    for k in range(NODE_CHUNKS):
        at = slice(k * CHUNK, (k + 1) * CHUNK)
        own_alpha = jnp.where(noedge_ref[at, 0:1] > 0, 1.0, acc_ref[at, FEAT:])
        message = acc_ref[at, :FEAT] + own_alpha * left_ref[at, :].astype(F32)
        summed = base_ref[at, :] + message
        summed_ref[at, :] = summed
        sums = [jnp.sum(summed, axis=0, keepdims=True)]
        sums += [jnp.sum(summed * summed, axis=0, keepdims=True)]
        totals += jnp.concatenate(sums, axis=0)
        if with_send:
            round_ref[at, :] = summed.astype(BF16)
        store = pltpu.make_async_copy(summed_ref.at[at], summed_hbm.at[at], out_sems.at[k])
        store.start()
        stores.append(store)
    for k in range(COPIES):
        stats_ref[k] = totals
    stores.append(pltpu.make_async_copy(stats_ref, stats_hbm, out_sems.at[NODE_CHUNKS]))
    stores[-1].start()
    if with_send:
        stores.append(pltpu.make_async_copy(round_ref, round_hbm, out_sems.at[NODE_CHUNKS + 1]))
        stores[-1].start()
    for store in stores:
        store.wait()


def shaped(rows, cols, dtype):
    return jax.ShapeDtypeStruct((rows, cols), dtype)


SMEM = pl.BlockSpec(memory_space=pltpu.SMEM)
VMEM = pl.BlockSpec(memory_space=pltpu.VMEM)
ANY = pl.BlockSpec(memory_space=pl.ANY)
HBM = pl.BlockSpec(memory_space=pltpu.HBM)


def call(body, name, outs, scratch, flops, args, in_specs=None, out_specs=None):
    cost = pl.CostEstimate(flops=flops, bytes_accessed=4 << 20, transcendentals=0)
    return pl.pallas_call(
        body,
        name=name,
        out_shape=outs,
        in_specs=in_specs or [VMEM] * len(args),
        out_specs=out_specs or [VMEM] * len(outs),
        scratch_shapes=scratch,
        cost_estimate=cost,
        compiler_params=pltpu.CompilerParams(vmem_limit_bytes=67_000_000),
    )(*args)


GIGA = 1 << 30


def send_rows(send_list, table):
    return call(
        send_kernel,
        "send_rows",
        [shaped(ROWS_IN, FEAT, BF16)],
        [
            pltpu.VMEM((2 * NODES_OWN, FEAT // 2), F32),
            pltpu.VMEM((2 * CHUNK, FEAT // 2), F32),
            pltpu.VMEM((ROWS_IN, FEAT), BF16),
            pltpu.SemaphoreType.DMA((ROWS_IN // (2 * CHUNK),)),
        ],
        GIGA,
        [send_list, send_list, table],
        in_specs=[SMEM, VMEM, VMEM],
        out_specs=[HBM],
    )[0]


def sort_edges(sources, targets, valids, bias):
    return call(
        sort_kernel,
        "sort_edges",
        [
            shaped(8, EDGES_OWN, jnp.int32),
            shaped(1, EDGES_OWN, jnp.int32),
            shaped(8, EDGES_OWN, F32),
            shaped(NODES_OWN, 8, F32),
            shaped(1, 32, jnp.int32),
        ],
        [
            pltpu.VMEM((EDGES_OWN, 8), jnp.int32),
            pltpu.VMEM((1, EDGES_OWN), F32),
            pltpu.VMEM((32, EDGES_OWN), F32),
        ],
        2 * GIGA,
        [sources, targets, valids, bias],
        out_specs=[VMEM, VMEM, VMEM, VMEM, SMEM],
    )


def own_part(layer, total_nodes, args):
    in_specs = [VMEM] * len(args)
    in_specs[0] = HBM
    in_specs[-1] = SMEM
    return call(
        functools.partial(own_kernel, layer, total_nodes, layer > 0),
        "own_part",
        [
            shaped(NODES_OWN, FEAT, BF16),
            shaped(NODES_OWN, FEAT, F32),
            shaped(EDGES_OWN, FEAT, BF16),
            shaped(8, EDGES_OWN, F32),
        ],
        [
            pltpu.VMEM((NODES_OWN + CHUNK, FEAT + 128), BF16),
            pltpu.VMEM((CHUNK, FEAT + 128), F32),
            pltpu.VMEM((NODES_OWN, FEAT), args[0].dtype),
            pltpu.VMEM((NODES_OWN, FEAT), BF16),
            pltpu.VMEM((NODES_OWN, FEAT), F32),
            pltpu.VMEM((EDGES_OWN, FEAT), BF16),
            pltpu.SemaphoreType.DMA((NODE_CHUNKS + 3,)),
        ],
        3 * GIGA,
        args,
        in_specs=in_specs,
        out_specs=[HBM, HBM, HBM, VMEM],
    )


def edge_part(layer, total_nodes, with_send, args):
    outs = [
        shaped(NODES_OWN, FEAT, F32),
        jax.ShapeDtypeStruct((COPIES, 2, FEAT), F32),
    ]
    if with_send:
        outs.append(shaped(NODES_OWN, FEAT, BF16))
    half = FEAT // 2
    scratch = [
        pltpu.VMEM((ROWS_IN, FEAT), BF16),
        pltpu.VMEM((NODES_OWN, FEAT), BF16),
        pltpu.VMEM((EDGES_OWN, FEAT), BF16),
        pltpu.VMEM((NODES_OWN, 8), F32),
        pltpu.VMEM((NODES_OWN, FEAT), F32),
        pltpu.SemaphoreType.DMA((len(args) + 3,)),
        pltpu.VMEM((2 * TABLE_ROWS, half), F32),
        pltpu.VMEM((2 * CHUNK, half), F32),
        pltpu.VMEM((2 * CHUNK, half), F32),
        pltpu.VMEM((EDGES_OWN, FEAT), BF16),
        pltpu.VMEM((8, EDGES_OWN), F32),
        pltpu.VMEM((2, 8, EDGES_OWN), F32),
        pltpu.VMEM((EDGES_OWN, 2 * FEAT), BF16),
        pltpu.VMEM((NODES_OWN + WINDOW, 2 * FEAT), F32),
        pltpu.SemaphoreType.DMA((NODE_CHUNKS + 2,)),
        pltpu.VMEM((NODES_OWN, FEAT), F32),
        pltpu.VMEM((COPIES, 2, FEAT), F32),
        pltpu.VMEM((NODES_OWN, FEAT), BF16),
        pltpu.VMEM((FEAT, FEAT), BF16),
        pltpu.VMEM((LAYERS, FEAT), BF16),
        pltpu.VMEM((8, EDGES_OWN), F32),
        pltpu.VMEM((8, EDGES_OWN), jnp.int32),
        pltpu.SMEM((1, EDGES_OWN), jnp.int32),
        pltpu.VMEM((8, EDGES_OWN), F32),
        pltpu.SMEM((1, 32), jnp.int32),
    ]
    if layer > 0:
        scratch += [pltpu.VMEM((2, FEAT), F32)]
        scratch += [pltpu.VMEM((LAYERS, FEAT), BF16)] * 2
    return call(
        functools.partial(edge_kernel, layer, total_nodes, layer > 0, with_send),
        "edge_part",
        outs,
        scratch,
        5 * GIGA,
        args,
        in_specs=[HBM] * len(args),
        out_specs=[HBM] * len(outs),
    )


def deliver(rows):
    return lax.all_to_all(
        rows.reshape(-1, 8, rows.shape[1]), GRP_BLK, split_axis=0, concat_axis=0, tiled=True
    ).reshape(rows.shape)


def shifted(value, axis, amount):
    size = lax.axis_size(axis)
    return lax.ppermute(value, axis, [(i, (i + amount) % size) for i in range(size)])


def copies_summed(copies, axes):
    return jnp.sum(lax.all_to_all(copies, axes, 0, 0, tiled=True), axis=0)


def total_along(copies):
    return copies_summed(copies, ("blk_0",))


def total_inside(stats):
    stats = stats + shifted(stats, "blk_2", 1)
    for axis in ("blk_1", "grp"):
        stats = stats + (
            shifted(stats, axis, 1) + shifted(stats, axis, 2) + shifted(stats, axis, 3)
        )
    return stats


def total_alone(copies):
    stats = copies_summed(copies, ("blk_1", "blk_2"))
    axes = ("grp", "blk_0")
    copies = jnp.broadcast_to(stats[None], (lax.axis_size(axes),) + stats.shape)
    return copies_summed(copies, axes)


def local(
    features,
    source_index,
    target_index,
    edge_valid,
    edge_bias,
    send_list,
    w_left,
    w_right,
    w_skip,
    attn_vec,
    norm_gain,
    norm_shift,
    peers,
):
    total_nodes = float(features.shape[0] * peers)
    row = (1, EDGES_OWN)
    sent = send_rows(send_list, features)
    received = deliver(sent)
    rows, srcs, bias, noedge, bound = sort_edges(
        source_index.reshape(row), target_index.reshape(row), edge_valid.reshape(row), edge_bias
    )
    weights = [w_left, w_right, w_skip, attn_vec, rows, bound]
    left, base, dst, own = own_part(0, total_nodes, [features] + weights)
    edges = [rows, srcs, bias, bound]
    summed, stats, rounded = edge_part(
        0,
        total_nodes,
        True,
        [received, left, dst, noedge, base, w_left, attn_vec, own] + edges,
    )
    stats = total_along(stats)
    sent = send_rows(send_list, rounded)
    sent, stats = lax.optimization_barrier((sent, stats))
    received = deliver(sent)
    stats = total_inside(stats)
    norms = [stats, norm_gain, norm_shift]
    left, base, dst, own = own_part(1, total_nodes, [summed] + norms + weights)
    summed, stats = edge_part(
        1,
        total_nodes,
        False,
        [received, left, dst, noedge, base, w_left, attn_vec, own] + edges + norms,
    )
    stats = total_alone(stats)
    terms = norm_terms(stats, total_nodes, norm_gain[1:2].astype(F32), norm_shift[1:2].astype(F32))
    return normalize(summed, terms)


def solution(mesh):
    split = Mesh(
        mesh.devices.reshape(mesh.shape["grp"], 8, 4, 2), ("grp", "blk_0", "blk_1", "blk_2")
    )
    edge = P(GRP_BLK, None)
    in_specs = (edge,) * 4 + (P(None, GRP_BLK), edge) + (P(),) * 6
    return jax.shard_map(
        functools.partial(local, peers=mesh.size),
        mesh=split,
        in_specs=in_specs,
        out_specs=edge,
        check_vma=False,
    )
```

```python
import functools

import jax
import jax.numpy as jnp
from jax import lax
from jax.experimental import pallas as pl
from jax.experimental.pallas import tpu as pltpu
from jax.sharding import Mesh
from jax.sharding import PartitionSpec as P

HEADS = 8
LAYERS = 2
GRP_BLK = ("grp", "blk_0", "blk_1", "blk_2")
NODES_OWN = 1024
EDGES_OWN = 2048
ROWS_IN = 2048
FEAT = 256
CHUNK = 256
EDGE_CHUNKS = EDGES_OWN // CHUNK
NODE_CHUNKS = NODES_OWN // CHUNK
WINDOW = 160
COPIES = 8
TABLE_ROWS = NODES_OWN + ROWS_IN
F32 = jnp.float32
BF16 = jnp.bfloat16


def iota(shape, dim):
    return lax.broadcasted_iota(jnp.int32, shape, dim)


def one_hot(mask):
    return jnp.where(mask, 1.0, 0.0).astype(BF16)


def dot(lhs, rhs):
    return jnp.dot(lhs, rhs, preferred_element_type=F32)


def dot_t(lhs, rhs):
    return lax.dot_general(lhs, rhs, (((1,), (1,)), ((), ())), preferred_element_type=F32)


def leaky(values):
    return jnp.where(values > 0, values, 0.2 * values)


def split_two(values):
    high = values.astype(BF16)
    return high, (values - high.astype(F32)).astype(BF16)


def split_three(values):
    high = values.astype(BF16)
    rest = values - high.astype(F32)
    mid = rest.astype(BF16)
    return high, mid, (rest - mid.astype(F32)).astype(BF16)


def head_rows(attn_ref, layer):
    shape = (16, FEAT)
    owner = iota(shape, 1) // (FEAT // HEADS) == iota(shape, 0)
    row = attn_ref[layer : layer + 1, :].astype(F32)
    return jnp.where(owner, row, 0.0).astype(BF16)


def head_spread():
    shape = (16, 2 * FEAT)
    return one_hot(iota(shape, 1) // (FEAT // HEADS) == iota(shape, 0))


def scores_of(heads, hidden):
    high, low = split_two(hidden)
    return (dot_t(heads, high) + dot_t(heads, low))[:HEADS]


def norm_terms(stats, total_nodes, gain, shift):
    mean = stats[0:1, :] / total_nodes
    spread = jnp.maximum(stats[1:2, :] / total_nodes - mean * mean, 0.0)
    return mean, lax.rsqrt(spread + 0.1), gain, shift


def normalize(values, terms):
    mean, inv, gain, shift = terms
    scaled = (values - mean) * inv * gain + shift
    grown = jnp.exp(jnp.minimum(scaled, 0.0)) - 1.0
    return jnp.where(scaled > 0, scaled, grown).astype(BF16)


def columns_of(row):
    return jnp.transpose(jnp.broadcast_to(row, (8, row.shape[1])))


def put_rows(pairs_ref, first, values):
    half = FEAT // 2
    pairs_ref[pl.ds(2 * first, CHUNK, stride=2), :] = values[:, :half]
    pairs_ref[pl.ds(2 * first + 1, CHUNK, stride=2), :] = values[:, half:]


def get_rows(pairs_ref):
    return jnp.concatenate(
        [pairs_ref[pl.ds(0, CHUNK, stride=2), :], pairs_ref[pl.ds(1, CHUNK, stride=2), :]], axis=1
    )


def fetch_rows(index_ref, first, pairs_ref, got_ref, scale):
    for e in range(CHUNK):
        row = pl.multiple_of(index_ref[0, first + e] * scale, 2)
        got_ref[2 * e : 2 * e + 2, :] = pairs_ref[pl.ds(row, 2), :]


def send_kernel(index_ref, list_ref, table_ref, out_hbm, pairs_ref, got_ref, out_ref, sems):
    for k in range(NODE_CHUNKS):
        put_rows(pairs_ref, k * CHUNK, table_ref[k * CHUNK : (k + 1) * CHUNK, :].astype(F32))

    def store(c):
        at = slice(c * 2 * CHUNK, (c + 1) * 2 * CHUNK)
        return pltpu.make_async_copy(out_ref.at[at], out_hbm.at[at], sems.at[c])

    count = ROWS_IN // (2 * CHUNK)
    for c in range(count):
        here = slice(c * 2 * CHUNK, c * 2 * CHUNK + CHUNK)
        after = slice(c * 2 * CHUNK + CHUNK, (c + 1) * 2 * CHUNK)
        fetch_rows(index_ref, c * 2 * CHUNK + CHUNK, pairs_ref, got_ref, 2)
        col = columns_of(list_ref[0:1, here].astype(F32)).astype(jnp.int32)[:, 0:1]
        hot = one_hot(col == iota((CHUNK, NODES_OWN), 1))
        out_ref[here, :] = dot(hot, table_ref[...]).astype(BF16)
        out_ref[after, :] = get_rows(got_ref).astype(BF16)
        store(c).start()
    for c in range(count):
        store(c).wait()


def sort_kernel(
    src_ref, tgt_ref, valid_ref, bias_ref, rows_ref, srcs_ref, bias_out, noedge_ref, bound_ref,
    key_ref, pos_ref, meta_ref,
):
    width = (1, EDGES_OWN)
    live_in = valid_ref[...] > 0
    src = src_ref[...]
    tgt = jnp.where(live_in, tgt_ref[...], NODES_OWN)
    key = tgt * EDGES_OWN + iota(width, 1)
    key_ref[...] = columns_of(key.astype(F32)).astype(jnp.int32)
    pos_ref[...] = jnp.zeros_like(pos_ref)

    def rank(c, carry):
        at = pl.ds(pl.multiple_of(c * CHUNK, CHUNK), CHUNK)
        less = jnp.where(key_ref[at, 0:1] < key, 1.0, 0.0)
        pos_ref[...] += jnp.sum(less, axis=0, keepdims=True)
        return carry

    lax.fori_loop(0, EDGE_CHUNKS, rank, 0)
    pos = pos_ref[...].astype(jnp.int32)
    sub = iota((8, EDGES_OWN), 0)
    ints = jnp.where(
        sub == 0,
        src // 256,
        jnp.where(sub == 1, src % 256, jnp.where(sub == 2, tgt // 256, tgt % 256)),
    )
    high, mid, low = split_three(bias_ref[...])
    meta = jnp.concatenate(
        [ints.astype(F32), high.astype(F32), mid.astype(F32), low.astype(F32)], axis=0
    ).astype(BF16)

    def place(c, carry):
        at = pl.ds(pl.multiple_of(c * CHUNK, CHUNK), CHUNK)
        perm = one_hot(pos == iota((CHUNK, EDGES_OWN), 0) + c * CHUNK)
        meta_ref[:, at] = dot_t(meta, perm)
        return carry

    lax.fori_loop(0, EDGE_CHUNKS, place, 0)
    placed = meta_ref[...]
    bias_out[...] = placed[8:16] + placed[16:24] + placed[24:32]
    src_s = (placed[0:1] * 256.0 + placed[1:2]).astype(jnp.int32)
    tgt_s = (placed[2:3] * 256.0 + placed[3:4]).astype(jnp.int32)
    lane8 = iota((8, EDGES_OWN), 1)
    srcs_ref[...] = 2 * src_s
    tgt8 = jnp.broadcast_to(tgt_s, (8, EDGES_OWN))
    before = pltpu.roll(tgt8, 1, 1)
    after = pltpu.roll(tgt8, EDGES_OWN - 1, 1)
    live = tgt8 < NODES_OWN
    first = (lane8 == 0) | (before != tgt8)
    last = (lane8 == EDGES_OWN - 1) | (after != tgt8)
    start = jnp.where(first, lane8, 0)
    end = jnp.where(last, lane8, EDGES_OWN)
    step = 1
    while step < EDGES_OWN:
        start = jnp.maximum(start, jnp.where(lane8 >= step, pltpu.roll(start, step, 1), 0))
        shifted = pltpu.roll(end, EDGES_OWN - step, 1)
        end = jnp.minimum(end, jnp.where(lane8 + step < EDGES_OWN, shifted, EDGES_OWN))
        step *= 2
    start = jnp.where(live, start, lane8)
    end = jnp.where(live, end, lane8)
    rows_ref[...] = jnp.where(
        sub == 0, tgt8, jnp.where(sub == 1, start, jnp.where(sub == 2, end, lane8))
    )
    bound_ref[0, 2 * EDGE_CHUNKS] = jnp.max(end - start) + 1
    for c in range(EDGE_CHUNKS):
        piece = tgt8[:, c * CHUNK : (c + 1) * CHUNK]
        bound_ref[0, 2 * c] = jnp.min(piece)
        bound_ref[0, 2 * c + 1] = jnp.max(jnp.where(piece < NODES_OWN, piece, -1))
    for k in range(NODE_CHUNKS):
        hit = jnp.where(iota((CHUNK, EDGES_OWN), 0) + k * CHUNK == tgt_s, 1.0, 0.0)
        found = jnp.max(hit, axis=1, keepdims=True)
        noedge_ref[k * CHUNK : (k + 1) * CHUNK, :] = jnp.broadcast_to(1.0 - found, (CHUNK, 8))


def own_kernel(layer, total_nodes, with_norm, *refs):
    refs = list(refs)
    state_ref = refs.pop(0)
    if with_norm:
        stats_ref, gain_ref, shift_ref = refs[:3]
        refs = refs[3:]
        terms = norm_terms(
            stats_ref[...],
            total_nodes,
            gain_ref[layer - 1 : layer, :].astype(F32),
            shift_ref[layer - 1 : layer, :].astype(F32),
        )
    wl_ref, wr_ref, ws_ref, attn_ref, rows_ref, bound_ref = refs[:6]
    left_out, base_out, dst_hbm, self_out = refs[6:10]
    table_ref, acc_ref, own_ref, left_ref, base_ref, dst_out, sems = refs[10:]
    loads = []
    for k in range(NODE_CHUNKS):
        at = slice(k * CHUNK, (k + 1) * CHUNK)
        loads.append(pltpu.make_async_copy(state_ref.at[at], own_ref.at[at], sems.at[k]))
        loads[-1].start()
    stores = [
        pltpu.make_async_copy(left_ref, left_out, sems.at[NODE_CHUNKS]),
        pltpu.make_async_copy(base_ref, base_out, sems.at[NODE_CHUNKS + 1]),
        pltpu.make_async_copy(dst_out, dst_hbm, sems.at[NODE_CHUNKS + 2]),
    ]
    heads = head_rows(attn_ref, layer)
    for k in range(NODE_CHUNKS):
        at = slice(k * CHUNK, (k + 1) * CHUNK)
        loads[k].wait()
        states = own_ref[at, :]
        if with_norm:
            states = normalize(states, terms)
        left = dot(states, wl_ref[layer]).astype(BF16)
        right = dot(states, wr_ref[layer]).astype(BF16)
        left_ref[at, :] = left
        table_ref[at, :FEAT] = right
        base_ref[at, :] = states.astype(F32) + dot(states, ws_ref[layer])
        own = scores_of(heads, leaky(left.astype(F32) + right.astype(F32)))
        high, mid, low = split_three(own)
        parts = [high.astype(F32), mid.astype(F32), low.astype(F32)]
        parts += [jnp.zeros((128 - 3 * HEADS, CHUNK), F32)]
        table_ref[at, FEAT:] = jnp.transpose(jnp.concatenate(parts, axis=0)).astype(BF16)
    table_ref[NODES_OWN:, :] = jnp.zeros((CHUNK, FEAT + 128), BF16)
    stores[0].start()
    stores[1].start()

    def step(c, carry):
        at = pl.ds(pl.multiple_of(c * CHUNK, CHUNK), CHUNK)
        col = columns_of(rows_ref[0:1, at].astype(F32)).astype(jnp.int32)[:, 0:1]
        low = lax.div(bound_ref[0, 2 * c], 16) * 16
        extra = lax.div(jnp.maximum(bound_ref[0, 2 * c + 1] - low, 0), CHUNK)

        def window(w):
            base = pl.multiple_of(jnp.minimum(low + w * CHUNK, NODES_OWN), 16)
            hot = one_hot(col - base == iota((CHUNK, CHUNK), 1))
            return dot(hot, table_ref[pl.ds(base, CHUNK), :])

        acc_ref[...] = window(0)

        def more(w, carry):
            acc_ref[...] += window(w)
            return carry

        lax.fori_loop(1, extra + 1, more, 0)
        dst_out[at, :] = acc_ref[:, :FEAT].astype(BF16)
        back = jnp.transpose(acc_ref[:, FEAT:])
        self_out[:, at] = back[0:8] + back[8:16] + back[16:24]
        return carry

    lax.fori_loop(0, EDGE_CHUNKS, step, 0, unroll=2)
    stores[2].start()
    for store in stores:
        store.wait()


def scan_both(ref, longest, lane, start, end, join, neutral, values):
    def advance(ahead, back, step):
        moved = pltpu.roll(ahead, step, 1)
        ahead = join(ahead, jnp.where(lane - step >= start, moved, neutral))
        moved = pltpu.roll(back, EDGES_OWN - step, 1)
        return ahead, join(back, jnp.where(lane + step <= end, moved, neutral))

    ahead, back = values, values
    for step in (1, 2, 4, 8):
        ahead, back = advance(ahead, back, step)
    ref[0] = ahead
    ref[1] = back

    def rest():
        step = 16
        while step < EDGES_OWN:
            ref[0], ref[1] = advance(ref[0], ref[1], step)
            step *= 2

    pl.when(longest > 16)(rest)
    return ref[0], ref[1]


def edge_kernel(layer, total_nodes, with_norm, with_send, *refs):
    refs = list(refs)
    recv_any, left_any, dst_any, noedge_any, base_any = refs[:5]
    small = 10 if with_norm else 7
    small_any = refs[5 : 5 + small]
    refs = refs[5 + small :]
    summed_hbm, stats_hbm = refs[:2]
    refs = refs[2:]
    if with_send:
        round_hbm = refs.pop(0)
    recv_ref, left_ref, dst_ref, noedge_ref, base_ref, sems = refs[:6]
    table_ref, even_ref, odd_ref, edge_ref, score_ref, scan_ref, mix_ref, acc_ref = refs[6:14]
    out_sems, summed_ref, stats_ref, round_ref = refs[14:18]
    small_refs = refs[18:]
    wl_ref, attn_ref, self_ref, rows_ref, srcs_ref, bias_ref, bound_ref = small_refs[:7]
    piece = ROWS_IN // 4
    pieces = [slice(k * piece, (k + 1) * piece) for k in range(4)]
    moves = [(small_any[0].at[layer], wl_ref), (recv_any.at[pieces[0]], recv_ref.at[pieces[0]])]
    moves += list(zip(small_any[7:], small_refs[7:]))
    moves += [(recv_any.at[at], recv_ref.at[at]) for at in pieces[1:]]
    moves += [(small_any[4], srcs_ref), (left_any, left_ref), (small_any[1], attn_ref)]
    moves += [(dst_any, dst_ref), (small_any[3], rows_ref), (small_any[6], bound_ref)]
    moves += [(small_any[2], self_ref), (small_any[5], bias_ref)]
    moves += [(noedge_any, noedge_ref), (base_any, base_ref)]
    copies = [
        pltpu.make_async_copy(source, target, sems.at[i])
        for i, (source, target) in enumerate(moves)
    ]
    for copy in copies:
        copy.start()
    waiting = iter(copies)

    def settle(count):
        for _ in range(count):
            next(waiting).wait()

    if with_norm:
        stats_in, gain_ref, shift_ref = small_refs[7:]
        settle(5)
        terms = norm_terms(
            stats_in[...],
            total_nodes,
            gain_ref[layer - 1 : layer, :].astype(F32),
            shift_ref[layer - 1 : layer, :].astype(F32),
        )
    else:
        settle(2)
    for c in range(ROWS_IN // CHUNK):
        if c and c * CHUNK % piece == 0:
            settle(1)
        states = recv_ref[c * CHUNK : (c + 1) * CHUNK, :]
        if with_norm:
            states = normalize(states.astype(F32), terms)
        left = dot(states, wl_ref[...]).astype(BF16).astype(F32)
        put_rows(table_ref, NODES_OWN + c * CHUNK, left)
    settle(3)
    heads = head_rows(attn_ref, layer)
    for k in range(NODE_CHUNKS):
        put_rows(table_ref, k * CHUNK, left_ref[k * CHUNK : (k + 1) * CHUNK, :].astype(F32))

    def fetch(c, out_ref):
        fetch_rows(srcs_ref, c * CHUNK, table_ref, out_ref, 1)

    def score(c, in_ref):
        at = slice(c * CHUNK, (c + 1) * CHUNK)
        src = get_rows(in_ref)
        edge_ref[at, :] = src.astype(BF16)
        score_ref[:, at] = scores_of(heads, leaky(src + dst_ref[at, :].astype(F32)))

    fetch(0, even_ref)
    settle(1)

    for c in range(EDGE_CHUNKS // 2):
        fetch(2 * c + 1, odd_ref)
        score(2 * c, even_ref)
        if 2 * c + 2 < EDGE_CHUNKS:
            fetch(2 * c + 2, even_ref)
        score(2 * c + 1, odd_ref)

    settle(4)
    tgt = rows_ref[0:1, :]
    start = rows_ref[1:2, :]
    end = rows_ref[2:3, :]
    lane = iota((8, EDGES_OWN), 1)
    live = tgt < NODES_OWN
    longest = bound_ref[0, 2 * EDGE_CHUNKS]
    scores = jnp.where(live, score_ref[...] + bias_ref[...], -1e30)
    own = self_ref[...]
    ahead, back = scan_both(scan_ref, longest, lane, start, end, jnp.maximum, -1e30, scores)
    top = jnp.maximum(jnp.maximum(ahead, back), own)
    weights = jnp.where(live, jnp.exp(scores - top), 0.0)
    own_weights = jnp.exp(own - top)
    ahead, back = scan_both(scan_ref, longest, lane, start, end, jnp.add, 0.0, weights)
    denom = own_weights + (ahead + (back - weights))
    last = live & (lane == end)
    score_ref[...] = weights / denom
    scan_ref[0] = jnp.where(last, own_weights / denom, 0.0)
    spread = head_spread()

    def mix(c, carry):
        at = pl.ds(pl.multiple_of(c * CHUNK, CHUNK), CHUNK)
        pair = jnp.concatenate([score_ref[:, at], scan_ref[0, :, at]], axis=0)
        wide = dot(jnp.transpose(pair).astype(BF16), spread)
        mix_ref[at, :FEAT] = (wide[:, :FEAT] * edge_ref[at, :].astype(F32)).astype(BF16)
        mix_ref[at, FEAT:] = wide[:, FEAT:].astype(BF16)
        return carry

    lax.fori_loop(0, EDGE_CHUNKS, mix, 0, unroll=EDGE_CHUNKS)
    acc_ref[...] = jnp.zeros_like(acc_ref)

    for c in range(EDGE_CHUNKS):
        here = slice(c * CHUNK, (c + 1) * CHUNK)
        low = lax.div(bound_ref[0, 2 * c], 8) * 8
        count = lax.div(jnp.maximum(bound_ref[0, 2 * c + 1] - low + WINDOW, 0), WINDOW)

        def window(w, carry, low=low, here=here):
            first = pl.multiple_of(low + w * WINDOW, 8)
            hot = one_hot(iota((WINDOW, CHUNK), 0) + first == rows_ref[0:1, here])
            acc_ref[pl.ds(first, WINDOW), :] += dot(hot, mix_ref[here, :])
            return carry

        window(0, 0)
        lax.fori_loop(1, count, window, 0)

    settle(2)
    totals = jnp.zeros((2, FEAT), F32)
    stores = []
    for k in range(NODE_CHUNKS):
        at = slice(k * CHUNK, (k + 1) * CHUNK)
        own_alpha = jnp.where(noedge_ref[at, 0:1] > 0, 1.0, acc_ref[at, FEAT:])
        message = acc_ref[at, :FEAT] + own_alpha * left_ref[at, :].astype(F32)
        summed = base_ref[at, :] + message
        summed_ref[at, :] = summed
        sums = [jnp.sum(summed, axis=0, keepdims=True)]
        sums += [jnp.sum(summed * summed, axis=0, keepdims=True)]
        totals += jnp.concatenate(sums, axis=0)
        if with_send:
            round_ref[at, :] = summed.astype(BF16)
        store = pltpu.make_async_copy(summed_ref.at[at], summed_hbm.at[at], out_sems.at[k])
        store.start()
        stores.append(store)
    for k in range(COPIES):
        stats_ref[k] = totals
    stores.append(pltpu.make_async_copy(stats_ref, stats_hbm, out_sems.at[NODE_CHUNKS]))
    stores[-1].start()
    if with_send:
        stores.append(pltpu.make_async_copy(round_ref, round_hbm, out_sems.at[NODE_CHUNKS + 1]))
        stores[-1].start()
    for store in stores:
        store.wait()


def shaped(rows, cols, dtype):
    return jax.ShapeDtypeStruct((rows, cols), dtype)


SMEM = pl.BlockSpec(memory_space=pltpu.SMEM)
VMEM = pl.BlockSpec(memory_space=pltpu.VMEM)
ANY = pl.BlockSpec(memory_space=pl.ANY)
HBM = pl.BlockSpec(memory_space=pltpu.HBM)


def call(body, name, outs, scratch, flops, args, in_specs=None, out_specs=None):
    cost = pl.CostEstimate(flops=flops, bytes_accessed=4 << 20, transcendentals=0)
    return pl.pallas_call(
        body,
        name=name,
        out_shape=outs,
        in_specs=in_specs or [VMEM] * len(args),
        out_specs=out_specs or [VMEM] * len(outs),
        scratch_shapes=scratch,
        cost_estimate=cost,
        compiler_params=pltpu.CompilerParams(vmem_limit_bytes=67_000_000),
    )(*args)


GIGA = 1 << 30


def send_rows(send_list, table):
    return call(
        send_kernel,
        "send_rows",
        [shaped(ROWS_IN, FEAT, BF16)],
        [
            pltpu.VMEM((2 * NODES_OWN, FEAT // 2), F32),
            pltpu.VMEM((2 * CHUNK, FEAT // 2), F32),
            pltpu.VMEM((ROWS_IN, FEAT), BF16),
            pltpu.SemaphoreType.DMA((ROWS_IN // (2 * CHUNK),)),
        ],
        GIGA,
        [send_list, send_list, table],
        in_specs=[SMEM, VMEM, VMEM],
        out_specs=[HBM],
    )[0]


def sort_edges(sources, targets, valids, bias):
    return call(
        sort_kernel,
        "sort_edges",
        [
            shaped(8, EDGES_OWN, jnp.int32),
            shaped(1, EDGES_OWN, jnp.int32),
            shaped(8, EDGES_OWN, F32),
            shaped(NODES_OWN, 8, F32),
            shaped(1, 32, jnp.int32),
        ],
        [
            pltpu.VMEM((EDGES_OWN, 8), jnp.int32),
            pltpu.VMEM((1, EDGES_OWN), F32),
            pltpu.VMEM((32, EDGES_OWN), F32),
        ],
        2 * GIGA,
        [sources, targets, valids, bias],
        out_specs=[VMEM, VMEM, VMEM, VMEM, SMEM],
    )


def own_part(layer, total_nodes, args):
    in_specs = [VMEM] * len(args)
    in_specs[0] = HBM
    in_specs[-1] = SMEM
    return call(
        functools.partial(own_kernel, layer, total_nodes, layer > 0),
        "own_part",
        [
            shaped(NODES_OWN, FEAT, BF16),
            shaped(NODES_OWN, FEAT, F32),
            shaped(EDGES_OWN, FEAT, BF16),
            shaped(8, EDGES_OWN, F32),
        ],
        [
            pltpu.VMEM((NODES_OWN + CHUNK, FEAT + 128), BF16),
            pltpu.VMEM((CHUNK, FEAT + 128), F32),
            pltpu.VMEM((NODES_OWN, FEAT), args[0].dtype),
            pltpu.VMEM((NODES_OWN, FEAT), BF16),
            pltpu.VMEM((NODES_OWN, FEAT), F32),
            pltpu.VMEM((EDGES_OWN, FEAT), BF16),
            pltpu.SemaphoreType.DMA((NODE_CHUNKS + 3,)),
        ],
        3 * GIGA,
        args,
        in_specs=in_specs,
        out_specs=[HBM, HBM, HBM, VMEM],
    )


def edge_part(layer, total_nodes, with_send, args):
    outs = [
        shaped(NODES_OWN, FEAT, F32),
        jax.ShapeDtypeStruct((COPIES, 2, FEAT), F32),
    ]
    if with_send:
        outs.append(shaped(NODES_OWN, FEAT, BF16))
    half = FEAT // 2
    scratch = [
        pltpu.VMEM((ROWS_IN, FEAT), BF16),
        pltpu.VMEM((NODES_OWN, FEAT), BF16),
        pltpu.VMEM((EDGES_OWN, FEAT), BF16),
        pltpu.VMEM((NODES_OWN, 8), F32),
        pltpu.VMEM((NODES_OWN, FEAT), F32),
        pltpu.SemaphoreType.DMA((len(args) + 3,)),
        pltpu.VMEM((2 * TABLE_ROWS, half), F32),
        pltpu.VMEM((2 * CHUNK, half), F32),
        pltpu.VMEM((2 * CHUNK, half), F32),
        pltpu.VMEM((EDGES_OWN, FEAT), BF16),
        pltpu.VMEM((8, EDGES_OWN), F32),
        pltpu.VMEM((2, 8, EDGES_OWN), F32),
        pltpu.VMEM((EDGES_OWN, 2 * FEAT), BF16),
        pltpu.VMEM((NODES_OWN + WINDOW, 2 * FEAT), F32),
        pltpu.SemaphoreType.DMA((NODE_CHUNKS + 2,)),
        pltpu.VMEM((NODES_OWN, FEAT), F32),
        pltpu.VMEM((COPIES, 2, FEAT), F32),
        pltpu.VMEM((NODES_OWN, FEAT), BF16),
        pltpu.VMEM((FEAT, FEAT), BF16),
        pltpu.VMEM((LAYERS, FEAT), BF16),
        pltpu.VMEM((8, EDGES_OWN), F32),
        pltpu.VMEM((8, EDGES_OWN), jnp.int32),
        pltpu.SMEM((1, EDGES_OWN), jnp.int32),
        pltpu.VMEM((8, EDGES_OWN), F32),
        pltpu.SMEM((1, 32), jnp.int32),
    ]
    if layer > 0:
        scratch += [pltpu.VMEM((2, FEAT), F32)]
        scratch += [pltpu.VMEM((LAYERS, FEAT), BF16)] * 2
    return call(
        functools.partial(edge_kernel, layer, total_nodes, layer > 0, with_send),
        "edge_part",
        outs,
        scratch,
        5 * GIGA,
        args,
        in_specs=[HBM] * len(args),
        out_specs=[HBM] * len(outs),
    )


def deliver(rows):
    return lax.all_to_all(
        rows.reshape(-1, 8, rows.shape[1]), GRP_BLK, split_axis=0, concat_axis=0, tiled=True
    ).reshape(rows.shape)


def shifted(value, axis, amount):
    size = lax.axis_size(axis)
    return lax.ppermute(value, axis, [(i, (i + amount) % size) for i in range(size)])


def copies_summed(copies, axes):
    return jnp.sum(lax.all_to_all(copies, axes, 0, 0, tiled=True), axis=0)


def total_along(copies):
    return copies_summed(copies, ("blk_0",))


def total_inside(stats):
    stats = stats + shifted(stats, "blk_2", 1)
    for axis in ("blk_1", "grp"):
        stats = stats + (
            shifted(stats, axis, 1) + shifted(stats, axis, 2) + shifted(stats, axis, 3)
        )
    return stats


def total_alone(copies):
    stats = copies_summed(copies, ("blk_1", "blk_2"))
    axes = ("grp", "blk_0")
    copies = jnp.broadcast_to(stats[None], (lax.axis_size(axes),) + stats.shape)
    return copies_summed(copies, axes)


def local(
    features,
    source_index,
    target_index,
    edge_valid,
    edge_bias,
    send_list,
    w_left,
    w_right,
    w_skip,
    attn_vec,
    norm_gain,
    norm_shift,
    peers,
):
    total_nodes = float(features.shape[0] * peers)
    row = (1, EDGES_OWN)
    sent = send_rows(send_list, features)
    received = deliver(sent)
    rows, srcs, bias, noedge, bound = sort_edges(
        source_index.reshape(row), target_index.reshape(row), edge_valid.reshape(row), edge_bias
    )
    weights = [w_left, w_right, w_skip, attn_vec, rows, bound]
    left, base, dst, own = own_part(0, total_nodes, [features] + weights)
    edges = [rows, srcs, bias, bound]
    summed, stats, rounded = edge_part(
        0,
        total_nodes,
        True,
        [received, left, dst, noedge, base, w_left, attn_vec, own] + edges,
    )
    stats = total_along(stats)
    sent = send_rows(send_list, rounded)
    sent, stats = lax.optimization_barrier((sent, stats))
    received = deliver(sent)
    stats = total_inside(stats)
    norms = [stats, norm_gain, norm_shift]
    left, base, dst, own = own_part(1, total_nodes, [summed] + norms + weights)
    summed, stats = edge_part(
        1,
        total_nodes,
        False,
        [received, left, dst, noedge, base, w_left, attn_vec, own] + edges + norms,
    )
    stats = total_alone(stats)
    terms = norm_terms(stats, total_nodes, norm_gain[1:2].astype(F32), norm_shift[1:2].astype(F32))
    return normalize(summed, terms)


def solution(mesh):
    split = Mesh(
        mesh.devices.reshape(mesh.shape["grp"], 8, 4, 2), ("grp", "blk_0", "blk_1", "blk_2")
    )
    edge = P(GRP_BLK, None)
    in_specs = (edge,) * 4 + (P(None, GRP_BLK), edge) + (P(),) * 6
    return jax.shard_map(
        functools.partial(local, peers=mesh.size),
        mesh=split,
        in_specs=in_specs,
        out_specs=edge,
        check_vma=False,
    )
```

```python
import functools

import jax
import jax.numpy as jnp
from jax import lax
from jax.experimental import pallas as pl
from jax.experimental.pallas import tpu as pltpu
from jax.sharding import Mesh
from jax.sharding import PartitionSpec as P

HEADS = 8
LAYERS = 2
GRP_BLK = ("grp", "blk_0", "blk_1", "blk_2")
NODES_OWN = 1024
EDGES_OWN = 2048
ROWS_IN = 2048
FEAT = 256
CHUNK = 256
EDGE_CHUNKS = EDGES_OWN // CHUNK
NODE_CHUNKS = NODES_OWN // CHUNK
WINDOW = 160
COPIES = 8
TABLE_ROWS = NODES_OWN + ROWS_IN
F32 = jnp.float32
BF16 = jnp.bfloat16


def iota(shape, dim):
    return lax.broadcasted_iota(jnp.int32, shape, dim)


def one_hot(mask):
    return jnp.where(mask, 1.0, 0.0).astype(BF16)


def dot(lhs, rhs):
    return jnp.dot(lhs, rhs, preferred_element_type=F32)


def dot_t(lhs, rhs):
    return lax.dot_general(lhs, rhs, (((1,), (1,)), ((), ())), preferred_element_type=F32)


def leaky(values):
    return jnp.where(values > 0, values, 0.2 * values)


def split_two(values):
    high = values.astype(BF16)
    return high, (values - high.astype(F32)).astype(BF16)


def split_three(values):
    high = values.astype(BF16)
    rest = values - high.astype(F32)
    mid = rest.astype(BF16)
    return high, mid, (rest - mid.astype(F32)).astype(BF16)


def head_rows(attn_ref, layer):
    shape = (16, FEAT)
    owner = iota(shape, 1) // (FEAT // HEADS) == iota(shape, 0)
    row = attn_ref[layer : layer + 1, :].astype(F32)
    return jnp.where(owner, row, 0.0).astype(BF16)


def head_spread():
    shape = (16, 2 * FEAT)
    return one_hot(iota(shape, 1) // (FEAT // HEADS) == iota(shape, 0))


def scores_of(heads, hidden):
    high, low = split_two(hidden)
    return (dot_t(heads, high) + dot_t(heads, low))[:HEADS]


def norm_terms(stats, total_nodes, gain, shift):
    mean = stats[0:1, :] / total_nodes
    spread = jnp.maximum(stats[1:2, :] / total_nodes - mean * mean, 0.0)
    return mean, lax.rsqrt(spread + 0.1), gain, shift


def normalize(values, terms):
    mean, inv, gain, shift = terms
    scaled = (values - mean) * inv * gain + shift
    grown = jnp.exp(jnp.minimum(scaled, 0.0)) - 1.0
    return jnp.where(scaled > 0, scaled, grown).astype(BF16)


def columns_of(row):
    return jnp.transpose(jnp.broadcast_to(row, (8, row.shape[1])))


def put_rows(pairs_ref, first, values):
    half = FEAT // 2
    pairs_ref[pl.ds(2 * first, CHUNK, stride=2), :] = values[:, :half]
    pairs_ref[pl.ds(2 * first + 1, CHUNK, stride=2), :] = values[:, half:]


def get_rows(pairs_ref):
    return jnp.concatenate(
        [pairs_ref[pl.ds(0, CHUNK, stride=2), :], pairs_ref[pl.ds(1, CHUNK, stride=2), :]], axis=1
    )


def fetch_rows(index_ref, first, pairs_ref, got_ref, scale):
    for e in range(CHUNK):
        row = pl.multiple_of(index_ref[0, first + e] * scale, 2)
        got_ref[2 * e : 2 * e + 2, :] = pairs_ref[pl.ds(row, 2), :]


def send_kernel(index_ref, list_ref, table_ref, out_hbm, pairs_ref, got_ref, out_ref, sems):
    for k in range(NODE_CHUNKS):
        put_rows(pairs_ref, k * CHUNK, table_ref[k * CHUNK : (k + 1) * CHUNK, :].astype(F32))

    def store(c):
        at = slice(c * 2 * CHUNK, (c + 1) * 2 * CHUNK)
        return pltpu.make_async_copy(out_ref.at[at], out_hbm.at[at], sems.at[c])

    count = ROWS_IN // (2 * CHUNK)
    for c in range(count):
        here = slice(c * 2 * CHUNK, c * 2 * CHUNK + CHUNK)
        after = slice(c * 2 * CHUNK + CHUNK, (c + 1) * 2 * CHUNK)
        fetch_rows(index_ref, c * 2 * CHUNK + CHUNK, pairs_ref, got_ref, 2)
        col = columns_of(list_ref[0:1, here].astype(F32)).astype(jnp.int32)[:, 0:1]
        hot = one_hot(col == iota((CHUNK, NODES_OWN), 1))
        out_ref[here, :] = dot(hot, table_ref[...]).astype(BF16)
        out_ref[after, :] = get_rows(got_ref).astype(BF16)
        store(c).start()
    for c in range(count):
        store(c).wait()


def sort_kernel(
    src_ref, tgt_ref, valid_ref, bias_ref, rows_ref, srcs_ref, bias_out, noedge_ref, bound_ref,
    key_ref, pos_ref, meta_ref,
):
    width = (1, EDGES_OWN)
    live_in = valid_ref[...] > 0
    src = src_ref[...]
    tgt = jnp.where(live_in, tgt_ref[...], NODES_OWN)
    key = tgt * EDGES_OWN + iota(width, 1)
    key_ref[...] = columns_of(key.astype(F32)).astype(jnp.int32)
    pos_ref[...] = jnp.zeros_like(pos_ref)

    def rank(c, carry):
        at = pl.ds(pl.multiple_of(c * CHUNK, CHUNK), CHUNK)
        less = jnp.where(key_ref[at, 0:1] < key, 1.0, 0.0)
        pos_ref[...] += jnp.sum(less, axis=0, keepdims=True)
        return carry

    lax.fori_loop(0, EDGE_CHUNKS, rank, 0)
    pos = pos_ref[...].astype(jnp.int32)
    sub = iota((8, EDGES_OWN), 0)
    ints = jnp.where(
        sub == 0,
        src // 256,
        jnp.where(sub == 1, src % 256, jnp.where(sub == 2, tgt // 256, tgt % 256)),
    )
    high, mid, low = split_three(bias_ref[...])
    meta = jnp.concatenate(
        [ints.astype(F32), high.astype(F32), mid.astype(F32), low.astype(F32)], axis=0
    ).astype(BF16)

    def place(c, carry):
        at = pl.ds(pl.multiple_of(c * CHUNK, CHUNK), CHUNK)
        perm = one_hot(pos == iota((CHUNK, EDGES_OWN), 0) + c * CHUNK)
        meta_ref[:, at] = dot_t(meta, perm)
        return carry

    lax.fori_loop(0, EDGE_CHUNKS, place, 0)
    placed = meta_ref[...]
    bias_out[...] = placed[8:16] + placed[16:24] + placed[24:32]
    src_s = (placed[0:1] * 256.0 + placed[1:2]).astype(jnp.int32)
    tgt_s = (placed[2:3] * 256.0 + placed[3:4]).astype(jnp.int32)
    lane8 = iota((8, EDGES_OWN), 1)
    srcs_ref[...] = 2 * src_s
    tgt8 = jnp.broadcast_to(tgt_s, (8, EDGES_OWN))
    before = pltpu.roll(tgt8, 1, 1)
    after = pltpu.roll(tgt8, EDGES_OWN - 1, 1)
    live = tgt8 < NODES_OWN
    first = (lane8 == 0) | (before != tgt8)
    last = (lane8 == EDGES_OWN - 1) | (after != tgt8)
    start = jnp.where(first, lane8, 0)
    end = jnp.where(last, lane8, EDGES_OWN)
    step = 1
    while step < EDGES_OWN:
        start = jnp.maximum(start, jnp.where(lane8 >= step, pltpu.roll(start, step, 1), 0))
        shifted = pltpu.roll(end, EDGES_OWN - step, 1)
        end = jnp.minimum(end, jnp.where(lane8 + step < EDGES_OWN, shifted, EDGES_OWN))
        step *= 2
    start = jnp.where(live, start, lane8)
    end = jnp.where(live, end, lane8)
    rows_ref[...] = jnp.where(
        sub == 0, tgt8, jnp.where(sub == 1, start, jnp.where(sub == 2, end, lane8))
    )
    bound_ref[0, 2 * EDGE_CHUNKS] = jnp.max(end - start) + 1
    for c in range(EDGE_CHUNKS):
        piece = tgt8[:, c * CHUNK : (c + 1) * CHUNK]
        bound_ref[0, 2 * c] = jnp.min(piece)
        bound_ref[0, 2 * c + 1] = jnp.max(jnp.where(piece < NODES_OWN, piece, -1))
    for k in range(NODE_CHUNKS):
        hit = jnp.where(iota((CHUNK, EDGES_OWN), 0) + k * CHUNK == tgt_s, 1.0, 0.0)
        found = jnp.max(hit, axis=1, keepdims=True)
        noedge_ref[k * CHUNK : (k + 1) * CHUNK, :] = jnp.broadcast_to(1.0 - found, (CHUNK, 8))


def own_kernel(layer, total_nodes, with_norm, *refs):
    refs = list(refs)
    state_ref = refs.pop(0)
    if with_norm:
        stats_ref, gain_ref, shift_ref = refs[:3]
        refs = refs[3:]
        terms = norm_terms(
            stats_ref[...],
            total_nodes,
            gain_ref[layer - 1 : layer, :].astype(F32),
            shift_ref[layer - 1 : layer, :].astype(F32),
        )
    wl_ref, wr_ref, ws_ref, attn_ref, rows_ref, bound_ref = refs[:6]
    left_out, base_out, dst_hbm, self_out = refs[6:10]
    table_ref, acc_ref, own_ref, left_ref, base_ref, dst_out, sems = refs[10:]
    loads = []
    for k in range(NODE_CHUNKS):
        at = slice(k * CHUNK, (k + 1) * CHUNK)
        loads.append(pltpu.make_async_copy(state_ref.at[at], own_ref.at[at], sems.at[k]))
        loads[-1].start()
    stores = [
        pltpu.make_async_copy(left_ref, left_out, sems.at[NODE_CHUNKS]),
        pltpu.make_async_copy(base_ref, base_out, sems.at[NODE_CHUNKS + 1]),
        pltpu.make_async_copy(dst_out, dst_hbm, sems.at[NODE_CHUNKS + 2]),
    ]
    heads = head_rows(attn_ref, layer)
    for k in range(NODE_CHUNKS):
        at = slice(k * CHUNK, (k + 1) * CHUNK)
        loads[k].wait()
        states = own_ref[at, :]
        if with_norm:
            states = normalize(states, terms)
        left = dot(states, wl_ref[layer]).astype(BF16)
        right = dot(states, wr_ref[layer]).astype(BF16)
        left_ref[at, :] = left
        table_ref[at, :FEAT] = right
        base_ref[at, :] = states.astype(F32) + dot(states, ws_ref[layer])
        own = scores_of(heads, leaky(left.astype(F32) + right.astype(F32)))
        high, mid, low = split_three(own)
        parts = [high.astype(F32), mid.astype(F32), low.astype(F32)]
        parts += [jnp.zeros((128 - 3 * HEADS, CHUNK), F32)]
        table_ref[at, FEAT:] = jnp.transpose(jnp.concatenate(parts, axis=0)).astype(BF16)
    table_ref[NODES_OWN:, :] = jnp.zeros((CHUNK, FEAT + 128), BF16)
    stores[0].start()
    stores[1].start()

    def step(c, carry):
        at = pl.ds(pl.multiple_of(c * CHUNK, CHUNK), CHUNK)
        col = columns_of(rows_ref[0:1, at].astype(F32)).astype(jnp.int32)[:, 0:1]
        low = lax.div(bound_ref[0, 2 * c], 16) * 16
        extra = lax.div(jnp.maximum(bound_ref[0, 2 * c + 1] - low, 0), CHUNK)

        def window(w):
            base = pl.multiple_of(jnp.minimum(low + w * CHUNK, NODES_OWN), 16)
            hot = one_hot(col - base == iota((CHUNK, CHUNK), 1))
            return dot(hot, table_ref[pl.ds(base, CHUNK), :])

        acc_ref[...] = window(0)

        def more(w, carry):
            acc_ref[...] += window(w)
            return carry

        lax.fori_loop(1, extra + 1, more, 0)
        dst_out[at, :] = acc_ref[:, :FEAT].astype(BF16)
        back = jnp.transpose(acc_ref[:, FEAT:])
        self_out[:, at] = back[0:8] + back[8:16] + back[16:24]
        return carry

    lax.fori_loop(0, EDGE_CHUNKS, step, 0, unroll=2)
    stores[2].start()
    for store in stores:
        store.wait()


def scan_both(ref, longest, lane, start, end, join, neutral, values):
    def advance(ahead, back, step):
        moved = pltpu.roll(ahead, step, 1)
        ahead = join(ahead, jnp.where(lane - step >= start, moved, neutral))
        moved = pltpu.roll(back, EDGES_OWN - step, 1)
        return ahead, join(back, jnp.where(lane + step <= end, moved, neutral))

    ahead, back = values, values
    for step in (1, 2, 4, 8):
        ahead, back = advance(ahead, back, step)
    ref[0] = ahead
    ref[1] = back

    def rest():
        step = 16
        while step < EDGES_OWN:
            ref[0], ref[1] = advance(ref[0], ref[1], step)
            step *= 2

    pl.when(longest > 16)(rest)
    return ref[0], ref[1]


def edge_kernel(layer, total_nodes, with_norm, with_send, *refs):
    refs = list(refs)
    recv_any, left_any, dst_any, noedge_any, base_any = refs[:5]
    small = 10 if with_norm else 7
    small_any = refs[5 : 5 + small]
    refs = refs[5 + small :]
    summed_hbm, stats_hbm = refs[:2]
    refs = refs[2:]
    if with_send:
        round_hbm = refs.pop(0)
    recv_ref, left_ref, dst_ref, noedge_ref, base_ref, sems = refs[:6]
    table_ref, even_ref, odd_ref, edge_ref, score_ref, scan_ref, mix_ref, acc_ref = refs[6:14]
    out_sems, summed_ref, stats_ref, round_ref = refs[14:18]
    small_refs = refs[18:]
    wl_ref, attn_ref, self_ref, rows_ref, srcs_ref, bias_ref, bound_ref = small_refs[:7]
    piece = ROWS_IN // 4
    pieces = [slice(k * piece, (k + 1) * piece) for k in range(4)]
    moves = [(small_any[0].at[layer], wl_ref), (recv_any.at[pieces[0]], recv_ref.at[pieces[0]])]
    moves += list(zip(small_any[7:], small_refs[7:]))
    moves += [(recv_any.at[at], recv_ref.at[at]) for at in pieces[1:]]
    moves += [(small_any[4], srcs_ref), (left_any, left_ref), (small_any[1], attn_ref)]
    moves += [(dst_any, dst_ref), (small_any[3], rows_ref), (small_any[6], bound_ref)]
    moves += [(small_any[2], self_ref), (small_any[5], bias_ref)]
    moves += [(noedge_any, noedge_ref), (base_any, base_ref)]
    copies = [
        pltpu.make_async_copy(source, target, sems.at[i])
        for i, (source, target) in enumerate(moves)
    ]
    for copy in copies:
        copy.start()
    waiting = iter(copies)

    def settle(count):
        for _ in range(count):
            next(waiting).wait()

    if with_norm:
        stats_in, gain_ref, shift_ref = small_refs[7:]
        settle(5)
        terms = norm_terms(
            stats_in[...],
            total_nodes,
            gain_ref[layer - 1 : layer, :].astype(F32),
            shift_ref[layer - 1 : layer, :].astype(F32),
        )
    else:
        settle(2)
    for c in range(ROWS_IN // CHUNK):
        if c and c * CHUNK % piece == 0:
            settle(1)
        states = recv_ref[c * CHUNK : (c + 1) * CHUNK, :]
        if with_norm:
            states = normalize(states.astype(F32), terms)
        left = dot(states, wl_ref[...]).astype(BF16).astype(F32)
        put_rows(table_ref, NODES_OWN + c * CHUNK, left)
    settle(3)
    heads = head_rows(attn_ref, layer)
    for k in range(NODE_CHUNKS):
        put_rows(table_ref, k * CHUNK, left_ref[k * CHUNK : (k + 1) * CHUNK, :].astype(F32))

    def fetch(c, out_ref):
        fetch_rows(srcs_ref, c * CHUNK, table_ref, out_ref, 1)

    def score(c, in_ref):
        at = slice(c * CHUNK, (c + 1) * CHUNK)
        src = get_rows(in_ref)
        edge_ref[at, :] = src.astype(BF16)
        score_ref[:, at] = scores_of(heads, leaky(src + dst_ref[at, :].astype(F32)))

    fetch(0, even_ref)
    settle(1)

    for c in range(EDGE_CHUNKS // 2):
        fetch(2 * c + 1, odd_ref)
        score(2 * c, even_ref)
        if 2 * c + 2 < EDGE_CHUNKS:
            fetch(2 * c + 2, even_ref)
        score(2 * c + 1, odd_ref)

    settle(4)
    tgt = rows_ref[0:1, :]
    start = rows_ref[1:2, :]
    end = rows_ref[2:3, :]
    lane = iota((8, EDGES_OWN), 1)
    live = tgt < NODES_OWN
    longest = bound_ref[0, 2 * EDGE_CHUNKS]
    scores = jnp.where(live, score_ref[...] + bias_ref[...], -1e30)
    own = self_ref[...]
    ahead, back = scan_both(scan_ref, longest, lane, start, end, jnp.maximum, -1e30, scores)
    top = jnp.maximum(jnp.maximum(ahead, back), own)
    weights = jnp.where(live, jnp.exp(scores - top), 0.0)
    own_weights = jnp.exp(own - top)
    ahead, back = scan_both(scan_ref, longest, lane, start, end, jnp.add, 0.0, weights)
    denom = own_weights + (ahead + (back - weights))
    last = live & (lane == end)
    score_ref[...] = weights / denom
    scan_ref[0] = jnp.where(last, own_weights / denom, 0.0)
    spread = head_spread()

    def mix(c, carry):
        at = pl.ds(pl.multiple_of(c * CHUNK, CHUNK), CHUNK)
        pair = jnp.concatenate([score_ref[:, at], scan_ref[0, :, at]], axis=0)
        wide = dot(jnp.transpose(pair).astype(BF16), spread)
        mix_ref[at, :FEAT] = (wide[:, :FEAT] * edge_ref[at, :].astype(F32)).astype(BF16)
        mix_ref[at, FEAT:] = wide[:, FEAT:].astype(BF16)
        return carry

    lax.fori_loop(0, EDGE_CHUNKS, mix, 0, unroll=EDGE_CHUNKS)
    acc_ref[...] = jnp.zeros_like(acc_ref)

    for c in range(EDGE_CHUNKS):
        here = slice(c * CHUNK, (c + 1) * CHUNK)
        low = lax.div(bound_ref[0, 2 * c], 8) * 8
        count = lax.div(jnp.maximum(bound_ref[0, 2 * c + 1] - low + WINDOW, 0), WINDOW)

        def window(w, carry, low=low, here=here):
            first = pl.multiple_of(low + w * WINDOW, 8)
            hot = one_hot(iota((WINDOW, CHUNK), 0) + first == rows_ref[0:1, here])
            acc_ref[pl.ds(first, WINDOW), :] += dot(hot, mix_ref[here, :])
            return carry

        window(0, 0)
        lax.fori_loop(1, count, window, 0)

    settle(2)
    totals = jnp.zeros((2, FEAT), F32)
    stores = []
    for k in range(NODE_CHUNKS):
        at = slice(k * CHUNK, (k + 1) * CHUNK)
        own_alpha = jnp.where(noedge_ref[at, 0:1] > 0, 1.0, acc_ref[at, FEAT:])
        message = acc_ref[at, :FEAT] + own_alpha * left_ref[at, :].astype(F32)
        summed = base_ref[at, :] + message
        summed_ref[at, :] = summed
        sums = [jnp.sum(summed, axis=0, keepdims=True)]
        sums += [jnp.sum(summed * summed, axis=0, keepdims=True)]
        totals += jnp.concatenate(sums, axis=0)
        if with_send:
            round_ref[at, :] = summed.astype(BF16)
        store = pltpu.make_async_copy(summed_ref.at[at], summed_hbm.at[at], out_sems.at[k])
        store.start()
        stores.append(store)
    for k in range(COPIES):
        stats_ref[k] = totals
    stores.append(pltpu.make_async_copy(stats_ref, stats_hbm, out_sems.at[NODE_CHUNKS]))
    stores[-1].start()
    if with_send:
        stores.append(pltpu.make_async_copy(round_ref, round_hbm, out_sems.at[NODE_CHUNKS + 1]))
        stores[-1].start()
    for store in stores:
        store.wait()


def shaped(rows, cols, dtype):
    return jax.ShapeDtypeStruct((rows, cols), dtype)


SMEM = pl.BlockSpec(memory_space=pltpu.SMEM)
VMEM = pl.BlockSpec(memory_space=pltpu.VMEM)
ANY = pl.BlockSpec(memory_space=pl.ANY)
HBM = pl.BlockSpec(memory_space=pltpu.HBM)


def call(body, name, outs, scratch, flops, args, in_specs=None, out_specs=None):
    cost = pl.CostEstimate(flops=flops, bytes_accessed=4 << 20, transcendentals=0)
    return pl.pallas_call(
        body,
        name=name,
        out_shape=outs,
        in_specs=in_specs or [VMEM] * len(args),
        out_specs=out_specs or [VMEM] * len(outs),
        scratch_shapes=scratch,
        cost_estimate=cost,
        compiler_params=pltpu.CompilerParams(vmem_limit_bytes=67_000_000),
    )(*args)


GIGA = 1 << 30


def send_rows(send_list, table):
    return call(
        send_kernel,
        "send_rows",
        [shaped(ROWS_IN, FEAT, BF16)],
        [
            pltpu.VMEM((2 * NODES_OWN, FEAT // 2), F32),
            pltpu.VMEM((2 * CHUNK, FEAT // 2), F32),
            pltpu.VMEM((ROWS_IN, FEAT), BF16),
            pltpu.SemaphoreType.DMA((ROWS_IN // (2 * CHUNK),)),
        ],
        GIGA,
        [send_list, send_list, table],
        in_specs=[SMEM, VMEM, VMEM],
        out_specs=[HBM],
    )[0]


def sort_edges(sources, targets, valids, bias):
    return call(
        sort_kernel,
        "sort_edges",
        [
            shaped(8, EDGES_OWN, jnp.int32),
            shaped(1, EDGES_OWN, jnp.int32),
            shaped(8, EDGES_OWN, F32),
            shaped(NODES_OWN, 8, F32),
            shaped(1, 32, jnp.int32),
        ],
        [
            pltpu.VMEM((EDGES_OWN, 8), jnp.int32),
            pltpu.VMEM((1, EDGES_OWN), F32),
            pltpu.VMEM((32, EDGES_OWN), F32),
        ],
        2 * GIGA,
        [sources, targets, valids, bias],
        out_specs=[VMEM, VMEM, VMEM, VMEM, SMEM],
    )


def own_part(layer, total_nodes, args):
    in_specs = [VMEM] * len(args)
    in_specs[0] = HBM
    in_specs[-1] = SMEM
    return call(
        functools.partial(own_kernel, layer, total_nodes, layer > 0),
        "own_part",
        [
            shaped(NODES_OWN, FEAT, BF16),
            shaped(NODES_OWN, FEAT, F32),
            shaped(EDGES_OWN, FEAT, BF16),
            shaped(8, EDGES_OWN, F32),
        ],
        [
            pltpu.VMEM((NODES_OWN + CHUNK, FEAT + 128), BF16),
            pltpu.VMEM((CHUNK, FEAT + 128), F32),
            pltpu.VMEM((NODES_OWN, FEAT), args[0].dtype),
            pltpu.VMEM((NODES_OWN, FEAT), BF16),
            pltpu.VMEM((NODES_OWN, FEAT), F32),
            pltpu.VMEM((EDGES_OWN, FEAT), BF16),
            pltpu.SemaphoreType.DMA((NODE_CHUNKS + 3,)),
        ],
        3 * GIGA,
        args,
        in_specs=in_specs,
        out_specs=[HBM, HBM, HBM, VMEM],
    )


def edge_part(layer, total_nodes, with_send, args):
    outs = [
        shaped(NODES_OWN, FEAT, F32),
        jax.ShapeDtypeStruct((COPIES, 2, FEAT), F32),
    ]
    if with_send:
        outs.append(shaped(NODES_OWN, FEAT, BF16))
    half = FEAT // 2
    scratch = [
        pltpu.VMEM((ROWS_IN, FEAT), BF16),
        pltpu.VMEM((NODES_OWN, FEAT), BF16),
        pltpu.VMEM((EDGES_OWN, FEAT), BF16),
        pltpu.VMEM((NODES_OWN, 8), F32),
        pltpu.VMEM((NODES_OWN, FEAT), F32),
        pltpu.SemaphoreType.DMA((len(args) + 3,)),
        pltpu.VMEM((2 * TABLE_ROWS, half), F32),
        pltpu.VMEM((2 * CHUNK, half), F32),
        pltpu.VMEM((2 * CHUNK, half), F32),
        pltpu.VMEM((EDGES_OWN, FEAT), BF16),
        pltpu.VMEM((8, EDGES_OWN), F32),
        pltpu.VMEM((2, 8, EDGES_OWN), F32),
        pltpu.VMEM((EDGES_OWN, 2 * FEAT), BF16),
        pltpu.VMEM((NODES_OWN + WINDOW, 2 * FEAT), F32),
        pltpu.SemaphoreType.DMA((NODE_CHUNKS + 2,)),
        pltpu.VMEM((NODES_OWN, FEAT), F32),
        pltpu.VMEM((COPIES, 2, FEAT), F32),
        pltpu.VMEM((NODES_OWN, FEAT), BF16),
        pltpu.VMEM((FEAT, FEAT), BF16),
        pltpu.VMEM((LAYERS, FEAT), BF16),
        pltpu.VMEM((8, EDGES_OWN), F32),
        pltpu.VMEM((8, EDGES_OWN), jnp.int32),
        pltpu.SMEM((1, EDGES_OWN), jnp.int32),
        pltpu.VMEM((8, EDGES_OWN), F32),
        pltpu.SMEM((1, 32), jnp.int32),
    ]
    if layer > 0:
        scratch += [pltpu.VMEM((2, FEAT), F32)]
        scratch += [pltpu.VMEM((LAYERS, FEAT), BF16)] * 2
    return call(
        functools.partial(edge_kernel, layer, total_nodes, layer > 0, with_send),
        "edge_part",
        outs,
        scratch,
        5 * GIGA,
        args,
        in_specs=[HBM] * len(args),
        out_specs=[HBM] * len(outs),
    )


def deliver(rows):
    return lax.all_to_all(
        rows.reshape(-1, 8, rows.shape[1]), GRP_BLK, split_axis=0, concat_axis=0, tiled=True
    ).reshape(rows.shape)


def shifted(value, axis, amount):
    size = lax.axis_size(axis)
    return lax.ppermute(value, axis, [(i, (i + amount) % size) for i in range(size)])


def copies_summed(copies, axes):
    return jnp.sum(lax.all_to_all(copies, axes, 0, 0, tiled=True), axis=0)


def total_along(copies):
    return copies_summed(copies, ("blk_0",))


def total_inside(stats):
    stats = stats + shifted(stats, "blk_2", 1)
    for axis in ("blk_1", "grp"):
        stats = stats + (
            shifted(stats, axis, 1) + shifted(stats, axis, 2) + shifted(stats, axis, 3)
        )
    return stats


def total_alone(copies):
    return total_inside(total_along(copies))


def local(
    features,
    source_index,
    target_index,
    edge_valid,
    edge_bias,
    send_list,
    w_left,
    w_right,
    w_skip,
    attn_vec,
    norm_gain,
    norm_shift,
    peers,
):
    total_nodes = float(features.shape[0] * peers)
    row = (1, EDGES_OWN)
    sent = send_rows(send_list, features)
    received = deliver(sent)
    rows, srcs, bias, noedge, bound = sort_edges(
        source_index.reshape(row), target_index.reshape(row), edge_valid.reshape(row), edge_bias
    )
    weights = [w_left, w_right, w_skip, attn_vec, rows, bound]
    left, base, dst, own = own_part(0, total_nodes, [features] + weights)
    edges = [rows, srcs, bias, bound]
    summed, stats, rounded = edge_part(
        0,
        total_nodes,
        True,
        [received, left, dst, noedge, base, w_left, attn_vec, own] + edges,
    )
    stats = total_along(stats)
    sent = send_rows(send_list, rounded)
    sent, stats = lax.optimization_barrier((sent, stats))
    received = deliver(sent)
    stats = total_inside(stats)
    norms = [stats, norm_gain, norm_shift]
    left, base, dst, own = own_part(1, total_nodes, [summed] + norms + weights)
    summed, stats = edge_part(
        1,
        total_nodes,
        False,
        [received, left, dst, noedge, base, w_left, attn_vec, own] + edges + norms,
    )
    stats = total_alone(stats)
    terms = norm_terms(stats, total_nodes, norm_gain[1:2].astype(F32), norm_shift[1:2].astype(F32))
    return normalize(summed, terms)


def solution(mesh):
    split = Mesh(
        mesh.devices.reshape(mesh.shape["grp"], 8, 4, 2), ("grp", "blk_0", "blk_1", "blk_2")
    )
    edge = P(GRP_BLK, None)
    in_specs = (edge,) * 4 + (P(None, GRP_BLK), edge) + (P(),) * 6
    return jax.shard_map(
        functools.partial(local, peers=mesh.size),
        mesh=split,
        in_specs=in_specs,
        out_specs=edge,
        check_vma=False,
    )
```
